64 devices in a mesh: rep: 8 (over x, y, core), dp: 8 (over z).
Axes of the slice: x: 2, y: 2, z: 8, core: 2. Of those that a mesh axis runs over, the one named last changes fastest.
The devices are a block of a 4x4x8 slice.
Arguments:
- x: bfloat16 [64, 4096, 512], P(('rep', 'dp')), parts along dimension 0
- dy: bfloat16 [64, 4096, 512], P(('rep', 'dp')), parts along dimension 0
- w_gate: bfloat16 [2, 512, 1792], replicated
- w_up: bfloat16 [2, 512, 1792], replicated
- w_down: bfloat16 [2, 1792, 512], replicated
- m_w_gate: float32 [2, 512, 1792], replicated
- m_w_up: float32 [2, 512, 1792], replicated
- m_w_down: float32 [2, 1792, 512], replicated
- v_w_gate: float32 [2, 512, 1792], replicated
- v_w_up: float32 [2, 512, 1792], replicated
- v_w_down: float32 [2, 1792, 512], replicated
Outputs:
- output 1: bfloat16 [16, 512, 1792], P('rep'), parts along dimension 0
- output 2: bfloat16 [16, 512, 1792], P('rep'), parts along dimension 0
- output 3: bfloat16 [16, 1792, 512], P('rep'), parts along dimension 0
- output 4: float32 [16, 512, 1792], P('rep'), parts along dimension 0
- output 5: float32 [16, 512, 1792], P('rep'), parts along dimension 0
- output 6: float32 [16, 1792, 512], P('rep'), parts along dimension 0
- output 7: float32 [16, 512, 1792], P('rep'), parts along dimension 0
- output 8: float32 [16, 512, 1792], P('rep'), parts along dimension 0
- output 9: float32 [16, 1792, 512], P('rep'), parts along dimension 0
There are 8 independent parts. The reference program is written for one: setup_inputs(seed, part) draws one part's arguments, and reference() takes and returns one part's arrays. A program takes and returns all parts, laid end to end along the dimension named above; an argument that names none is the same for every part.
All inputs are finite; a program needn't handle non-finite values.
Results may differ from the reference program's by a relative error of at most 0.02.
Values are sent between devices in bfloat16 or wider.
A program may use at most 768 MiB of HBM per device.

```python
import jax
import jax.numpy as jnp
from jax import lax

SEQUENCES = 8
TOKENS = 4096
D = 512
FF = 1792
LAYERS = 2
NAMES = ("w_gate", "w_up", "w_down")
SHAPES = {"w_gate": (LAYERS, D, FF), "w_up": (LAYERS, D, FF), "w_down": (LAYERS, FF, D)}


def bump(key, n, height):
    away = (jnp.arange(n, dtype=jnp.int32) - jax.random.randint(key, (), 0, n, jnp.int32)) % n
    return jnp.where(away < n // 8, height, 1.0)


def together(key, own, strength):
    shared = jax.random.normal(key, own.shape[1:], jnp.float32)
    return (own + strength * shared) * lax.rsqrt(1 + strength * strength)


def setup_inputs(seed: int = 0, part: int = 0) -> dict:
    kx, kdy, ka, kb, kz, kf, kh, kl, *keys = jax.random.split(jax.random.key(seed), 8 + 3 * len(NAMES))
    kx, kdy, ka, kb = (jax.random.fold_in(k, part) for k in (kx, kdy, ka, kb))
    kw, km, kv = (keys[i::3] for i in range(3))
    shape = (SEQUENCES, TOKENS, D)
    much_x, much_dy = jax.random.uniform(kz, (2,), jnp.float32, 0.0, 1.0)
    loud = 2.0 ** jax.random.uniform(jax.random.fold_in(kz, 1), (), jnp.float32, -1.0, 2.0)
    layers = 2.0 ** jax.random.uniform(kl, (LAYERS, 1, 1), jnp.float32, -1.0, 1.0)
    x = together(ka, jax.random.normal(kx, shape, jnp.float32), much_x) * bump(kf, D, 4.0)
    dy = together(kb, jax.random.normal(kdy, shape, jnp.float32), much_dy)
    drawn = {"x": x.astype(jnp.bfloat16), "dy": (loud * dy * (SEQUENCES * TOKENS) ** -0.5).astype(jnp.bfloat16)}
    for key, name in zip(kw, NAMES, strict=True):
        w = jax.random.normal(key, SHAPES[name], jnp.float32) * SHAPES[name][1] ** -0.5
        drawn[name] = (w * {"w_gate": 1.0, "w_up": bump(kh, FF, 4.0), "w_down": layers}[name]).astype(jnp.bfloat16)
    for key, name in zip(km, NAMES, strict=True):
        drawn[f"m_{name}"] = 0.1 * jax.random.normal(key, SHAPES[name], jnp.float32)
    for key, name in zip(kv, NAMES, strict=True):
        drawn[f"v_{name}"] = jax.random.uniform(key, SHAPES[name], jnp.float32, 0.005, 0.015)
    return drawn


def matmul(a, w):
    return jnp.dot(a, w, preferred_element_type=jnp.float32).astype(jnp.bfloat16)


def normed(h):
    wide = h.astype(jnp.float32)
    scale = lax.rsqrt(jnp.mean(wide**2, -1, keepdims=True) + 1e-6)
    return (wide * scale).astype(jnp.bfloat16)


def layer(h, w):
    a = normed(h)
    gate = jnp.dot(a, w["w_gate"], preferred_element_type=jnp.float32)
    up = jnp.dot(a, w["w_up"], preferred_element_type=jnp.float32)
    return h + matmul((jax.nn.silu(gate) * up).astype(jnp.bfloat16), w["w_down"])


def adamw(w, m, v, g):
    m = 0.9 * m + 0.1 * g
    v = 0.95 * v + 0.05 * g * g
    step = m * lax.rsqrt(v + 1e-8) + 0.1 * w
    return (w - 0.02 * step).astype(jnp.bfloat16), m, v


def stack(weights, h):
    return lax.scan(lambda h, w: (layer(h, w), None), h, weights)[0]


def reference(x, dy, w_gate, w_up, w_down, m_w_gate, m_w_up, m_w_down, v_w_gate, v_w_up, v_w_down):
    weights = dict(zip(NAMES, (w_gate, w_up, w_down), strict=True))

    def take(so_far, sequence):
        h, by_y = sequence
        _, back = jax.vjp(lambda w: stack(w, h), weights)
        return jax.tree.map(lambda total, term: total + term.astype(jnp.float32), so_far, back(by_y)[0]), None

    none_yet = {name: jnp.zeros(w.shape, jnp.float32) for name, w in weights.items()}
    by_weights, _ = lax.scan(take, none_yet, (x, dy))
    gradients = [by_weights[name].astype(jnp.bfloat16).astype(jnp.float32) for name in NAMES]
    new = [
        adamw(w.astype(jnp.float32), m, v, g)
        for w, m, v, g in zip((w_gate, w_up, w_down), (m_w_gate, m_w_up, m_w_down), (v_w_gate, v_w_up, v_w_down), gradients, strict=True)
    ]
    return tuple(one[which] for which in range(3) for one in new)
```

```python
import functools

import jax
import jax.numpy as jnp
from jax import lax
from jax.experimental import pallas as pl
from jax.experimental.pallas import tpu as pltpu
from jax.sharding import PartitionSpec as P

TM = 512
FS = 256
F32, BF16 = jnp.float32, jnp.bfloat16
VMEM_LIMIT = 67_000_000


def dot(a, b):
    return jnp.dot(a, b, preferred_element_type=F32)


def dot_t(a, b):
    return lax.dot_general(a, b, (((1,), (1,)), ((), ())), preferred_element_type=F32)


def scale_of(wide):
    return lax.rsqrt(jnp.mean(wide * wide, -1, keepdims=True) + 1e-6)


def normed(h):
    wide = h.astype(F32)
    return (wide * scale_of(wide)).astype(BF16)


def sigmoid(g):
    return 0.5 * jnp.tanh(0.5 * g) + 0.5


def forward_tile(x, w_gu, w_d, act_ref):
    slices = w_gu.shape[0]
    a = normed(x)
    for j in range(slices):
        gu = dot(a, w_gu[j])
        g, u = gu[:, :FS], gu[:, FS:]
        act_ref[:, j * FS : (j + 1) * FS] = (g * sigmoid(g) * u).astype(BF16)
    y = dot(act_ref[...], w_d[...].reshape(slices * FS, -1)).astype(BF16)
    return a, (x.astype(F32) + y.astype(F32)).astype(BF16)


def slice_tile(a, a_t, dy, dy_t, wgu, wd, acc_ref):
    gu = dot(a, wgu)
    g, u = gu[:, :FS], gu[:, FS:]
    dact = dot_t(dy, wd).astype(BF16).astype(F32)
    s = sigmoid(g)
    silu = g * s
    act = (silu * u).astype(BF16)
    du = (dact * silu).astype(BF16)
    dg = (dact * u * (s + silu * (1.0 - s))).astype(BF16)
    acc_ref[:, 2 * FS :] += dot(dy_t, act)
    dgu = jnp.concatenate([dg, du], axis=1)
    acc_ref[:, : 2 * FS] += dot(a_t, dgu)
    return dgu


def norm_back(da, h, dy):
    d = h.shape[-1]
    da = da.astype(BF16).astype(F32)
    h = h.astype(F32)
    r = scale_of(h)
    along = jnp.sum(da * h, -1, keepdims=True)
    dh = (da * r - h * (along * r * r * r * (1.0 / d))).astype(BF16)
    return (dy.astype(F32) + dh.astype(F32)).astype(BF16)


class Ring:
    def __init__(self, n, rows, own, got, out, g_hbm, send, recv, out_sem):
        self.n, self.half, self.rows = n, n // 2, rows // n
        self.own, self.got, self.out, self.g_hbm = own, got, out, g_hbm
        self.send, self.recv, self.out_sem = send, recv, out_sem
        self.me = lax.axis_index("dp")
        self.to = ({"dp": lax.rem(self.me + n - 1, n)}, {"dp": lax.rem(self.me + 1, n)})

    def part(self, offset, way, halved):
        owner = lax.rem(self.me + offset + self.n, self.n)
        size = self.rows // 2 if halved else self.rows
        start = owner * self.rows + (size if halved and way == 1 else 0)
        return pl.ds(pl.multiple_of(start, size), size)

    def landing(self, way, halved):
        size = self.rows // 2 if halved else self.rows
        return pl.ds(size if halved and way == 1 else 0, size)

    def sign(self, way):
        return 1 if way == 0 else -1

    def copy(self, slot, k, way):
        h = self.half
        if k < h:
            halved = k == 0
            rows = self.part(self.sign(way) * (k - h), way, halved)
            src = self.own.at[slot, rows]
            dst = self.got.at[slot, k, way, self.landing(way, halved)]
        else:
            rows = self.part(self.sign(way) * (k - h), way, k == 2 * h - 1)
            src = dst = self.out.at[slot, rows]
        return pltpu.make_async_remote_copy(
            src_ref=src,
            dst_ref=dst,
            send_sem=self.send.at[slot, k, way],
            recv_sem=self.recv.at[slot, k, way],
            device_id=self.to[way],
            device_id_type=pl.DeviceIdType.MESH,
        )

    def write_out(self, slot, t):
        return pltpu.make_async_copy(self.out.at[slot], self.g_hbm.at[t], self.out_sem.at[slot])

    def event(self, slot, t, k):
        h = self.half
        if 0 < k <= 2 * h:
            for way in (0, 1):
                self.copy(slot, k - 1, way).wait_recv()
        if 0 < k < h:
            for way in (0, 1):
                rows = self.part(self.sign(way) * (k - h), way, k == 1)
                came = self.got[slot, k - 1, way, self.landing(way, k == 1)].astype(F32)
                self.own[slot, rows] = (self.own[slot, rows].astype(F32) + came).astype(BF16)
        if k == h:
            rows = self.part(0, 0, False)
            total = self.own[slot, rows].astype(F32) + self.got[slot, h - 1, 0].astype(F32) + self.got[slot, h - 1, 1].astype(F32)
            self.out[slot, rows] = total.astype(BF16)
        if k < 2 * h:
            for way in (0, 1):
                self.copy(slot, k, way).start()
        if k == 2 * h:
            self.write_out(slot, t).start()
            for sent in range(2 * h):
                for way in (0, 1):
                    self.copy(slot, sent, way).wait_send()
        if k == 2 * h + 1:
            self.write_out(slot, t).wait()


SLOTS = 4
EVERY = 3


def train_kernel(n, x, dy, wg, wu, wd, g_out, w_gu, w_d, a1, a2, at, dyv, dyt, h1, da, act, acc, own, got, out, sem, wsem, send, recv, out_sem):
    layers, slices = w_gu.shape[:2]
    tiles = x.shape[0]
    total = layers * slices
    barrier = pltpu.get_barrier_semaphore()
    ring = Ring(n, acc.shape[0], own, got, out, g_out, send, recv, out_sem)
    for device in ring.to:
        pl.semaphore_signal(barrier, inc=1, device_id=device, device_id_type=pl.DeviceIdType.MESH)

    def weights(l):
        return [
            copy
            for j in range(slices)
            for copy in (
                pltpu.make_async_copy(wg.at[l, :, pl.ds(j * FS, FS)], w_gu.at[l, j, :, pl.ds(0, FS)], wsem.at[l, j, 0]),
                pltpu.make_async_copy(wu.at[l, :, pl.ds(j * FS, FS)], w_gu.at[l, j, :, pl.ds(FS, FS)], wsem.at[l, j, 1]),
                pltpu.make_async_copy(wd.at[l, pl.ds(j * FS, FS), :], w_d.at[l, j], wsem.at[l, j, 2]),
            )
        ]

    def state(m):
        return pltpu.make_async_copy(x.at[m], a1.at[m], sem.at[m])

    all_dy = pltpu.make_async_copy(dy, dyv, sem.at[tiles])
    state(0).start()
    for c in weights(0):
        c.start()
    for m in range(1, tiles):
        state(m).start()
    all_dy.start()
    for c in weights(1):
        c.start()
    for c in weights(0):
        c.wait()

    def forward(m, _):
        state(m).wait()
        a, h = forward_tile(a1[m], w_gu.at[0], w_d.at[0], act)
        a1[m] = a
        h1[m] = h
        a = normed(h)
        a2[m] = a
        at[m] = a.T
        da[m] = jnp.zeros(da.shape[1:], F32)

        @pl.when(m == 0)
        def _():
            all_dy.wait()

        dyt[m] = dyv[m].T
        return 0

    lax.fori_loop(0, tiles, forward, 0)
    for c in weights(1):
        c.wait()
    pl.semaphore_wait(barrier, 2)

    offsets = [EVERY * k for k in range(2 * ring.half + 2)]

    def events(s, m):
        for k in reversed(range(len(offsets))):
            ago, at_tile = divmod(offsets[k], tiles)
            t = s - 1 - ago

            @pl.when((m == at_tile) & (t >= 0) & (t < total))
            def _():
                ring.event(lax.rem(t, SLOTS), t, k)

    def one_slice(s, _):
        second = s < slices
        l = jnp.where(second, 1, 0)
        j = jnp.where(second, s, s - slices)
        acc[...] = jnp.zeros_like(acc)

        def one_tile(m, _):
            events(s, m)

            @pl.when(s == slices)
            def _():
                back = norm_back(da[m], h1[m], dyv[m])
                dyv[m] = back
                dyt[m] = back.T
                a = a1[m]
                a2[m] = a
                at[m] = a.T

            dgu = slice_tile(a2[m], at[m], dyv[m], dyt[m], w_gu[l, j], w_d[l, j], acc)

            @pl.when(second)
            def _():
                da[m] += dot_t(dgu, w_gu[l, j])

            return 0

        lax.fori_loop(0, tiles, one_tile, 0)
        own[lax.rem(s, SLOTS)] = acc[...].astype(BF16)
        return 0

    lax.fori_loop(0, total, one_slice, 0)

    def drain(s, _):
        def one(m, _):
            events(s, m)
            return 0

        return lax.fori_loop(0, tiles, one, 0)

    lax.fori_loop(total, total + 1 + offsets[-1] // tiles, drain, 0)


def adam_math(w, m, v, g):
    m = 0.9 * m + 0.1 * g
    v = 0.95 * v + 0.05 * g * g
    step = m * lax.rsqrt(v + 1e-8) + 0.1 * w
    return (w - 0.02 * step).astype(BF16), m, v


def adam_kernel(g_ref, *refs):
    ins, outs = refs[:9], refs[9:]
    for i in range(3):
        g = g_ref[0, :, i * FS : (i + 1) * FS].astype(F32)
        if i == 2:
            g = g.T
        w, m, v = (ins[k * 3 + i] for k in range(3))
        new = adam_math(w[0].astype(F32), m[0], v[0], g)
        for k in range(3):
            outs[k * 3 + i][0] = new[k]


def adam(g, arrays):
    layers, d, ff = arrays[0].shape
    slices = ff // FS
    wide = pl.BlockSpec((1, d, FS), lambda s: (layers - 1 - s // slices, 0, s % slices))
    tall = pl.BlockSpec((1, FS, d), lambda s: (layers - 1 - s // slices, s % slices, 0))
    specs = [wide, wide, tall] * 3
    return pl.pallas_call(
        adam_kernel,
        grid=(layers * slices,),
        in_specs=[pl.BlockSpec((1, d, 3 * FS), lambda s: (s, 0, 0))] + specs,
        out_specs=specs,
        out_shape=[jax.ShapeDtypeStruct(a.shape, a.dtype) for a in arrays],
        compiler_params=pltpu.CompilerParams(vmem_limit_bytes=60_000_000),
        cost_estimate=pl.CostEstimate(flops=10**9, bytes_accessed=120 * 10**6, transcendentals=0),
    )(g, *arrays)


def solution(mesh):
    n = mesh.shape["dp"]

    def step(x, dy, *arrays):
        wg, wu, wd = arrays[:3]
        tokens, d = x.shape[1:]
        layers, _, ff = wg.shape
        tiles, slices = tokens // TM, ff // FS
        x, dy = x.reshape(tiles, TM, d), dy.reshape(tiles, TM, d)
        hbm = pl.BlockSpec(memory_space=pl.ANY)
        half = n // 2
        mm = 2 * tokens * d * ff
        g = pl.pallas_call(
            functools.partial(train_kernel, n),
            in_specs=[hbm] * 5,
            out_specs=hbm,
            out_shape=jax.ShapeDtypeStruct((layers * slices, d, 3 * FS), BF16),
            scratch_shapes=[
                pltpu.VMEM((layers, slices, d, 2 * FS), BF16),
                pltpu.VMEM((layers, slices, FS, d), BF16),
                pltpu.VMEM((tiles, TM, d), BF16),
                pltpu.VMEM((tiles, TM, d), BF16),
                pltpu.VMEM((tiles, d, TM), BF16),
                pltpu.VMEM((tiles, TM, d), BF16),
                pltpu.VMEM((tiles, d, TM), BF16),
                pltpu.VMEM((tiles, TM, d), BF16),
                pltpu.VMEM((tiles, TM, d), F32),
                pltpu.VMEM((TM, ff), BF16),
                pltpu.VMEM((d, 3 * FS), F32),
                pltpu.VMEM((SLOTS, d, 3 * FS), BF16),
                pltpu.VMEM((SLOTS, half, 2, d // n, 3 * FS), BF16),
                pltpu.VMEM((SLOTS, d, 3 * FS), BF16),
                pltpu.SemaphoreType.DMA((tiles + 1,)),
                pltpu.SemaphoreType.DMA((layers, slices, 3)),
                pltpu.SemaphoreType.DMA((SLOTS, 2 * half, 2)),
                pltpu.SemaphoreType.DMA((SLOTS, 2 * half, 2)),
                pltpu.SemaphoreType.DMA((SLOTS,)),
            ],
            compiler_params=pltpu.CompilerParams(vmem_limit_bytes=VMEM_LIMIT, collective_id=0, has_side_effects=True),
            cost_estimate=pl.CostEstimate(flops=17 * mm, bytes_accessed=30 * 10**6, transcendentals=0),
        )(x, dy, wg, wu, wd)
        return tuple(adam(g, arrays))

    return jax.shard_map(
        step,
        mesh=mesh,
        in_specs=(P(("rep", "dp"), None, None),) * 2 + (P(None, None, None),) * 9,
        out_specs=(P("rep", None, None),) * 9,
        check_vma=False,
    )
```

```python
import functools

import jax
import jax.numpy as jnp
from jax import lax
from jax.experimental import pallas as pl
from jax.experimental.pallas import tpu as pltpu
from jax.sharding import PartitionSpec as P


TM = 512
FS = 256
F32, BF16 = jnp.float32, jnp.bfloat16
VMEM_LIMIT = 67_000_000


def dot(a, b):
    return jnp.dot(a, b, preferred_element_type=F32)


def dot_t(a, b):
    return lax.dot_general(a, b, (((1,), (1,)), ((), ())), preferred_element_type=F32)


def scale_of(wide):
    return lax.rsqrt(jnp.mean(wide * wide, -1, keepdims=True) + 1e-6)


def normed(h):
    wide = h.astype(F32)
    return (wide * scale_of(wide)).astype(BF16)


def sigmoid(g):
    return 0.5 * jnp.tanh(0.5 * g) + 0.5


def forward_tile(x, w_gu, w_d, act_ref):
    slices = w_gu.shape[0]
    a = normed(x)
    for j in range(slices):
        gu = dot(a, w_gu[j])
        g, u = gu[:, :FS], gu[:, FS:]
        act_ref[:, j * FS : (j + 1) * FS] = (g * sigmoid(g) * u).astype(BF16)
    y = dot(act_ref[...], w_d[...].reshape(slices * FS, -1)).astype(BF16)
    return a, (x.astype(F32) + y.astype(F32)).astype(BF16)


def slice_tile(a, a_t, dy, dy_t, wgu, wd, acc_ref):
    gu = dot(a, wgu)
    g, u = gu[:, :FS], gu[:, FS:]
    dact = dot_t(dy, wd).astype(BF16).astype(F32)
    s = sigmoid(g)
    silu = g * s
    act = (silu * u).astype(BF16)
    du = (dact * silu).astype(BF16)
    dg = (dact * u * (s + silu * (1.0 - s))).astype(BF16)
    acc_ref[:, 2 * FS :] += dot(dy_t, act)
    dgu = jnp.concatenate([dg, du], axis=1)
    acc_ref[:, : 2 * FS] += dot(a_t, dgu)
    return dgu


def norm_back(da, h, dy):
    d = h.shape[-1]
    da = da.astype(BF16).astype(F32)
    h = h.astype(F32)
    r = scale_of(h)
    along = jnp.sum(da * h, -1, keepdims=True)
    dh = (da * r - h * (along * r * r * r * (1.0 / d))).astype(BF16)
    return (dy.astype(F32) + dh.astype(F32)).astype(BF16)


class Ring:
    def __init__(self, n, own, got, out, sums, far, send, recv, out_sem):
        self.n, self.half, self.rows = n, n // 2, own.shape[2]
        self.kept = self.half - 2
        self.sends = self.half + self.kept
        self.own, self.got, self.out, self.sums, self.far = own, got, out, sums, far
        self.send, self.recv, self.out_sem = send, recv, out_sem
        self.me = lax.axis_index("dp")
        self.to = ({"dp": lax.rem(self.me + n - 1, n)}, {"dp": lax.rem(self.me + 1, n)})

    def chunk(self, way, offset):
        return lax.rem(self.me + (offset if way == 0 else -offset) + self.n, self.n)

    def part(self, way, halved):
        size = self.rows // 2 if halved else self.rows
        return pl.ds(size if halved and way == 1 else 0, size)

    def copy(self, slot, k, way):
        h = self.half
        rows = self.part(way, k == 0)
        chunk = self.chunk(way, k - h)
        if k < h:
            src = self.own.at[slot, chunk, rows]
            dst = self.got.at[slot, k, way, rows]
        else:
            src = dst = self.out.at[slot, chunk, rows]
        return pltpu.make_async_remote_copy(
            src_ref=src,
            dst_ref=dst,
            send_sem=self.send.at[slot, k, way],
            recv_sem=self.recv.at[slot, k, way],
            device_id=self.to[way],
            device_id_type=pl.DeviceIdType.MESH,
        )

    def write_out(self, slot, t):
        copies = []
        for offset in range(-self.kept, self.kept + 1):
            chunk = self.chunk(0, offset)
            copies.append((self.out.at[slot, chunk], self.sums.at[t, chunk]))
        for way in (0, 1):
            chunk = self.chunk(way, self.kept)
            for part in (0, 1):
                copies.append((self.out.at[slot, chunk, self.part(part, True)], self.far[2 * way + part].at[t]))
        return [pltpu.make_async_copy(a, b, self.out_sem.at[slot, i]) for i, (a, b) in enumerate(copies)]

    def event(self, slot, t, k):
        h = self.half
        if 0 < k <= self.sends:
            for way in (0, 1):
                self.copy(slot, k - 1, way).wait_recv()
        if 0 < k < h:
            for way in (0, 1):
                rows, chunk = self.part(way, k == 1), self.chunk(way, k - h)
                came = self.got[slot, k - 1, way, rows].astype(F32)
                self.own[slot, chunk, rows] = (self.own[slot, chunk, rows].astype(F32) + came).astype(BF16)
        if k == h:
            total = self.own[slot, self.me].astype(F32) + self.got[slot, h - 1, 0].astype(F32) + self.got[slot, h - 1, 1].astype(F32)
            self.out[slot, self.me] = total.astype(BF16)
        if k < self.sends:
            for way in (0, 1):
                self.copy(slot, k, way).start()
        if k == self.sends:
            for copy in self.write_out(slot, t):
                copy.start()
            for sent in range(self.sends):
                for way in (0, 1):
                    self.copy(slot, sent, way).wait_send()
        if k == self.sends + 1:
            for copy in self.write_out(slot, t):
                copy.wait()


SLOTS = 4
EVERY = 5


def train_kernel(n, x, dy, wg, wu, wd, sums, far0, far1, far2, far3, w_gu, w_d, a1, a2, at, dyv, dyt, h1, da, act, acc, own, got, out, sem, wsem, send, recv, out_sem):
    layers, slices = w_gu.shape[:2]
    tiles = x.shape[0]
    total = layers * slices
    barrier = pltpu.get_barrier_semaphore()
    ring = Ring(n, own, got, out, sums, (far0, far1, far2, far3), send, recv, out_sem)
    for device in ring.to:
        pl.semaphore_signal(barrier, inc=1, device_id=device, device_id_type=pl.DeviceIdType.MESH)

    def weights(l):
        return [
            copy
            for j in range(slices)
            for copy in (
                pltpu.make_async_copy(wg.at[l, :, pl.ds(j * FS, FS)], w_gu.at[l, j, :, pl.ds(0, FS)], wsem.at[l, j, 0]),
                pltpu.make_async_copy(wu.at[l, :, pl.ds(j * FS, FS)], w_gu.at[l, j, :, pl.ds(FS, FS)], wsem.at[l, j, 1]),
                pltpu.make_async_copy(wd.at[l, pl.ds(j * FS, FS), :], w_d.at[l, j], wsem.at[l, j, 2]),
            )
        ]

    def state(m):
        return pltpu.make_async_copy(x.at[m], a1.at[m], sem.at[m])

    all_dy = pltpu.make_async_copy(dy, dyv, sem.at[tiles])
    state(0).start()
    for c in weights(0):
        c.start()
    for m in range(1, tiles):
        state(m).start()
    all_dy.start()
    for c in weights(1):
        c.start()
    for c in weights(0):
        c.wait()

    def forward(m, _):
        state(m).wait()
        a, h = forward_tile(a1[m], w_gu.at[0], w_d.at[0], act)
        a1[m] = a
        h1[m] = h
        a = normed(h)
        a2[m] = a
        at[m] = a.T
        da[m] = jnp.zeros(da.shape[1:], F32)

        @pl.when(m == 0)
        def _():
            all_dy.wait()

        dyt[m] = dyv[m].T
        return 0

    lax.fori_loop(0, tiles, forward, 0)
    for c in weights(1):
        c.wait()
    pl.semaphore_wait(barrier, 2)

    offsets = [EVERY * k for k in range(ring.sends + 1)] + [EVERY * ring.sends + 3]

    def events(s, m):
        for k in reversed(range(len(offsets))):
            ago, at_tile = divmod(offsets[k], tiles)
            t = s - 1 - ago

            @pl.when((m == at_tile) & (t >= 0) & (t < total))
            def _():
                ring.event(lax.rem(t, SLOTS), t, k)

    def one_slice(s, _):
        second = s < slices
        l = jnp.where(second, 1, 0)
        j = jnp.where(second, s, s - slices)
        acc[...] = jnp.zeros_like(acc)

        def one_tile(m, _):
            events(s, m)

            @pl.when(s == slices)
            def _():
                back = norm_back(da[m], h1[m], dyv[m])
                dyv[m] = back
                dyt[m] = back.T
                a = a1[m]
                a2[m] = a
                at[m] = a.T

            dgu = slice_tile(a2[m], at[m], dyv[m], dyt[m], w_gu[l, j], w_d[l, j], acc)

            @pl.when(second)
            def _():
                da[m] += dot_t(dgu, w_gu[l, j])

            return 0

        lax.fori_loop(0, tiles, one_tile, 0)
        slot = lax.rem(s, SLOTS)
        wide = acc.shape[0] // n
        own[slot, :, :wide] = acc[:, : 2 * FS].astype(BF16).reshape(n, wide, 2 * FS)
        own[slot, :, wide:] = acc[:, 2 * FS :].T.astype(BF16).reshape(n, FS // n, -1)
        return 0

    lax.fori_loop(0, total, one_slice, 0)

    def drain(s, _):
        def one(m, _):
            events(s, m)
            return 0

        return lax.fori_loop(0, tiles, one, 0)

    lax.fori_loop(total, total + 1 + offsets[-1] // tiles, drain, 0)


def adam_math(w, m, v, g):
    m = 0.9 * m + 0.1 * g
    v = 0.95 * v + 0.05 * g * g
    step = m * lax.rsqrt(v + 1e-8) + 0.1 * w
    return (w - 0.02 * step).astype(BF16), m, v


def adam_kernel(halves, where, *refs):
    gs, ins, outs = refs[:halves], refs[halves : halves + 9], refs[-9:]
    slices = gs[0].shape[0]
    wide = ins[0].shape[2]
    for j in range(slices):
        g = [r[j].reshape(r.shape[-2:]) for r in gs]
        g = (g[0] if halves == 1 else jnp.concatenate(g, axis=0)).astype(F32)
        columns = slice(j * FS, (j + 1) * FS)
        for i, here in ((0, (0, 0, slice(None), columns)), (1, (0, 0, slice(None), columns)), (2, (0, j, 0))):
            part = (g[:wide, :FS], g[:wide, FS:], g[wide:])[i]
            w, m, v = (ins[k * 3 + i][here] for k in range(3))
            new = adam_math(w.astype(F32), m, v, part)
            for k in range(3):
                outs[k * 3 + i][here] = new[k]


def adam(n, offsets, gs, g_spec, arrays, so_far):
    layers = arrays[0].shape[0]
    slices = arrays[2].shape[1]
    extra = [] if so_far is None else list(so_far)
    where = lax.axis_index("dp").astype(jnp.int32).reshape(1)
    step = offsets[1] - offsets[0] if len(offsets) > 1 else 1

    def chunk(o, where):
        return lax.rem(where[0] + o * step + (offsets[0] + n), n)

    wide = pl.BlockSpec((1, 1) + arrays[0].shape[2:], lambda l, o, where: (l, chunk(o, where), 0, 0))
    tall = pl.BlockSpec((1, slices, 1) + arrays[2].shape[3:], lambda l, o, where: (l, 0, chunk(o, where), 0, 0))
    specs = [wide, wide, tall] * 3
    size = sum(a.size * a.dtype.itemsize for a in arrays) * 2 * len(offsets) // n
    return pl.pallas_call(
        functools.partial(adam_kernel, len(gs)),
        grid_spec=pltpu.PrefetchScalarGridSpec(
            num_scalar_prefetch=1,
            grid=(layers, len(offsets)),
            in_specs=[g_spec(chunk)] * len(gs) + specs + [pl.BlockSpec(memory_space=pl.ANY)] * len(extra),
            out_specs=specs,
        ),
        out_shape=[jax.ShapeDtypeStruct(a.shape, a.dtype) for a in arrays],
        input_output_aliases={1 + len(gs) + 9 + i: i for i in range(len(extra))},
        compiler_params=pltpu.CompilerParams(vmem_limit_bytes=60_000_000),
        cost_estimate=pl.CostEstimate(flops=40 * size, bytes_accessed=size, transcendentals=0),
    )(where, *gs, *arrays, *extra)


def solution(mesh):
    n = mesh.shape["dp"]

    def step(x, dy, *arrays):
        wg, wu, wd = arrays[:3]
        tokens, d = x.shape[1:]
        layers, _, ff = wg.shape
        tiles, slices = tokens // TM, ff // FS
        x, dy = x.reshape(tiles, TM, d), dy.reshape(tiles, TM, d)
        hbm = pl.BlockSpec(memory_space=pl.ANY)
        half, rows = n // 2, (d + FS) // n
        mm = 2 * tokens * d * ff
        sums, *far = pl.pallas_call(
            functools.partial(train_kernel, n),
            in_specs=[hbm] * 5,
            out_specs=[hbm] * 5,
            out_shape=[jax.ShapeDtypeStruct((layers * slices, n, rows, d), BF16)]
            + [jax.ShapeDtypeStruct((layers * slices, rows // 2, d), BF16)] * 4,
            scratch_shapes=[
                pltpu.VMEM((layers, slices, d, 2 * FS), BF16),
                pltpu.VMEM((layers, slices, FS, d), BF16),
                pltpu.VMEM((tiles, TM, d), BF16),
                pltpu.VMEM((tiles, TM, d), BF16),
                pltpu.VMEM((tiles, d, TM), BF16),
                pltpu.VMEM((tiles, TM, d), BF16),
                pltpu.VMEM((tiles, d, TM), BF16),
                pltpu.VMEM((tiles, TM, d), BF16),
                pltpu.VMEM((tiles, TM, d), F32),
                pltpu.VMEM((TM, ff), BF16),
                pltpu.VMEM((d, 3 * FS), F32),
                pltpu.VMEM((SLOTS, n, rows, d), BF16),
                pltpu.VMEM((SLOTS, half, 2, rows, d), BF16),
                pltpu.VMEM((SLOTS, n, rows, d), BF16),
                pltpu.SemaphoreType.DMA((tiles + 1,)),
                pltpu.SemaphoreType.DMA((layers, slices, 3)),
                pltpu.SemaphoreType.DMA((SLOTS, 2 * half - 2, 2)),
                pltpu.SemaphoreType.DMA((SLOTS, 2 * half - 2, 2)),
                pltpu.SemaphoreType.DMA((SLOTS, n + 1)),
            ],
            compiler_params=pltpu.CompilerParams(vmem_limit_bytes=VMEM_LIMIT, collective_id=0, has_side_effects=True),
            cost_estimate=pl.CostEstimate(flops=17 * mm, bytes_accessed=30 * 10**6, transcendentals=0),
        )(x, dy, wg, wu, wd)
        chunks = [a.reshape(layers, n, d // n, ff) if a.shape[1] == d else a.reshape(layers, slices, n, FS // n, d) for a in arrays]
        left = [(i, (i + n - 1) % n) for i in range(n)]
        right = [(i, (i + 1) % n) for i in range(n)]

        def whole(chunk):
            return pl.BlockSpec((slices, 1, rows, d), lambda l, o, where: (layers - 1 - l, chunk(o, where), 0, 0))

        def halves(chunk):
            return pl.BlockSpec((slices, rows // 2, d), lambda l, o, where: (layers - 1 - l, 0, 0))

        near = []
        for i, way in enumerate((left, left, right, right)):
            near.append(lax.ppermute(far[i], "dp", way))
        new = adam(n, tuple(range(2 - half, half - 1)), [sums], whole, chunks, None)
        last = []
        for i, way in ((0, left), (3, right)):
            last.append(lax.ppermute(near[i], "dp", way))
        new = adam(n, (half - 1,), near[:2], halves, chunks, new)
        new = adam(n, (1 - half,), near[2:], halves, chunks, new)
        new = adam(n, (half,), last, halves, chunks, new)
        return tuple(o.reshape(a.shape) for o, a in zip(new, arrays))

    return jax.shard_map(
        step,
        mesh=mesh,
        in_specs=(P(("rep", "dp"), None, None),) * 2 + (P(None, None, None),) * 9,
        out_specs=(P("rep", None, None),) * 9,
        check_vma=False,
    )
```

```python
import functools

import jax
import jax.numpy as jnp
from jax import lax
from jax.experimental import pallas as pl
from jax.experimental.pallas import tpu as pltpu
from jax.sharding import PartitionSpec as P


TM = 512
FS = 256
F32, BF16 = jnp.float32, jnp.bfloat16
VMEM_LIMIT = 67_000_000


def dot(a, b):
    return jnp.dot(a, b, preferred_element_type=F32)


def dot_t(a, b):
    return lax.dot_general(a, b, (((1,), (1,)), ((), ())), preferred_element_type=F32)


def scale_of(wide):
    return lax.rsqrt(jnp.mean(wide * wide, -1, keepdims=True) + 1e-6)


def normed(h):
    wide = h.astype(F32)
    return (wide * scale_of(wide)).astype(BF16)


def sigmoid(g):
    return 0.5 * jnp.tanh(0.5 * g) + 0.5


def forward_first(h, w_gu, act_ref):
    a = normed(h)
    for j in range(w_gu.shape[0]):
        gu = dot(a, w_gu[j])
        g, u = gu[:, :FS], gu[:, FS:]
        act_ref[:, j * FS : (j + 1) * FS] = (g * sigmoid(g) * u).astype(BF16)
    return a


def forward_second(h, w_d, act_ref):
    slices = w_d.shape[0]
    y = dot(act_ref[...], w_d[...].reshape(slices * FS, -1)).astype(BF16)
    return (h.astype(F32) + y.astype(F32)).astype(BF16)


def slice_first(a, dy, wgu, wd, buf):
    gu = dot(a, wgu)
    dact = dot_t(dy, wd)
    g, u = gu[:, :FS], gu[:, FS:]
    dact = dact.astype(BF16).astype(F32)
    s = sigmoid(g)
    silu = g * s
    buf[:, 2 * FS : 3 * FS] = (silu * u).astype(BF16)
    buf[:, FS : 2 * FS] = (dact * silu).astype(BF16)
    buf[:, :FS] = (dact * u * (s + silu * (1.0 - s))).astype(BF16)


def slice_second(a_t, dy_t, buf, acc_gu, acc_d):
    acc_d[...] += dot(dy_t, buf[:, 2 * FS : 3 * FS])
    acc_gu[...] += dot(a_t, buf[:, : 2 * FS])


def norm_back(da, h, dy):
    d = h.shape[-1]
    da = da.astype(BF16).astype(F32)
    h = h.astype(F32)
    r = scale_of(h)
    along = jnp.sum(da * h, -1, keepdims=True)
    dh = (da * r - h * (along * r * r * r * (1.0 / d))).astype(BF16)
    return (dy.astype(F32) + dh.astype(F32)).astype(BF16)


class Ring:
    def __init__(self, n, own, got, out, sums, far, send, recv, out_sem):
        self.n, self.half, self.rows = n, n // 2, own.shape[2]
        self.kept = self.half - 2
        self.sends = self.half + self.kept
        self.own, self.got, self.out, self.sums, self.far = own, got, out, sums, far
        self.send, self.recv, self.out_sem = send, recv, out_sem
        self.me = lax.axis_index("dp")
        self.to = ({"dp": lax.rem(self.me + n - 1, n)}, {"dp": lax.rem(self.me + 1, n)})

    def chunk(self, way, offset):
        return lax.rem(self.me + (offset if way == 0 else -offset) + self.n, self.n)

    def part(self, way, halved):
        size = self.rows // 2 if halved else self.rows
        return pl.ds(size if halved and way == 1 else 0, size)

    def copy(self, slot, k, way):
        h = self.half
        rows = self.part(way, k == 0)
        chunk = self.chunk(way, k - h)
        if k < h:
            src = self.own.at[slot, chunk, rows]
            dst = self.got.at[slot, k, way, rows]
        else:
            src = dst = self.out.at[slot, chunk, rows]
        return pltpu.make_async_remote_copy(
            src_ref=src,
            dst_ref=dst,
            send_sem=self.send.at[slot, k, way],
            recv_sem=self.recv.at[slot, k, way],
            device_id=self.to[way],
            device_id_type=pl.DeviceIdType.MESH,
        )

    def write_out(self, slot, t):
        copies = []
        for offset in range(-self.kept, self.kept + 1):
            chunk = self.chunk(0, offset)
            copies.append((self.out.at[slot, chunk], self.sums.at[t, chunk]))
        for way in (0, 1):
            chunk = self.chunk(way, self.kept)
            for part in (0, 1):
                copies.append((self.out.at[slot, chunk, self.part(part, True)], self.far[2 * way + part].at[t]))
        return [pltpu.make_async_copy(a, b, self.out_sem.at[slot, i]) for i, (a, b) in enumerate(copies)]

    def event(self, slot, t, k):
        h = self.half
        if 0 < k <= self.sends:
            for way in (0, 1):
                self.copy(slot, k - 1, way).wait_recv()
        if 0 < k < h:
            for way in (0, 1):
                rows, chunk = self.part(way, k == 1), self.chunk(way, k - h)
                came = self.got[slot, k - 1, way, rows].astype(F32)
                self.own[slot, chunk, rows] = (self.own[slot, chunk, rows].astype(F32) + came).astype(BF16)
        if k == h:
            total = self.own[slot, self.me].astype(F32) + self.got[slot, h - 1, 0].astype(F32) + self.got[slot, h - 1, 1].astype(F32)
            self.out[slot, self.me] = total.astype(BF16)
        if k < self.sends:
            for way in (0, 1):
                self.copy(slot, k, way).start()
        if k == self.sends:
            for copy in self.write_out(slot, t):
                copy.start()
            for sent in range(self.sends):
                for way in (0, 1):
                    self.copy(slot, sent, way).wait_send()
        if k == self.sends + 1:
            for copy in self.write_out(slot, t):
                copy.wait()


SLOTS = 4
EVERY = 5


def train_kernel(n, x, dy, wg, wu, wd, sums, far0, far1, far2, far3, w_gu, w_d, a1, a2, at, dyv, dyt, h1, da, buf0, buf1, acc_gu, acc_d, own, got, out, sem, wsem, send, recv, out_sem):
    layers, slices = w_gu.shape[:2]
    tiles = x.shape[0]
    total = layers * slices
    barrier = pltpu.get_barrier_semaphore()
    ring = Ring(n, own, got, out, sums, (far0, far1, far2, far3), send, recv, out_sem)
    for device in ring.to:
        pl.semaphore_signal(barrier, inc=1, device_id=device, device_id_type=pl.DeviceIdType.MESH)

    def weights(l):
        return [
            copy
            for j in range(slices)
            for copy in (
                pltpu.make_async_copy(wg.at[l, :, pl.ds(j * FS, FS)], w_gu.at[l, j, :, pl.ds(0, FS)], wsem.at[l, j, 0]),
                pltpu.make_async_copy(wu.at[l, :, pl.ds(j * FS, FS)], w_gu.at[l, j, :, pl.ds(FS, FS)], wsem.at[l, j, 1]),
                pltpu.make_async_copy(wd.at[l, pl.ds(j * FS, FS), :], w_d.at[l, j], wsem.at[l, j, 2]),
            )
        ]

    def state(m):
        return pltpu.make_async_copy(x.at[m], h1.at[m], sem.at[m])

    all_dy = pltpu.make_async_copy(dy, dyv, sem.at[tiles])
    state(0).start()
    for c in weights(0):
        c.start()
    for m in range(1, tiles):
        state(m).start()
    all_dy.start()
    for c in weights(1):
        c.start()
    for c in weights(0):
        c.wait()

    def forward_a(m):
        a1[m] = forward_first(h1[m], w_gu.at[0], buf0)

    def forward_b(m):
        h = forward_second(h1[m], w_d.at[0], buf0)
        h1[m] = h
        a = normed(h)
        a2[m] = a
        at[m] = a.T
        dyt[m] = dyv[m].T
        da[m] = jnp.zeros(da.shape[1:], F32)

    def forward(m, _):
        state(m + 1).wait()
        forward_b(m)
        forward_a(m + 1)
        return 0

    state(0).wait()
    forward_a(0)
    all_dy.wait()
    lax.fori_loop(0, tiles - 1, forward, 0)
    forward_b(tiles - 1)
    for c in weights(1):
        c.wait()
    pl.semaphore_wait(barrier, 2)

    offsets = [1 + EVERY * k for k in range(ring.sends + 1)] + [EVERY * ring.sends + 4]

    def events(s, m):
        for k in reversed(range(len(offsets))):
            ago, at_tile = divmod(offsets[k], tiles)
            t = s - 1 - ago

            @pl.when((m == at_tile) & (t >= 0) & (t < total))
            def _():
                ring.event(lax.rem(t, SLOTS), t, k)

    def finish(s):
        slot = lax.rem(s, SLOTS)
        wide = acc_gu.shape[0] // n
        own[slot, :, :wide] = acc_gu[...].astype(BF16).reshape(n, wide, 2 * FS)
        own[slot, :, wide:] = acc_d[...].T.astype(BF16).reshape(n, FS // n, -1)
        acc_gu[...] = jnp.zeros_like(acc_gu)
        acc_d[...] = jnp.zeros_like(acc_d)

    def backward(l, first_s):
        second = l == layers - 1
        states = a2 if second else a1

        def turn(m):
            back = norm_back(da[m], h1[m], dyv[m])
            dyv[m] = back
            dyt[m] = back.T
            at[m] = a1[m].T

        def slice_a(m, j, buf):
            slice_first(states[m], dyv[m], w_gu[l, j], w_d[l, j], buf)

        def slice_b(m, j, buf):
            slice_second(at[m], dyt[m], buf, acc_gu, acc_d)
            if second:
                da[m] += dot_t(buf[:, : 2 * FS], w_gu[l, j])

        def one_slice(j, _):
            s = first_s + j

            def pair(i, _):
                m = 2 * i
                events(s, m)
                if not second:
                    @pl.when(j == 0)
                    def _():
                        turn(m)
                        turn(m + 1)

                slice_a(m, j, buf0)
                slice_b(lax.rem(m + tiles - 1, tiles), jnp.where(i == 0, lax.rem(j + slices - 1, slices), j), buf1)

                @pl.when((i == 0) & (j > 0))
                def _():
                    finish(s - 1)

                events(s, m + 1)
                slice_a(m + 1, j, buf1)
                slice_b(m, j, buf0)
                return 0

            return lax.fori_loop(0, tiles // 2, pair, 0)

        buf1[:, : 3 * FS] = jnp.zeros((TM, 3 * FS), BF16)
        lax.fori_loop(0, slices, one_slice, 0)
        slice_b(tiles - 1, slices - 1, buf1)
        finish(first_s + slices - 1)

    acc_gu[...] = jnp.zeros_like(acc_gu)
    acc_d[...] = jnp.zeros_like(acc_d)
    for l in reversed(range(layers)):
        backward(l, (layers - 1 - l) * slices)

    def drain(s, _):
        def one(m, _):
            events(s, m)
            return 0

        return lax.fori_loop(0, tiles, one, 0)

    lax.fori_loop(total, total + 1 + offsets[-1] // tiles, drain, 0)


def adam_math(w, m, v, g):
    m = 0.9 * m + 0.1 * g
    v = 0.95 * v + 0.05 * g * g
    step = m * lax.rsqrt(v + 1e-8) + 0.1 * w
    return (w - 0.02 * step).astype(BF16), m, v


def adam_kernel(halves, where, *refs):
    gs, ins, outs = refs[:halves], refs[halves : halves + 9], refs[-9:]
    slices = gs[0].shape[0]
    wide = ins[0].shape[2]
    for j in range(slices):
        g = [r[j].reshape(r.shape[-2:]) for r in gs]
        g = (g[0] if halves == 1 else jnp.concatenate(g, axis=0)).astype(F32)
        columns = slice(j * FS, (j + 1) * FS)
        for i, here in ((0, (0, 0, slice(None), columns)), (1, (0, 0, slice(None), columns)), (2, (0, j, 0))):
            part = (g[:wide, :FS], g[:wide, FS:], g[wide:])[i]
            w, m, v = (ins[k * 3 + i][here] for k in range(3))
            new = adam_math(w.astype(F32), m, v, part)
            for k in range(3):
                outs[k * 3 + i][here] = new[k]


def adam(n, offsets, gs, g_spec, arrays, so_far):
    layers = arrays[0].shape[0]
    slices = arrays[2].shape[1]
    extra = [] if so_far is None else list(so_far)
    where = lax.axis_index("dp").astype(jnp.int32).reshape(1)
    step = offsets[1] - offsets[0] if len(offsets) > 1 else 1

    def chunk(o, where):
        return lax.rem(where[0] + o * step + (offsets[0] + n), n)

    wide = pl.BlockSpec((1, 1) + arrays[0].shape[2:], lambda l, o, where: (l, chunk(o, where), 0, 0))
    tall = pl.BlockSpec((1, slices, 1) + arrays[2].shape[3:], lambda l, o, where: (l, 0, chunk(o, where), 0, 0))
    specs = [wide, wide, tall] * 3
    size = sum(a.size * a.dtype.itemsize for a in arrays) * 2 * len(offsets) // n
    return pl.pallas_call(
        functools.partial(adam_kernel, len(gs)),
        grid_spec=pltpu.PrefetchScalarGridSpec(
            num_scalar_prefetch=1,
            grid=(layers, len(offsets)),
            in_specs=[g_spec(chunk)] * len(gs) + specs + [pl.BlockSpec(memory_space=pl.ANY)] * len(extra),
            out_specs=specs,
        ),
        out_shape=[jax.ShapeDtypeStruct(a.shape, a.dtype) for a in arrays],
        input_output_aliases={1 + len(gs) + 9 + i: i for i in range(len(extra))},
        compiler_params=pltpu.CompilerParams(vmem_limit_bytes=60_000_000),
        cost_estimate=pl.CostEstimate(flops=40 * size, bytes_accessed=size, transcendentals=0),
    )(where, *gs, *arrays, *extra)


def solution(mesh):
    n = mesh.shape["dp"]

    def step(x, dy, *arrays):
        wg, wu, wd = arrays[:3]
        tokens, d = x.shape[1:]
        layers, _, ff = wg.shape
        tiles, slices = tokens // TM, ff // FS
        x, dy = x.reshape(tiles, TM, d), dy.reshape(tiles, TM, d)
        hbm = pl.BlockSpec(memory_space=pl.ANY)
        half, rows = n // 2, (d + FS) // n
        mm = 2 * tokens * d * ff
        sums, *far = pl.pallas_call(
            functools.partial(train_kernel, n),
            in_specs=[hbm] * 5,
            out_specs=[hbm] * 5,
            out_shape=[jax.ShapeDtypeStruct((layers * slices, n, rows, d), BF16)]
            + [jax.ShapeDtypeStruct((layers * slices, rows // 2, d), BF16)] * 4,
            scratch_shapes=[
                pltpu.VMEM((layers, slices, d, 2 * FS), BF16),
                pltpu.VMEM((layers, slices, FS, d), BF16),
                pltpu.VMEM((tiles, TM, d), BF16),
                pltpu.VMEM((tiles, TM, d), BF16),
                pltpu.VMEM((tiles, d, TM), BF16),
                pltpu.VMEM((tiles, TM, d), BF16),
                pltpu.VMEM((tiles, d, TM), BF16),
                pltpu.VMEM((tiles, TM, d), BF16),
                pltpu.VMEM((tiles, TM, d), F32),
                pltpu.VMEM((TM, ff), BF16),
                pltpu.VMEM((TM, 3 * FS), BF16),
                pltpu.VMEM((d, 2 * FS), F32),
                pltpu.VMEM((d, FS), F32),
                pltpu.VMEM((SLOTS, n, rows, d), BF16),
                pltpu.VMEM((SLOTS, half, 2, rows, d), BF16),
                pltpu.VMEM((SLOTS, n, rows, d), BF16),
                pltpu.SemaphoreType.DMA((tiles + 1,)),
                pltpu.SemaphoreType.DMA((layers, slices, 3)),
                pltpu.SemaphoreType.DMA((SLOTS, 2 * half - 2, 2)),
                pltpu.SemaphoreType.DMA((SLOTS, 2 * half - 2, 2)),
                pltpu.SemaphoreType.DMA((SLOTS, n + 1)),
            ],
            compiler_params=pltpu.CompilerParams(vmem_limit_bytes=VMEM_LIMIT, collective_id=0, has_side_effects=True),
            cost_estimate=pl.CostEstimate(flops=17 * mm, bytes_accessed=30 * 10**6, transcendentals=0),
        )(x, dy, wg, wu, wd)
        chunks = [a.reshape(layers, n, d // n, ff) if a.shape[1] == d else a.reshape(layers, slices, n, FS // n, d) for a in arrays]
        left = [(i, (i + n - 1) % n) for i in range(n)]
        right = [(i, (i + 1) % n) for i in range(n)]

        def whole(chunk):
            return pl.BlockSpec((slices, 1, rows, d), lambda l, o, where: (layers - 1 - l, chunk(o, where), 0, 0))

        def halves(chunk):
            return pl.BlockSpec((slices, rows // 2, d), lambda l, o, where: (layers - 1 - l, 0, 0))

        near = []
        for i, way in enumerate((left, left, right, right)):
            near.append(lax.ppermute(far[i], "dp", way))
        new = adam(n, tuple(range(2 - half, half - 1)), [sums], whole, chunks, None)
        last = []
        for i, way in ((0, left), (3, right)):
            last.append(lax.ppermute(near[i], "dp", way))
        new = adam(n, (half - 1,), near[:2], halves, chunks, new)
        new = adam(n, (1 - half,), near[2:], halves, chunks, new)
        new = adam(n, (half,), last, halves, chunks, new)
        return tuple(o.reshape(a.shape) for o, a in zip(new, arrays))

    return jax.shard_map(
        step,
        mesh=mesh,
        in_specs=(P(("rep", "dp"), None, None),) * 2 + (P(None, None, None),) * 9,
        out_specs=(P("rep", None, None),) * 9,
        check_vma=False,
    )
```

```python
import functools

import jax
import jax.numpy as jnp
from jax import lax
from jax.experimental import pallas as pl
from jax.experimental.pallas import tpu as pltpu
from jax.sharding import PartitionSpec as P


TM = 512
FS = 256
F32, BF16 = jnp.float32, jnp.bfloat16
VMEM_LIMIT = 67_000_000


def dot(a, b):
    return jnp.dot(a, b, preferred_element_type=F32)


def dot_t(a, b):
    return lax.dot_general(a, b, (((1,), (1,)), ((), ())), preferred_element_type=F32)


def scale_of(wide):
    return lax.rsqrt(jnp.mean(wide * wide, -1, keepdims=True) + 1e-6)


def normed(h):
    wide = h.astype(F32)
    return (wide * scale_of(wide)).astype(BF16)


def sigmoid(g):
    return 0.5 * jnp.tanh(0.5 * g) + 0.5


def forward_first(h, w_gu, act_ref, ready=lambda j: None):
    a = normed(h)
    for j in range(w_gu.shape[1] // (2 * FS)):
        ready(j)
        gu = dot(a, w_gu[:, 2 * j * FS : 2 * (j + 1) * FS])
        g, u = gu[:, :FS], gu[:, FS:]
        act_ref[:, j * FS : (j + 1) * FS] = (g * sigmoid(g) * u).astype(BF16)
    return a


def forward_second(h, w_d, act_ref):
    slices = w_d.shape[0]
    y = dot(act_ref[...], w_d[...].reshape(slices * FS, -1)).astype(BF16)
    return (h.astype(F32) + y.astype(F32)).astype(BF16)


def slice_first(a, dy, wgu, wd, buf):
    gu = dot(a, wgu)
    dact = dot_t(dy, wd)
    g, u = gu[:, :FS], gu[:, FS:]
    dact = dact.astype(BF16).astype(F32)
    s = sigmoid(g)
    silu = g * s
    buf[:, 2 * FS : 3 * FS] = (silu * u).astype(BF16)
    buf[:, FS : 2 * FS] = (dact * silu).astype(BF16)
    buf[:, :FS] = (dact * u * (s + silu * (1.0 - s))).astype(BF16)


def slice_second(a_t, dy_t, buf, acc_gu, acc_d):
    acc_d[...] += dot(dy_t, buf[:, 2 * FS : 3 * FS])
    acc_gu[...] += dot(a_t, buf[:, : 2 * FS])


def norm_back(da, h, dy):
    d = h.shape[-1]
    da = da.astype(BF16).astype(F32)
    h = h.astype(F32)
    r = scale_of(h)
    along = jnp.sum(da * h, -1, keepdims=True)
    dh = (da * r - h * (along * r * r * r * (1.0 / d))).astype(BF16)
    return (dy.astype(F32) + dh.astype(F32)).astype(BF16)


class Ring:
    def __init__(self, n, own, got, out, sums, far, send, recv, out_sem):
        self.n, self.half, self.rows = n, n // 2, own.shape[2]
        self.kept = self.half - 2
        self.sends = self.half + self.kept
        self.own, self.got, self.out, self.sums, self.far = own, got, out, sums, far
        self.send, self.recv, self.out_sem = send, recv, out_sem
        self.me = lax.axis_index("dp")
        self.to = ({"dp": lax.rem(self.me + n - 1, n)}, {"dp": lax.rem(self.me + 1, n)})

    def chunk(self, way, offset):
        return lax.rem(self.me + (offset if way == 0 else -offset) + self.n, self.n)

    def part(self, way, halved):
        size = self.rows // 2 if halved else self.rows
        return pl.ds(size if halved and way == 1 else 0, size)

    def copy(self, slot, k, way):
        h = self.half
        rows = self.part(way, k == 0)
        chunk = self.chunk(way, k - h)
        if k < h:
            src = self.own.at[slot, chunk, rows]
            dst = self.got.at[slot, k, way, rows]
        else:
            src = dst = self.out.at[slot, chunk, rows]
        return pltpu.make_async_remote_copy(
            src_ref=src,
            dst_ref=dst,
            send_sem=self.send.at[slot, k, way],
            recv_sem=self.recv.at[slot, k, way],
            device_id=self.to[way],
            device_id_type=pl.DeviceIdType.MESH,
        )

    def write_out(self, slot, t):
        copies = []
        for offset in range(-self.kept, self.kept + 1):
            chunk = self.chunk(0, offset)
            copies.append((self.out.at[slot, chunk], self.sums.at[t, chunk]))
        for way in (0, 1):
            chunk = self.chunk(way, self.kept)
            for part in (0, 1):
                copies.append((self.out.at[slot, chunk, self.part(part, True)], self.far[2 * way + part].at[t]))
        return [pltpu.make_async_copy(a, b, self.out_sem.at[slot, i]) for i, (a, b) in enumerate(copies)]

    def event(self, slot, t, k):
        h = self.half
        if 0 < k <= self.sends:
            for way in (0, 1):
                self.copy(slot, k - 1, way).wait_recv()
        if 0 < k < h:
            for way in (0, 1):
                rows, chunk = self.part(way, k == 1), self.chunk(way, k - h)
                came = self.got[slot, k - 1, way, rows].astype(F32)
                self.own[slot, chunk, rows] = (self.own[slot, chunk, rows].astype(F32) + came).astype(BF16)
        if k == h:
            total = self.own[slot, self.me].astype(F32) + self.got[slot, h - 1, 0].astype(F32) + self.got[slot, h - 1, 1].astype(F32)
            self.out[slot, self.me] = total.astype(BF16)
        if k < self.sends:
            for way in (0, 1):
                self.copy(slot, k, way).start()
        if k == self.sends:
            for copy in self.write_out(slot, t):
                copy.start()
        for sent in range(max(k - 2, 0), k - 1) if k < self.sends else range(k - 2, k) if k == self.sends else ():
            for way in (0, 1):
                self.copy(slot, sent, way).wait_send()
        if k == self.sends + 1:
            for copy in self.write_out(slot, t):
                copy.wait()


SLOTS = 4
EVERY = 6
EARLY, SOONER = 2, 5


def train_kernel(n, x, dy, wg, wu, wd, sums, far0, far1, far2, far3, dgu, w_gu, w_d, a1, a2, at, dyv, dyt, h1, pulled, act, buf0, buf1,
                 acc_gu, acc_d, own, got, out, sem, wsem, push_sem, pull_sem, send, recv, out_sem):
    layers, slices = w_d.shape[:2]
    tiles = x.shape[0]
    total = layers * slices
    barrier = pltpu.get_barrier_semaphore()
    ring = Ring(n, own, got, out, sums, (far0, far1, far2, far3), send, recv, out_sem)
    for device in ring.to:
        pl.semaphore_signal(barrier, inc=1, device_id=device, device_id_type=pl.DeviceIdType.MESH)

    def columns(j):
        return pl.ds(pl.multiple_of(j * (2 * FS), 2 * FS), 2 * FS)

    def weights(l, j):
        return (
            pltpu.make_async_copy(wg.at[l, :, pl.ds(j * FS, FS)], w_gu.at[l, :, pl.ds(2 * j * FS, FS)], wsem.at[l, j, 0]),
            pltpu.make_async_copy(wu.at[l, :, pl.ds(j * FS, FS)], w_gu.at[l, :, pl.ds(2 * j * FS + FS, FS)], wsem.at[l, j, 1]),
            pltpu.make_async_copy(wd.at[l, pl.ds(j * FS, FS), :], w_d.at[l, j], wsem.at[l, j, 2]),
        )

    def state(m):
        return pltpu.make_async_copy(x.at[m], h1.at[m], sem.at[m])

    all_dy = pltpu.make_async_copy(dy, dyv, sem.at[tiles])
    state(0).start()
    for i in (0, 1, 2):
        for j in range(slices):
            weights(0, j)[i].start()
        if i == 1:
            state(1).start()
    all_dy.start()
    for m in range(2, tiles):
        state(m).start()
    for j in range(slices):
        for c in weights(1, j):
            c.start()

    def forward_a(m, ready=lambda j: None):
        a1[m] = forward_first(h1[m], w_gu.at[0], act, ready)

    def forward_b(m):
        h = forward_second(h1[m], w_d.at[0], act)
        h1[m] = h
        a = normed(h)
        a2[m] = a
        at[m] = a.T
        dyt[m] = dyv[m].T

    def forward(m, _):
        state(m + 1).wait()
        forward_b(m)
        forward_a(m + 1)
        return 0

    def ready(j):
        for first, last in ((0, 2), (2, slices)):
            if j == first:
                for here in range(first, last):
                    for c in weights(0, here)[:2]:
                        c.wait()

    state(0).wait()
    forward_a(0, ready)
    for j in range(slices):
        weights(0, j)[2].wait()
    all_dy.wait()
    lax.fori_loop(0, tiles - 1, forward, 0)
    forward_b(tiles - 1)
    for j in range(slices):
        for c in weights(1, j):
            c.wait()
    pl.semaphore_wait(barrier, 2)

    def offset(k, every):
        return 1 + every * k if k <= ring.sends else 5 + every * ring.sends

    def events(now, m, odd):
        for k in reversed(range(ring.sends + 2)):
            cases = []
            for every, low, high in ((SOONER, 0, EARLY), (EVERY, EARLY, total)):
                ago, at_tile = divmod(offset(k, every), tiles)
                place = now - 1 - ago
                t = jnp.where(place > slices, place - 1, place)
                if at_tile % 2 == odd:
                    cases.append(((m == at_tile) & (place != slices) & (t >= low) & (t < high), t))
            if cases:
                here, t = cases[0]
                for other, u in cases[1:]:
                    t = jnp.where(other, u, t)
                    here = here | other

                @pl.when(here)
                def _():
                    ring.event(lax.rem(t, SLOTS), t, k)

    def finish(s):
        slot = lax.rem(s, SLOTS)
        wide = acc_gu.shape[0] // n
        own[slot, :, :wide] = acc_gu[...].astype(BF16).reshape(n, wide, 2 * FS)
        own[slot, :, wide:] = acc_d[...].T.astype(BF16).reshape(n, FS // n, -1)
        acc_gu[...] = jnp.zeros_like(acc_gu)
        acc_d[...] = jnp.zeros_like(acc_d)

    def push(m, j, i):
        return pltpu.make_async_copy((buf0, buf1)[i].at[:, pl.ds(0, 2 * FS)], dgu.at[m, :, columns(j)], push_sem.at[i])

    def pull(m):
        return pltpu.make_async_copy(dgu.at[m], pulled.at[lax.rem(m, 2)], pull_sem.at[lax.rem(m, 2)])

    def backward(l):
        second = l == layers - 1
        states = a2 if second else a1

        def slice_a(m, j, buf):
            slice_first(states[m], dyv[m], w_gu[l, :, columns(j)], w_d[l, j], buf)

        def slice_b(m, buf):
            slice_second(at[m], dyt[m], buf, acc_gu, acc_d)

        def one_slice(j, _):
            now = j if second else slices + 1 + j

            def pair(i, _):
                for half, here, there in ((0, buf0, buf1), (1, buf1, buf0)):
                    m = 2 * i + half
                    events(now, m, half)
                    if second:
                        @pl.when((i > 0) | (j > 0))
                        def _():
                            push(m, j, half).wait()

                    slice_a(m, j, here)
                    slice_b(lax.rem(m + tiles - 1, tiles), there)
                    if second:
                        push(m, j, half).start()
                    if half == 0:
                        @pl.when((i == 0) & (j > 0))
                        def _():
                            finish((0 if second else slices) + j - 1)

                return 0

            return lax.fori_loop(0, tiles // 2, pair, 0)

        buf1[...] = jnp.zeros_like(buf1)
        lax.fori_loop(0, slices, one_slice, 0)
        if second:
            for m in (0, 1):
                pull(m).start()
        slice_b(tiles - 1, buf1)
        finish((slices if second else total) - 1)

    def turn(m, _):
        for odd in (0, 1):
            events(slices, m, odd)
        pull(m).wait()
        parts = 2
        size = TM // parts
        for part in range(parts):
            rows = pl.ds(part * size, size)
            da = dot_t(pulled[lax.rem(m, 2), rows], w_gu[layers - 1])
            back = norm_back(da, h1[m, rows], dyv[m, rows])
            dyv[m, rows] = back
            dyt[m, :, rows] = back.T
            at[m, :, rows] = a1[m, rows].T

        @pl.when(m + 2 < tiles)
        def _():
            pull(m + 2).start()

        return 0

    acc_gu[...] = jnp.zeros_like(acc_gu)
    acc_d[...] = jnp.zeros_like(acc_d)
    backward(layers - 1)
    for i in (0, 1):
        push(i, 0, i).wait()
    lax.fori_loop(0, tiles, turn, 0)
    backward(0)

    def drain(now, _):
        def pair(i, _):
            for half in (0, 1):
                events(now, 2 * i + half, half)
            return 0

        return lax.fori_loop(0, tiles // 2, pair, 0)

    end = total + 1
    lax.fori_loop(end, end + 1 + offset(ring.sends + 1, EVERY) // tiles, drain, 0)


def adam_math(w, m, v, g):
    m = 0.9 * m + 0.1 * g
    v = 0.95 * v + 0.05 * g * g
    step = m * lax.rsqrt(v + 1e-8) + 0.1 * w
    return (w - 0.02 * step).astype(BF16), m, v


def adam_kernel(halves, where, *refs):
    gs, ins, outs = refs[:halves], refs[halves : halves + 9], refs[-9:]
    slices = gs[0].shape[0]
    wide = ins[0].shape[2]
    for j in range(slices):
        g = [r[j].reshape(r.shape[-2:]) for r in gs]
        g = (g[0] if halves == 1 else jnp.concatenate(g, axis=0)).astype(F32)
        columns = slice(j * FS, (j + 1) * FS)
        for i, here in ((0, (0, 0, slice(None), columns)), (1, (0, 0, slice(None), columns)), (2, (0, j, 0))):
            part = (g[:wide, :FS], g[:wide, FS:], g[wide:])[i]
            w, m, v = (ins[k * 3 + i][here] for k in range(3))
            new = adam_math(w.astype(F32), m, v, part)
            for k in range(3):
                outs[k * 3 + i][here] = new[k]


def adam(n, offsets, gs, g_spec, arrays, so_far):
    layers = arrays[0].shape[0]
    slices = arrays[2].shape[1]
    extra = [] if so_far is None else list(so_far)
    where = lax.axis_index("dp").astype(jnp.int32).reshape(1)
    step = offsets[1] - offsets[0] if len(offsets) > 1 else 1

    def chunk(o, where):
        return lax.rem(where[0] + o * step + (offsets[0] + n), n)

    wide = pl.BlockSpec((1, 1) + arrays[0].shape[2:], lambda l, o, where: (l, chunk(o, where), 0, 0))
    tall = pl.BlockSpec((1, slices, 1) + arrays[2].shape[3:], lambda l, o, where: (l, 0, chunk(o, where), 0, 0))
    specs = [wide, wide, tall] * 3
    size = sum(a.size * a.dtype.itemsize for a in arrays) * 2 * len(offsets) // n
    return pl.pallas_call(
        functools.partial(adam_kernel, len(gs)),
        grid_spec=pltpu.PrefetchScalarGridSpec(
            num_scalar_prefetch=1,
            grid=(layers, len(offsets)),
            in_specs=[g_spec(chunk)] * len(gs) + specs + [pl.BlockSpec(memory_space=pl.ANY)] * len(extra),
            out_specs=specs,
        ),
        out_shape=[jax.ShapeDtypeStruct(a.shape, a.dtype) for a in arrays],
        input_output_aliases={1 + len(gs) + 9 + i: i for i in range(len(extra))},
        compiler_params=pltpu.CompilerParams(vmem_limit_bytes=32_000_000),
        cost_estimate=pl.CostEstimate(flops=40 * size, bytes_accessed=size, transcendentals=0),
    )(where, *gs, *arrays, *extra)


def solution(mesh):
    n = mesh.shape["dp"]

    def step(x, dy, *arrays):
        wg, wu, wd = arrays[:3]
        tokens, d = x.shape[1:]
        layers, _, ff = wg.shape
        tiles, slices = tokens // TM, ff // FS
        x, dy = x.reshape(tiles, TM, d), dy.reshape(tiles, TM, d)
        hbm = pl.BlockSpec(memory_space=pl.ANY)
        half, rows = n // 2, (d + FS) // n
        mm = 2 * tokens * d * ff
        sums, *far, _ = pl.pallas_call(
            functools.partial(train_kernel, n),
            in_specs=[hbm] * 5,
            out_specs=[hbm] * 6,
            out_shape=[jax.ShapeDtypeStruct((layers * slices, n, rows, d), BF16)]
            + [jax.ShapeDtypeStruct((layers * slices, rows // 2, d), BF16)] * 4
            + [jax.ShapeDtypeStruct((tiles, TM, 2 * ff), BF16)],
            scratch_shapes=[
                pltpu.VMEM((layers, d, 2 * ff), BF16),
                pltpu.VMEM((layers, slices, FS, d), BF16),
                pltpu.VMEM((tiles, TM, d), BF16),
                pltpu.VMEM((tiles, TM, d), BF16),
                pltpu.VMEM((tiles, d, TM), BF16),
                pltpu.VMEM((tiles, TM, d), BF16),
                pltpu.VMEM((tiles, d, TM), BF16),
                pltpu.VMEM((tiles, TM, d), BF16),
                pltpu.VMEM((2, TM, 2 * ff), BF16),
                pltpu.VMEM((TM, ff), BF16),
                pltpu.VMEM((TM, 3 * FS), BF16),
                pltpu.VMEM((TM, 3 * FS), BF16),
                pltpu.VMEM((d, 2 * FS), F32),
                pltpu.VMEM((d, FS), F32),
                pltpu.VMEM((SLOTS, n, rows, d), BF16),
                pltpu.VMEM((SLOTS, half, 2, rows, d), BF16),
                pltpu.VMEM((SLOTS, n, rows, d), BF16),
                pltpu.SemaphoreType.DMA((tiles + 1,)),
                pltpu.SemaphoreType.DMA((layers, slices, 3)),
                pltpu.SemaphoreType.DMA((2,)),
                pltpu.SemaphoreType.DMA((2,)),
                pltpu.SemaphoreType.DMA((SLOTS, 2 * half - 2, 2)),
                pltpu.SemaphoreType.DMA((SLOTS, 2 * half - 2, 2)),
                pltpu.SemaphoreType.DMA((SLOTS, n + 1)),
            ],
            compiler_params=pltpu.CompilerParams(vmem_limit_bytes=VMEM_LIMIT, collective_id=0, has_side_effects=True),
            cost_estimate=pl.CostEstimate(flops=17 * mm, bytes_accessed=90 * 10**6, transcendentals=0),
        )(x, dy, wg, wu, wd)
        chunks = [a.reshape(layers, n, d // n, ff) if a.shape[1] == d else a.reshape(layers, slices, n, FS // n, d) for a in arrays]
        left = [(i, (i + n - 1) % n) for i in range(n)]
        right = [(i, (i + 1) % n) for i in range(n)]

        def whole(chunk):
            return pl.BlockSpec((slices, 1, rows, d), lambda l, o, where: (layers - 1 - l, chunk(o, where), 0, 0))

        def halves(chunk):
            return pl.BlockSpec((slices, rows // 2, d), lambda l, o, where: (layers - 1 - l, 0, 0))

        near = []
        for i, way in enumerate((left, left, right, right)):
            near.append(lax.ppermute(far[i], "dp", way))
        new = adam(n, tuple(range(2 - half, half - 1)), [sums], whole, chunks, None)
        last = []
        for i, way in ((0, left), (3, right)):
            last.append(lax.ppermute(near[i], "dp", way))
        new = adam(n, (half - 1,), near[:2], halves, chunks, new)
        new = adam(n, (1 - half,), near[2:], halves, chunks, new)
        new = adam(n, (half,), last, halves, chunks, new)
        return tuple(o.reshape(a.shape) for o, a in zip(new, arrays))

    return jax.shard_map(
        step,
        mesh=mesh,
        in_specs=(P(("rep", "dp"), None, None),) * 2 + (P(None, None, None),) * 9,
        out_specs=(P("rep", None, None),) * 9,
        check_vma=False,
    )
```

```python
import functools

import jax
import jax.numpy as jnp
from jax import lax
from jax.experimental import pallas as pl
from jax.experimental.pallas import tpu as pltpu
from jax.sharding import PartitionSpec as P


TM = 512
PAIR = 2
FS = 256
F32, BF16 = jnp.float32, jnp.bfloat16
VMEM_LIMIT = 67_000_000


def dot(a, b):
    return jnp.dot(a, b, preferred_element_type=F32)


def dot_t(a, b):
    return lax.dot_general(a, b, (((1,), (1,)), ((), ())), preferred_element_type=F32)


def scale_of(wide):
    return lax.rsqrt(jnp.mean(wide * wide, -1, keepdims=True) + 1e-6)


def normed(h):
    wide = h.astype(F32)
    return (wide * scale_of(wide)).astype(BF16)


def sigmoid(g):
    return 0.5 * jnp.tanh(0.5 * g) + 0.5


def forward_first(h, w_gu, act_ref, ready=lambda j: None):
    a = normed(h)
    for j in range(w_gu.shape[1] // (2 * FS)):
        ready(j)
        gu = dot(a, w_gu[:, 2 * j * FS : 2 * (j + 1) * FS])
        g, u = gu[:, :FS], gu[:, FS:]
        act_ref[:, j * FS : (j + 1) * FS] = (g * sigmoid(g) * u).astype(BF16)
    return a


def forward_second(h, w_d, act_ref):
    slices = w_d.shape[0]
    y = dot(act_ref[...], w_d[...].reshape(slices * FS, -1)).astype(BF16)
    return (h.astype(F32) + y.astype(F32)).astype(BF16)


def slice_first(a, dy, wgu, wd, buf):
    gu = dot(a, wgu)
    dact = dot_t(dy, wd)
    g, u = gu[:, :FS], gu[:, FS:]
    dact = dact.astype(BF16).astype(F32)
    s = sigmoid(g)
    silu = g * s
    shape = buf.shape[:2] + (FS,)
    buf[:, :, 2 * FS : 3 * FS] = (silu * u).astype(BF16).reshape(shape)
    buf[:, :, FS : 2 * FS] = (dact * silu).astype(BF16).reshape(shape)
    buf[:, :, :FS] = (dact * u * (s + silu * (1.0 - s))).astype(BF16).reshape(shape)


def slice_second(a_t, dy_t, buf, acc_gu, acc_d):
    acc_d[...] += sum(dot(dy_t[i], buf[i, :, 2 * FS : 3 * FS]) for i in range(PAIR))
    acc_gu[...] += sum(dot(a_t[i], buf[i, :, : 2 * FS]) for i in range(PAIR))


def norm_back(da, h, dy):
    d = h.shape[-1]
    da = da.astype(BF16).astype(F32)
    h = h.astype(F32)
    r = scale_of(h)
    along = jnp.sum(da * h, -1, keepdims=True)
    dh = (da * r - h * (along * r * r * r * (1.0 / d))).astype(BF16)
    return (dy.astype(F32) + dh.astype(F32)).astype(BF16)


class Ring:
    def __init__(self, n, own, got, out, sums, far, send, recv, out_sem):
        self.n, self.half, self.rows = n, n // 2, own.shape[2]
        self.kept = self.half - 2
        self.sends = self.half + self.kept
        self.own, self.got, self.out, self.sums, self.far = own, got, out, sums, far
        self.send, self.recv, self.out_sem = send, recv, out_sem
        self.me = lax.axis_index("dp")
        self.to = ({"dp": lax.rem(self.me + n - 1, n)}, {"dp": lax.rem(self.me + 1, n)})

    def chunk(self, way, offset):
        return lax.rem(self.me + (offset if way == 0 else -offset) + self.n, self.n)

    def part(self, way, halved):
        size = self.rows // 2 if halved else self.rows
        return pl.ds(size if halved and way == 1 else 0, size)

    def copy(self, slot, k, way):
        h = self.half
        rows = self.part(way, k == 0)
        chunk = self.chunk(way, k - h)
        if k < h:
            src = self.own.at[slot, chunk, rows]
            dst = self.got.at[slot, k, way, rows]
        else:
            src = dst = self.out.at[slot, chunk, rows]
        return pltpu.make_async_remote_copy(
            src_ref=src,
            dst_ref=dst,
            send_sem=self.send.at[slot, k, way],
            recv_sem=self.recv.at[slot, k, way],
            device_id=self.to[way],
            device_id_type=pl.DeviceIdType.MESH,
        )

    def write_out(self, slot, t):
        copies = []
        for offset in range(-self.kept, self.kept + 1):
            chunk = self.chunk(0, offset)
            copies.append((self.out.at[slot, chunk], self.sums.at[t, chunk]))
        for way in (0, 1):
            chunk = self.chunk(way, self.kept)
            for part in (0, 1):
                copies.append((self.out.at[slot, chunk, self.part(part, True)], self.far[2 * way + part].at[t]))
        return [pltpu.make_async_copy(a, b, self.out_sem.at[slot, i]) for i, (a, b) in enumerate(copies)]

    def event(self, slot, t, k):
        h = self.half
        if 0 < k <= self.sends:
            for way in (0, 1):
                self.copy(slot, k - 1, way).wait_recv()
        if 0 < k < h:
            for way in (0, 1):
                rows, chunk = self.part(way, k == 1), self.chunk(way, k - h)
                came = self.got[slot, k - 1, way, rows].astype(F32)
                self.own[slot, chunk, rows] = (self.own[slot, chunk, rows].astype(F32) + came).astype(BF16)
        if k == h:
            total = self.own[slot, self.me].astype(F32) + self.got[slot, h - 1, 0].astype(F32) + self.got[slot, h - 1, 1].astype(F32)
            self.out[slot, self.me] = total.astype(BF16)
        if k < self.sends:
            for way in (0, 1):
                self.copy(slot, k, way).start()
        if k == self.sends:
            for copy in self.write_out(slot, t):
                copy.start()
        for sent in range(h) if k == h else range(h, self.sends) if k == self.sends else ():
            for way in (0, 1):
                self.copy(slot, sent, way).wait_send()
        if k == self.sends + 1:
            for copy in self.write_out(slot, t):
                copy.wait()


SLOTS = 4
EVERY = 3


def train_kernel(n, x, dy, wg, wu, wd, sums, far0, far1, far2, far3, dgu, w_gu, w_d, a1, a2, at, dyv, dyt, h1, pulled, act, buf0, buf1,
                 acc_gu, acc_d, own, got, out, sem, wsem, push_sem, pull_sem, send, recv, out_sem):
    layers, slices = w_d.shape[:2]
    tiles = x.shape[0]
    total = layers * slices
    barrier = pltpu.get_barrier_semaphore()
    ring = Ring(n, own, got, out, sums, (far0, far1, far2, far3), send, recv, out_sem)
    for device in ring.to:
        pl.semaphore_signal(barrier, inc=1, device_id=device, device_id_type=pl.DeviceIdType.MESH)

    def columns(j):
        return pl.ds(pl.multiple_of(j * (2 * FS), 2 * FS), 2 * FS)

    def weights(l, j):
        return (
            pltpu.make_async_copy(wg.at[l, :, pl.ds(j * FS, FS)], w_gu.at[l, :, pl.ds(2 * j * FS, FS)], wsem.at[l, j, 0]),
            pltpu.make_async_copy(wu.at[l, :, pl.ds(j * FS, FS)], w_gu.at[l, :, pl.ds(2 * j * FS + FS, FS)], wsem.at[l, j, 1]),
            pltpu.make_async_copy(wd.at[l, pl.ds(j * FS, FS), :], w_d.at[l, j], wsem.at[l, j, 2]),
        )

    def state(m):
        return pltpu.make_async_copy(x.at[m], h1.at[m], sem.at[m])

    all_dy = pltpu.make_async_copy(dy, dyv, sem.at[tiles])
    state(0).start()
    for j in range(slices):
        for c in weights(0, j)[:2]:
            c.start()
    state(1).start()
    for j in range(slices):
        weights(0, j)[2].start()
    all_dy.start()
    for m in range(2, tiles):
        state(m).start()
    for j in range(slices):
        for c in weights(1, j):
            c.start()

    def forward_a(m, ready=lambda j: None):
        a1[m] = forward_first(h1[m], w_gu.at[0], act, ready)

    def forward_b(m):
        h = forward_second(h1[m], w_d.at[0], act)
        h1[m] = h
        a = normed(h)
        a2[m] = a
        at[m] = a.T
        dyt[m] = dyv[m].T

    def forward(m, _):
        state(m + 1).wait()
        forward_b(m)
        forward_a(m + 1)
        return 0

    def ready(j):
        for first, last in ((0, 2), (2, slices)):
            if j == first:
                for here in range(first, last):
                    for c in weights(0, here)[:2]:
                        c.wait()

    state(0).wait()
    forward_a(0, ready)
    for j in range(slices):
        weights(0, j)[2].wait()
    all_dy.wait()
    lax.fori_loop(0, tiles - 1, forward, 0)
    forward_b(tiles - 1)
    for j in range(slices):
        for c in weights(1, j):
            c.wait()
    pl.semaphore_wait(barrier, 2)

    steps = tiles // PAIR
    turns = tiles // steps
    offsets = [1 + EVERY * k for k in range(ring.sends + 1)] + [3 + EVERY * ring.sends]

    def round_of(now):
        found = []
        for ago in range(1 + offsets[-1] // steps):
            place = now - 1 - ago
            t = jnp.where(place >= slices, place - turns, place)
            there = (place >= 0) & (t < total) & ((place < slices) | (t >= slices))
            found.append((there, t, lax.rem(t + SLOTS, SLOTS)))
        return found

    def events(found, u, odd=None):
        for k in reversed(range(len(offsets))):
            ago, at_step = divmod(offsets[k], steps)
            if odd is not None and at_step % 2 != odd:
                continue
            there, t, slot = found[ago]

            @pl.when((u == at_step) & there)
            def _():
                ring.event(slot, t, k)

    def finish(s):
        slot = lax.rem(s, SLOTS)
        wide = acc_gu.shape[0] // n
        own[slot, :, :wide] = acc_gu[...].astype(BF16).reshape(n, wide, 2 * FS)
        own[slot, :, wide:] = acc_d[...].T.astype(BF16).reshape(n, FS // n, -1)
        acc_gu[...] = jnp.zeros_like(acc_gu)
        acc_d[...] = jnp.zeros_like(acc_d)

    def push(u, j, i):
        return pltpu.make_async_copy(
            (buf0, buf1)[i].at[:, :, pl.ds(0, 2 * FS)], dgu.at[pl.ds(u * PAIR, PAIR), :, columns(j)], push_sem.at[i]
        )

    def pull(m):
        return pltpu.make_async_copy(dgu.at[m], pulled.at[lax.rem(m, 2)], pull_sem.at[lax.rem(m, 2)])

    def backward(l):
        second = l == layers - 1
        states = a2 if second else a1

        def slice_a(u, j, buf):
            here = pl.ds(u * PAIR, PAIR)
            rows = (PAIR * TM, dyv.shape[-1])
            slice_first(states[here].reshape(rows), dyv[here].reshape(rows), w_gu[l, :, columns(j)], w_d[l, j], buf)

        def slice_b(u, buf):
            here = pl.ds(u * PAIR, PAIR)
            slice_second(at.at[here], dyt.at[here], buf, acc_gu, acc_d)

        def one_slice(j, _):
            found = round_of(j if second else slices + turns + j)

            def two_steps(i, _):
                for half, here, there in ((0, buf0, buf1), (1, buf1, buf0)):
                    u = 2 * i + half
                    events(found, u, half)
                    if second:
                        @pl.when((i > 0) | (j > 0))
                        def _():
                            push(u, j, half).wait()

                    slice_a(u, j, here)
                    slice_b(lax.rem(u + steps - 1, steps), there)
                    if second:
                        push(u, j, half).start()
                    if half == 0:
                        @pl.when((i == 0) & (j > 0))
                        def _():
                            finish((0 if second else slices) + j - 1)

                return 0

            return lax.fori_loop(0, steps // 2, two_steps, 0)

        buf1[...] = jnp.zeros_like(buf1)
        lax.fori_loop(0, slices, one_slice, 0)
        if second:
            for m in (0, 1):
                pull(m).start()
        slice_b(steps - 1, buf1)
        finish((slices if second else total) - 1)

    def turn(m, _):
        events(round_of(slices + m // steps), lax.rem(m, steps))
        pull(m).wait()
        parts = 2
        size = TM // parts
        for part in range(parts):
            rows = pl.ds(part * size, size)
            da = dot_t(pulled[lax.rem(m, 2), rows], w_gu[layers - 1])
            back = norm_back(da, h1[m, rows], dyv[m, rows])
            dyv[m, rows] = back
            dyt[m, :, rows] = back.T
            at[m, :, rows] = a1[m, rows].T

        @pl.when(m + 2 < tiles)
        def _():
            pull(m + 2).start()

        return 0

    acc_gu[...] = jnp.zeros_like(acc_gu)
    acc_d[...] = jnp.zeros_like(acc_d)
    backward(layers - 1)
    for i in (0, 1):
        push(i, 0, i).wait()
    lax.fori_loop(0, tiles, turn, 0)
    backward(0)

    def drain(now, _):
        found = round_of(now)

        def one(u, _):
            events(found, u)
            return 0

        return lax.fori_loop(0, steps, one, 0)

    end = total + turns
    lax.fori_loop(end, end + 1 + offsets[-1] // steps, drain, 0)


def adam_math(w, m, v, g):
    m = 0.9 * m + 0.1 * g
    v = 0.95 * v + 0.05 * g * g
    step = m * lax.rsqrt(v + 1e-8) + 0.1 * w
    return (w - 0.02 * step).astype(BF16), m, v


def adam_kernel(halves, where, *refs):
    gs, ins, outs = refs[:halves], refs[halves : halves + 9], refs[-9:]
    slices = gs[0].shape[0]
    wide = ins[0].shape[2]
    for j in range(slices):
        g = [r[j].reshape(r.shape[-2:]) for r in gs]
        g = (g[0] if halves == 1 else jnp.concatenate(g, axis=0)).astype(F32)
        columns = slice(j * FS, (j + 1) * FS)
        for i, here in ((0, (0, 0, slice(None), columns)), (1, (0, 0, slice(None), columns)), (2, (0, j, 0))):
            part = (g[:wide, :FS], g[:wide, FS:], g[wide:])[i]
            w, m, v = (ins[k * 3 + i][here] for k in range(3))
            new = adam_math(w.astype(F32), m, v, part)
            for k in range(3):
                outs[k * 3 + i][here] = new[k]


def adam(n, offsets, gs, g_spec, arrays, so_far):
    layers = arrays[0].shape[0]
    slices = arrays[2].shape[1]
    extra = [] if so_far is None else list(so_far)
    where = lax.axis_index("dp").astype(jnp.int32).reshape(1)
    step = offsets[1] - offsets[0] if len(offsets) > 1 else 1

    def chunk(o, where):
        return lax.rem(where[0] + o * step + (offsets[0] + n), n)

    wide = pl.BlockSpec((1, 1) + arrays[0].shape[2:], lambda l, o, where: (l, chunk(o, where), 0, 0))
    tall = pl.BlockSpec((1, slices, 1) + arrays[2].shape[3:], lambda l, o, where: (l, 0, chunk(o, where), 0, 0))
    specs = [wide, wide, tall] * 3
    size = sum(a.size * a.dtype.itemsize for a in arrays) * 2 * len(offsets) // n
    return pl.pallas_call(
        functools.partial(adam_kernel, len(gs)),
        grid_spec=pltpu.PrefetchScalarGridSpec(
            num_scalar_prefetch=1,
            grid=(layers, len(offsets)),
            in_specs=[g_spec(chunk)] * len(gs) + specs + [pl.BlockSpec(memory_space=pl.ANY)] * len(extra),
            out_specs=specs,
        ),
        out_shape=[jax.ShapeDtypeStruct(a.shape, a.dtype) for a in arrays],
        input_output_aliases={1 + len(gs) + 9 + i: i for i in range(len(extra))},
        compiler_params=pltpu.CompilerParams(vmem_limit_bytes=60_000_000),
        cost_estimate=pl.CostEstimate(flops=40 * size, bytes_accessed=size, transcendentals=0),
    )(where, *gs, *arrays, *extra)


def solution(mesh):
    n = mesh.shape["dp"]

    def step(x, dy, *arrays):
        wg, wu, wd = arrays[:3]
        tokens, d = x.shape[1:]
        layers, _, ff = wg.shape
        tiles, slices = tokens // TM, ff // FS
        x, dy = x.reshape(tiles, TM, d), dy.reshape(tiles, TM, d)
        hbm = pl.BlockSpec(memory_space=pl.ANY)
        half, rows = n // 2, (d + FS) // n
        mm = 2 * tokens * d * ff
        sums, *far, _ = pl.pallas_call(
            functools.partial(train_kernel, n),
            in_specs=[hbm] * 5,
            out_specs=[hbm] * 6,
            out_shape=[jax.ShapeDtypeStruct((layers * slices, n, rows, d), BF16)]
            + [jax.ShapeDtypeStruct((layers * slices, rows // 2, d), BF16)] * 4
            + [jax.ShapeDtypeStruct((tiles, TM, 2 * ff), BF16)],
            scratch_shapes=[
                pltpu.VMEM((layers, d, 2 * ff), BF16),
                pltpu.VMEM((layers, slices, FS, d), BF16),
                pltpu.VMEM((tiles, TM, d), BF16),
                pltpu.VMEM((tiles, TM, d), BF16),
                pltpu.VMEM((tiles, d, TM), BF16),
                pltpu.VMEM((tiles, TM, d), BF16),
                pltpu.VMEM((tiles, d, TM), BF16),
                pltpu.VMEM((tiles, TM, d), BF16),
                pltpu.VMEM((2, TM, 2 * ff), BF16),
                pltpu.VMEM((TM, ff), BF16),
                pltpu.VMEM((PAIR, TM, 3 * FS), BF16),
                pltpu.VMEM((PAIR, TM, 3 * FS), BF16),
                pltpu.VMEM((d, 2 * FS), F32),
                pltpu.VMEM((d, FS), F32),
                pltpu.VMEM((SLOTS, n, rows, d), BF16),
                pltpu.VMEM((SLOTS, half, 2, rows, d), BF16),
                pltpu.VMEM((SLOTS, n, rows, d), BF16),
                pltpu.SemaphoreType.DMA((tiles + 1,)),
                pltpu.SemaphoreType.DMA((layers, slices, 3)),
                pltpu.SemaphoreType.DMA((2,)),
                pltpu.SemaphoreType.DMA((2,)),
                pltpu.SemaphoreType.DMA((SLOTS, 2 * half - 2, 2)),
                pltpu.SemaphoreType.DMA((SLOTS, 2 * half - 2, 2)),
                pltpu.SemaphoreType.DMA((SLOTS, n + 1)),
            ],
            compiler_params=pltpu.CompilerParams(vmem_limit_bytes=VMEM_LIMIT, collective_id=0, has_side_effects=True),
            cost_estimate=pl.CostEstimate(flops=17 * mm, bytes_accessed=90 * 10**6, transcendentals=0),
        )(x, dy, wg, wu, wd)
        chunks = [a.reshape(layers, n, d // n, ff) if a.shape[1] == d else a.reshape(layers, slices, n, FS // n, d) for a in arrays]
        left = [(i, (i + n - 1) % n) for i in range(n)]
        right = [(i, (i + 1) % n) for i in range(n)]

        def whole(chunk):
            return pl.BlockSpec((slices, 1, rows, d), lambda l, o, where: (layers - 1 - l, chunk(o, where), 0, 0))

        def halves(chunk):
            return pl.BlockSpec((slices, rows // 2, d), lambda l, o, where: (layers - 1 - l, 0, 0))

        near = []
        for i, way in enumerate((left, left, right, right)):
            near.append(lax.ppermute(far[i], "dp", way))
        new = adam(n, tuple(range(2 - half, half - 1)), [sums], whole, chunks, None)
        last = []
        for i, way in ((0, left), (3, right)):
            last.append(lax.ppermute(near[i], "dp", way))
        new = adam(n, (half - 1,), near[:2], halves, chunks, new)
        new = adam(n, (1 - half,), near[2:], halves, chunks, new)
        new = adam(n, (half,), last, halves, chunks, new)
        return tuple(o.reshape(a.shape) for o, a in zip(new, arrays))

    return jax.shard_map(
        step,
        mesh=mesh,
        in_specs=(P(("rep", "dp"), None, None),) * 2 + (P(None, None, None),) * 9,
        out_specs=(P("rep", None, None),) * 9,
        check_vma=False,
    )
```

```python
import functools

import jax
import jax.numpy as jnp
from jax import lax
from jax.experimental import pallas as pl
from jax.experimental.pallas import tpu as pltpu
from jax.sharding import PartitionSpec as P


TM = 512
PAIR = 2
FS = 256
F32, BF16 = jnp.float32, jnp.bfloat16
VMEM_LIMIT = 67_000_000


def dot(a, b):
    return jnp.dot(a, b, preferred_element_type=F32)


def dot_t(a, b):
    return lax.dot_general(a, b, (((1,), (1,)), ((), ())), preferred_element_type=F32)


def scale_of(wide):
    return lax.rsqrt(jnp.mean(wide * wide, -1, keepdims=True) + 1e-6)


def normed(h):
    wide = h.astype(F32)
    return (wide * scale_of(wide)).astype(BF16)


def sigmoid(g):
    return 0.5 * jnp.tanh(0.5 * g) + 0.5


def forward_first(h, w_gu, act_ref, ready=lambda j: None):
    a = normed(h)
    for j in range(w_gu.shape[1] // (2 * FS)):
        ready(j)
        gu = dot(a, w_gu[:, 2 * j * FS : 2 * (j + 1) * FS])
        g, u = gu[:, :FS], gu[:, FS:]
        act_ref[:, j * FS : (j + 1) * FS] = (g * sigmoid(g) * u).astype(BF16)
    return a


def forward_second(h, w_d, act_ref):
    slices = w_d.shape[0]
    y = dot(act_ref[...], w_d[...].reshape(slices * FS, -1)).astype(BF16)
    return (h.astype(F32) + y.astype(F32)).astype(BF16)


def slice_first(a, dy, wgu, wd, buf):
    gu = dot(a, wgu)
    dact = dot_t(dy, wd)
    g, u = gu[:, :FS], gu[:, FS:]
    dact = dact.astype(BF16).astype(F32)
    s = sigmoid(g)
    silu = g * s
    shape = buf.shape[:2] + (FS,)
    buf[:, :, 2 * FS : 3 * FS] = (silu * u).astype(BF16).reshape(shape)
    buf[:, :, FS : 2 * FS] = (dact * silu).astype(BF16).reshape(shape)
    buf[:, :, :FS] = (dact * u * (s + silu * (1.0 - s))).astype(BF16).reshape(shape)


def slice_second(a_t, dy_t, buf, acc_gu, acc_d):
    acc_d[...] += sum(dot(dy_t[i], buf[i, :, 2 * FS : 3 * FS]) for i in range(PAIR))
    acc_gu[...] += sum(dot(a_t[i], buf[i, :, : 2 * FS]) for i in range(PAIR))


def norm_back(da, h, dy):
    d = h.shape[-1]
    da = da.astype(BF16).astype(F32)
    h = h.astype(F32)
    r = scale_of(h)
    along = jnp.sum(da * h, -1, keepdims=True)
    dh = (da * r - h * (along * r * r * r * (1.0 / d))).astype(BF16)
    return (dy.astype(F32) + dh.astype(F32)).astype(BF16)


class Ring:
    def __init__(self, n, slices, own, got, out, sums, far, send, recv, out_sem, leaf_send, leaf_recv):
        self.n, self.half, self.rows = n, n // 2, own.shape[2]
        self.kept = self.half - 2
        self.sends = self.half + self.kept
        self.slices = slices
        self.own, self.got, self.out, self.sums, self.far = own, got, out, sums, far
        self.send, self.recv, self.out_sem = send, recv, out_sem
        self.leaf_send, self.leaf_recv = leaf_send, leaf_recv
        self.me = lax.axis_index("dp")
        self.to = ({"dp": lax.rem(self.me + n - 1, n)}, {"dp": lax.rem(self.me + 1, n)})

    def chunk(self, way, offset):
        return lax.rem(self.me + (offset if way == 0 else -offset) + self.n, self.n)

    def part(self, way, halved):
        size = self.rows // 2 if halved else self.rows
        return pl.ds(size if halved and way == 1 else 0, size)

    def copy(self, slot, k, way):
        h = self.half
        rows = self.part(way, k == 0)
        chunk = self.chunk(way, k - h)
        if k < h:
            src = self.own.at[slot, chunk, rows]
            dst = self.got.at[slot, k, way, rows]
        else:
            src = dst = self.out.at[slot, chunk, rows]
        return pltpu.make_async_remote_copy(
            src_ref=src,
            dst_ref=dst,
            send_sem=self.send.at[slot, k, way],
            recv_sem=self.recv.at[slot, k, way],
            device_id=self.to[way],
            device_id_type=pl.DeviceIdType.MESH,
        )

    def write_out(self, slot, t):
        chunks = [self.chunk(0, offset) for offset in range(-self.kept, self.kept + 1)]
        return [
            pltpu.make_async_copy(self.out.at[slot, chunk], self.sums.at[t, chunk], self.out_sem.at[slot, i])
            for i, chunk in enumerate(chunks)
        ]

    def write_far(self, slot, t, first):
        copies = []
        for way in (0, 1):
            chunk = self.chunk(way, self.kept)
            for place, part in ((0, way), (1, 1 - way)) if first else ((2, 1 - way),):
                to = self.far[way].at[place, t - self.slices if first else t]
                copies.append((self.out.at[slot, chunk, self.part(part, True)], to))
        i = 2 * self.kept + 1
        return [pltpu.make_async_copy(a, b, self.out_sem.at[slot, i + j]) for j, (a, b) in enumerate(copies)]

    def leaf(self, slot, t):
        return [
            pltpu.make_async_remote_copy(
                src_ref=self.out.at[slot, self.chunk(way, self.kept), self.part(way, True)],
                dst_ref=self.far[way].at[3, t],
                send_sem=self.leaf_send.at[slot, way],
                recv_sem=self.leaf_recv.at[slot, way],
                device_id=self.to[way],
                device_id_type=pl.DeviceIdType.MESH,
            )
            for way in (0, 1)
        ]

    def event(self, slot, t, k):
        h = self.half
        if 0 < k <= self.sends:
            for way in (0, 1):
                self.copy(slot, k - 1, way).wait_recv()
        if 0 < k < h:
            for way in (0, 1):
                rows, chunk = self.part(way, k == 1), self.chunk(way, k - h)
                came = self.got[slot, k - 1, way, rows].astype(F32)
                self.own[slot, chunk, rows] = (self.own[slot, chunk, rows].astype(F32) + came).astype(BF16)
        if k == h:
            total = self.own[slot, self.me].astype(F32) + self.got[slot, h - 1, 0].astype(F32) + self.got[slot, h - 1, 1].astype(F32)
            self.out[slot, self.me] = total.astype(BF16)
        if k < self.sends:
            for way in (0, 1):
                self.copy(slot, k, way).start()
        if k >= self.sends:
            start = k == self.sends

            @pl.when(t < self.slices)
            def _():
                for copy in self.leaf(slot, t) + self.write_far(slot, t, False):
                    copy.start() if start else copy.wait()

            @pl.when(t >= self.slices)
            def _():
                for copy in self.write_far(slot, t, True):
                    copy.start() if start else copy.wait()

            for copy in self.write_out(slot, t):
                copy.start() if start else copy.wait()
        for sent in range(h) if k == h else range(h, self.sends) if k == self.sends else ():
            for way in (0, 1):
                self.copy(slot, sent, way).wait_send()


SLOTS = 4
EVERY = 3


def train_kernel(n, x, dy, wg, wu, wd, sums, far0, far1, dgu, w_gu, w_d, a1, a2, at, dyv, dyt, h1, pulled, act, buf0, buf1,
                 acc_gu, acc_d, own, got, out, sem, wsem, push_sem, pull_sem, send, recv, out_sem, leaf_send, leaf_recv):
    layers, slices = w_d.shape[:2]
    tiles = x.shape[0]
    total = layers * slices
    barrier = pltpu.get_barrier_semaphore()
    ring = Ring(n, slices, own, got, out, sums, (far0, far1), send, recv, out_sem, leaf_send, leaf_recv)
    for device in ring.to:
        pl.semaphore_signal(barrier, inc=1, device_id=device, device_id_type=pl.DeviceIdType.MESH)

    def columns(j):
        return pl.ds(pl.multiple_of(j * (2 * FS), 2 * FS), 2 * FS)

    def weights(l, j):
        return (
            pltpu.make_async_copy(wg.at[l, :, pl.ds(j * FS, FS)], w_gu.at[l, :, pl.ds(2 * j * FS, FS)], wsem.at[l, j, 0]),
            pltpu.make_async_copy(wu.at[l, :, pl.ds(j * FS, FS)], w_gu.at[l, :, pl.ds(2 * j * FS + FS, FS)], wsem.at[l, j, 1]),
            pltpu.make_async_copy(wd.at[l, pl.ds(j * FS, FS), :], w_d.at[l, j], wsem.at[l, j, 2]),
        )

    def state(m):
        return pltpu.make_async_copy(x.at[m], h1.at[m], sem.at[m])

    all_dy = pltpu.make_async_copy(dy, dyv, sem.at[tiles])
    state(0).start()
    for j in range(slices):
        for c in weights(0, j)[:2]:
            c.start()
    state(1).start()
    for j in range(slices):
        weights(0, j)[2].start()
    all_dy.start()
    for m in range(2, tiles):
        state(m).start()
    for j in range(slices):
        for c in weights(1, j):
            c.start()

    def forward_a(m, ready=lambda j: None):
        a1[m] = forward_first(h1[m], w_gu.at[0], act, ready)

    def forward_b(m):
        h = forward_second(h1[m], w_d.at[0], act)
        h1[m] = h
        a = normed(h)
        a2[m] = a
        at[m] = a.T
        dyt[m] = dyv[m].T

    def forward(m, _):
        state(m + 1).wait()
        forward_b(m)
        forward_a(m + 1)
        return 0

    def ready(j):
        for first, last in ((0, 2), (2, slices)):
            if j == first:
                for here in range(first, last):
                    for c in weights(0, here)[:2]:
                        c.wait()

    state(0).wait()
    forward_a(0, ready)
    for j in range(slices):
        weights(0, j)[2].wait()
    all_dy.wait()
    lax.fori_loop(0, tiles - 1, forward, 0)
    forward_b(tiles - 1)
    for j in range(slices):
        for c in weights(1, j):
            c.wait()
    pl.semaphore_wait(barrier, 2)

    steps = tiles // PAIR
    turns = tiles // steps
    offsets = [1 + EVERY * k for k in range(ring.sends + 1)] + [3 + EVERY * ring.sends]

    def round_of(now):
        found = []
        for ago in range(1 + offsets[-1] // steps):
            place = now - 1 - ago
            t = jnp.where(place >= slices, place - turns, place)
            there = (place >= 0) & (t < total) & ((place < slices) | (t >= slices))
            found.append((there, t, lax.rem(t + SLOTS, SLOTS)))
        return found

    def events(found, u, odd=None):
        for k in reversed(range(len(offsets))):
            ago, at_step = divmod(offsets[k], steps)
            if odd is not None and at_step % 2 != odd:
                continue
            there, t, slot = found[ago]

            @pl.when((u == at_step) & there)
            def _():
                ring.event(slot, t, k)

    def finish(s):
        slot = lax.rem(s, SLOTS)
        wide, tall = acc_gu.shape[0] // n // 2, FS // n // 2
        gu = acc_gu[...].astype(BF16).reshape(n, 2, wide, 2 * FS)
        down = acc_d[...].T.astype(BF16).reshape(n, 2, tall, acc_d.shape[0])
        for half in (0, 1):
            start = half * (wide + tall)
            own[slot, :, start : start + wide] = gu[:, half]
            own[slot, :, start + wide : start + wide + tall] = down[:, half]
        acc_gu[...] = jnp.zeros_like(acc_gu)
        acc_d[...] = jnp.zeros_like(acc_d)

    def push(u, j, i):
        return pltpu.make_async_copy(
            (buf0, buf1)[i].at[:, :, pl.ds(0, 2 * FS)], dgu.at[pl.ds(u * PAIR, PAIR), :, columns(j)], push_sem.at[i]
        )

    def pull(m):
        return pltpu.make_async_copy(dgu.at[m], pulled.at[lax.rem(m, 2)], pull_sem.at[lax.rem(m, 2)])

    def backward(l):
        second = l == layers - 1
        states = a2 if second else a1

        def slice_a(u, j, buf):
            here = pl.ds(u * PAIR, PAIR)
            rows = (PAIR * TM, dyv.shape[-1])
            slice_first(states[here].reshape(rows), dyv[here].reshape(rows), w_gu[l, :, columns(j)], w_d[l, j], buf)

        def slice_b(u, buf):
            here = pl.ds(u * PAIR, PAIR)
            slice_second(at.at[here], dyt.at[here], buf, acc_gu, acc_d)

        def one_slice(j, _):
            found = round_of(j if second else slices + turns + j)

            def two_steps(i, _):
                for half, here, there in ((0, buf0, buf1), (1, buf1, buf0)):
                    u = 2 * i + half
                    events(found, u, half)
                    if second:
                        @pl.when((i > 0) | (j > 0))
                        def _():
                            push(u, j, half).wait()

                    slice_a(u, j, here)
                    slice_b(lax.rem(u + steps - 1, steps), there)
                    if second:
                        push(u, j, half).start()
                    if half == 0:
                        @pl.when((i == 0) & (j > 0))
                        def _():
                            finish((0 if second else slices) + j - 1)

                return 0

            return lax.fori_loop(0, steps // 2, two_steps, 0)

        buf1[...] = jnp.zeros_like(buf1)
        lax.fori_loop(0, slices, one_slice, 0)
        if second:
            for m in (0, 1):
                pull(m).start()
        slice_b(steps - 1, buf1)
        finish((slices if second else total) - 1)

    def turn(m, _):
        events(round_of(slices + m // steps), lax.rem(m, steps))
        pull(m).wait()
        parts = 2
        size = TM // parts
        for part in range(parts):
            rows = pl.ds(part * size, size)
            da = dot_t(pulled[lax.rem(m, 2), rows], w_gu[layers - 1])
            back = norm_back(da, h1[m, rows], dyv[m, rows])
            dyv[m, rows] = back
            dyt[m, :, rows] = back.T
            at[m, :, rows] = a1[m, rows].T

        @pl.when(m + 2 < tiles)
        def _():
            pull(m + 2).start()

        return 0

    acc_gu[...] = jnp.zeros_like(acc_gu)
    acc_d[...] = jnp.zeros_like(acc_d)
    backward(layers - 1)
    for i in (0, 1):
        push(i, 0, i).wait()
    lax.fori_loop(0, tiles, turn, 0)
    backward(0)

    def drain(now, _):
        found = round_of(now)

        def one(u, _):
            events(found, u)
            return 0

        return lax.fori_loop(0, steps, one, 0)

    end = total + turns
    lax.fori_loop(end, end + 1 + offsets[-1] // steps, drain, 0)


def adam_math(w, m, v, g):
    m = 0.9 * m + 0.1 * g
    v = 0.95 * v + 0.05 * g * g
    step = m * lax.rsqrt(v + 1e-8) + 0.1 * w
    return (w - 0.02 * step).astype(BF16), m, v


def adam_kernel(sources, table, me, *refs):
    gs, ins, outs = refs[:sources], refs[sources : sources + 9], refs[-9:]
    source = table[pl.program_id(0), 3]
    slices, wide = ins[2].shape[1], ins[0].shape[2]
    for j in range(slices):
        g = None
        for i, ref in enumerate(gs):
            here = (ref[j, 0] if ref.shape[0] == slices else ref[0, j]).astype(F32)
            g = here if g is None else jnp.where(source == i, here, g)
        columns = slice(j * FS, (j + 1) * FS)
        for i, here in ((0, (0, 0, slice(None), columns)), (1, (0, 0, slice(None), columns)), (2, (0, j, 0))):
            part = (g[:wide, :FS], g[:wide, FS:], g[wide:])[i]
            w, m, v = (ins[k * 3 + i][here] for k in range(3))
            new = adam_math(w.astype(F32), m, v, part)
            for k in range(3):
                outs[k * 3 + i][here] = new[k]


def adam(n, steps, gs, arrays, so_far, vmem):
    layers, slices = arrays[0].shape[0], arrays[2].shape[1]
    rows, d = gs[0].shape[-2:]
    half_rows = rows if gs[0].shape[1] == slices else rows // 2
    blocks = [0] * len(gs)
    table = []
    for layer, offset, half, source, block in steps:
        blocks[source] = block
        table.append([layer, offset + n, half, source] + blocks)
    table = jnp.array(table, jnp.int32)
    me = lax.axis_index("dp").astype(jnp.int32).reshape(1)

    def chunk(s, table, me):
        return lax.rem(me[0] + table[s, 1], n)

    def source(i, g):
        if g.shape[1] == slices:
            return pl.BlockSpec((1, slices, half_rows, d), lambda s, table, me: (table[s, 4 + i], 0, 0, 0))

        def whole(s, table, me):
            return layers - 1 - table[s, 0], lax.rem(me[0] + table[s, 4 + i], n), table[s, 2], 0

        return pl.BlockSpec((slices, 1, half_rows, d), whole)

    wide = pl.BlockSpec(
        (1, 1, arrays[0].shape[2] // 2, arrays[0].shape[3]), lambda s, table, me: (table[s, 0], chunk(s, table, me), table[s, 2], 0)
    )
    tall = pl.BlockSpec(
        (1, slices, 1, arrays[2].shape[3] // 2, d), lambda s, table, me: (table[s, 0], 0, chunk(s, table, me), table[s, 2], 0)
    )
    specs = [wide, wide, tall] * 3
    extra = [] if so_far is None else list(so_far)
    size = sum(a.size * a.dtype.itemsize for a in arrays) * len(steps) // (n * layers)
    return pl.pallas_call(
        functools.partial(adam_kernel, len(gs)),
        grid_spec=pltpu.PrefetchScalarGridSpec(
            num_scalar_prefetch=2,
            grid=(len(steps),),
            in_specs=[source(i, g) for i, g in enumerate(gs)] + specs + [pl.BlockSpec(memory_space=pl.ANY)] * len(extra),
            out_specs=specs,
        ),
        out_shape=[jax.ShapeDtypeStruct(a.shape, a.dtype) for a in arrays],
        input_output_aliases={2 + len(gs) + 9 + i: i for i in range(len(extra))},
        compiler_params=pltpu.CompilerParams(vmem_limit_bytes=vmem),
        cost_estimate=pl.CostEstimate(flops=40 * size, bytes_accessed=size, transcendentals=0),
    )(table, me, *gs, *arrays, *extra)


def solution(mesh):
    n = mesh.shape["dp"]

    def step(x, dy, *arrays):
        wg, wu, wd = arrays[:3]
        tokens, d = x.shape[1:]
        layers, _, ff = wg.shape
        tiles, slices = tokens // TM, ff // FS
        x, dy = x.reshape(tiles, TM, d), dy.reshape(tiles, TM, d)
        hbm = pl.BlockSpec(memory_space=pl.ANY)
        half, rows = n // 2, (d + FS) // n
        mm = 2 * tokens * d * ff
        sums, *far, _ = pl.pallas_call(
            functools.partial(train_kernel, n),
            in_specs=[hbm] * 5,
            out_specs=[hbm] * 4,
            out_shape=[jax.ShapeDtypeStruct((layers * slices, n, rows, d), BF16)]
            + [jax.ShapeDtypeStruct((4, slices, rows // 2, d), BF16)] * 2
            + [jax.ShapeDtypeStruct((tiles, TM, 2 * ff), BF16)],
            scratch_shapes=[
                pltpu.VMEM((layers, d, 2 * ff), BF16),
                pltpu.VMEM((layers, slices, FS, d), BF16),
                pltpu.VMEM((tiles, TM, d), BF16),
                pltpu.VMEM((tiles, TM, d), BF16),
                pltpu.VMEM((tiles, d, TM), BF16),
                pltpu.VMEM((tiles, TM, d), BF16),
                pltpu.VMEM((tiles, d, TM), BF16),
                pltpu.VMEM((tiles, TM, d), BF16),
                pltpu.VMEM((2, TM, 2 * ff), BF16),
                pltpu.VMEM((TM, ff), BF16),
                pltpu.VMEM((PAIR, TM, 3 * FS), BF16),
                pltpu.VMEM((PAIR, TM, 3 * FS), BF16),
                pltpu.VMEM((d, 2 * FS), F32),
                pltpu.VMEM((d, FS), F32),
                pltpu.VMEM((SLOTS, n, rows, d), BF16),
                pltpu.VMEM((SLOTS, half, 2, rows, d), BF16),
                pltpu.VMEM((SLOTS, n, rows, d), BF16),
                pltpu.SemaphoreType.DMA((tiles + 1,)),
                pltpu.SemaphoreType.DMA((layers, slices, 3)),
                pltpu.SemaphoreType.DMA((2,)),
                pltpu.SemaphoreType.DMA((2,)),
                pltpu.SemaphoreType.DMA((SLOTS, 2 * half - 2, 2)),
                pltpu.SemaphoreType.DMA((SLOTS, 2 * half - 2, 2)),
                pltpu.SemaphoreType.DMA((SLOTS, n + 1)),
                pltpu.SemaphoreType.DMA((SLOTS, 2)),
                pltpu.SemaphoreType.DMA((SLOTS, 2)),
            ],
            compiler_params=pltpu.CompilerParams(vmem_limit_bytes=VMEM_LIMIT, collective_id=0, has_side_effects=True),
            cost_estimate=pl.CostEstimate(flops=17 * mm, bytes_accessed=90 * 10**6, transcendentals=0),
        )(x, dy, wg, wu, wd)
        chunks = [a.reshape(layers, n, d // n, ff) if a.shape[1] == d else a.reshape(layers, slices, n, FS // n, d) for a in arrays]
        ways = ([(i, (i + n - 1) % n) for i in range(n)], [(i, (i + 1) % n) for i in range(n)])
        first, second = range(layers)
        kept = half - 2
        here = {
            l: [(l, offset, part, 0, offset + n) for offset in range(-kept, kept + 1) for part in (0, 1)] for l in (first, second)
        }
        near, last = [], []
        for way in (0, 1):
            near.append(lax.ppermute(far[way], "dp", ways[way]))
        steps = here[second] + [(second, kept + 1, 0, 1, 3), (second, -kept - 1, 1, 2, 3)] + here[first]
        new = adam(n, steps, [sums, *far], chunks, None, 60_000_000)
        for way in (0, 1):
            last.append(lax.ppermute(near[way][0], "dp", ways[way]))
        steps = []
        for way, sign in ((0, 1), (1, -1)):
            steps += [(first, sign * (kept + 1), way, way, 0), (first, sign * (kept + 1), 1 - way, way, 1)]
            steps += [(second, sign * (kept + 1), 1 - way, way, 2), (second, sign * half, way, way, 3)]
        new = adam(n, steps, near, chunks, new, 52_000_000)
        new = adam(n, [(first, half, 0, 0, 0), (first, -half, 1, 1, 0)], [a[None] for a in last], chunks, new, 60_000_000)
        return tuple(o.reshape(a.shape) for o, a in zip(new, arrays))

    return jax.shard_map(
        step,
        mesh=mesh,
        in_specs=(P(("rep", "dp"), None, None),) * 2 + (P(None, None, None),) * 9,
        out_specs=(P("rep", None, None),) * 9,
        check_vma=False,
    )
```

```python
import functools

import jax
import jax.numpy as jnp
from jax import lax
from jax.experimental import pallas as pl
from jax.experimental.pallas import tpu as pltpu
from jax.sharding import PartitionSpec as P


TM = 512
PAIR = 2
FS = 256
F32, BF16 = jnp.float32, jnp.bfloat16
VMEM_LIMIT = 67_000_000


def dot(a, b):
    return jnp.dot(a, b, preferred_element_type=F32)


def dot_t(a, b):
    return lax.dot_general(a, b, (((1,), (1,)), ((), ())), preferred_element_type=F32)


def scale_of(wide):
    return lax.rsqrt(jnp.mean(wide * wide, -1, keepdims=True) + 1e-6)


def normed(h):
    wide = h.astype(F32)
    return (wide * scale_of(wide)).astype(BF16)


def sigmoid(g):
    return 0.5 * jnp.tanh(0.5 * g) + 0.5


def forward_first(h, w_gu, act_ref, ready=lambda j: None):
    a = normed(h)
    for j in range(w_gu.shape[1] // (2 * FS)):
        ready(j)
        gu = dot(a, w_gu[:, 2 * j * FS : 2 * (j + 1) * FS])
        g, u = gu[:, :FS], gu[:, FS:]
        act_ref[:, j * FS : (j + 1) * FS] = (g * sigmoid(g) * u).astype(BF16)
    return a


def forward_second(h, w_d, act_ref):
    slices = w_d.shape[0]
    y = dot(act_ref[...], w_d[...].reshape(slices * FS, -1)).astype(BF16)
    return (h.astype(F32) + y.astype(F32)).astype(BF16)


def slice_first(a, dy, wgu, wd, buf):
    gu = dot(a, wgu)
    dact = dot_t(dy, wd)
    g, u = gu[:, :FS], gu[:, FS:]
    dact = dact.astype(BF16).astype(F32)
    s = sigmoid(g)
    silu = g * s
    shape = buf.shape[:2] + (FS,)
    buf[:, :, 2 * FS : 3 * FS] = (silu * u).astype(BF16).reshape(shape)
    buf[:, :, FS : 2 * FS] = (dact * silu).astype(BF16).reshape(shape)
    buf[:, :, :FS] = (dact * u * (s + silu * (1.0 - s))).astype(BF16).reshape(shape)


def slice_second(a_t, dy_t, buf, acc_gu, acc_d):
    acc_d[...] += sum(dot(dy_t[i], buf[i, :, 2 * FS : 3 * FS]) for i in range(PAIR))
    acc_gu[...] += sum(dot(a_t[i], buf[i, :, : 2 * FS]) for i in range(PAIR))


def norm_back(da, h, dy):
    d = h.shape[-1]
    da = da.astype(BF16).astype(F32)
    h = h.astype(F32)
    r = scale_of(h)
    along = jnp.sum(da * h, -1, keepdims=True)
    dh = (da * r - h * (along * r * r * r * (1.0 / d))).astype(BF16)
    return (dy.astype(F32) + dh.astype(F32)).astype(BF16)


class Ring:
    def __init__(self, n, own, got, out, sums, far, send, recv, out_sem):
        self.n, self.half, self.rows = n, n // 2, own.shape[2]
        self.kept = self.half - 2
        self.sends = self.half + self.kept
        self.own, self.got, self.out, self.sums, self.far = own, got, out, sums, far
        self.send, self.recv, self.out_sem = send, recv, out_sem
        self.me = lax.axis_index("dp")
        self.to = ({"dp": lax.rem(self.me + n - 1, n)}, {"dp": lax.rem(self.me + 1, n)})

    def chunk(self, way, offset):
        return lax.rem(self.me + (offset if way == 0 else -offset) + self.n, self.n)

    def part(self, way, halved):
        size = self.rows // 2 if halved else self.rows
        return pl.ds(size if halved and way == 1 else 0, size)

    def copy(self, slot, k, way):
        h = self.half
        rows = self.part(way, k == 0)
        chunk = self.chunk(way, k - h)
        if k < h:
            src = self.own.at[slot, chunk, rows]
            dst = self.got.at[slot, k, way, rows]
        else:
            src = dst = self.out.at[slot, chunk, rows]
        return pltpu.make_async_remote_copy(
            src_ref=src,
            dst_ref=dst,
            send_sem=self.send.at[slot, k, way],
            recv_sem=self.recv.at[slot, k, way],
            device_id=self.to[way],
            device_id_type=pl.DeviceIdType.MESH,
        )

    def write_out(self, slot, t):
        copies = []
        for offset in range(-self.kept, self.kept + 1):
            chunk = self.chunk(0, offset)
            copies.append((self.out.at[slot, chunk], self.sums.at[t, chunk]))
        for way in (0, 1):
            chunk = self.chunk(way, self.kept)
            for part in (0, 1):
                copies.append((self.out.at[slot, chunk, self.part(part, True)], self.far[2 * way + part].at[t]))
        return [pltpu.make_async_copy(a, b, self.out_sem.at[slot, i]) for i, (a, b) in enumerate(copies)]

    def event(self, slot, t, k):
        h = self.half
        if 0 < k <= self.sends:
            for way in (0, 1):
                self.copy(slot, k - 1, way).wait_recv()
        if 0 < k < h:
            for way in (0, 1):
                rows, chunk = self.part(way, k == 1), self.chunk(way, k - h)
                came = self.got[slot, k - 1, way, rows].astype(F32)
                self.own[slot, chunk, rows] = (self.own[slot, chunk, rows].astype(F32) + came).astype(BF16)
        if k == h:
            total = self.own[slot, self.me].astype(F32) + self.got[slot, h - 1, 0].astype(F32) + self.got[slot, h - 1, 1].astype(F32)
            self.out[slot, self.me] = total.astype(BF16)
        if k < self.sends:
            for way in (0, 1):
                self.copy(slot, k, way).start()
        if k == self.sends:
            for copy in self.write_out(slot, t):
                copy.start()
        for sent in range(h) if k == h else range(h, self.sends) if k == self.sends else ():
            for way in (0, 1):
                self.copy(slot, sent, way).wait_send()
        if k == self.sends + 1:
            for copy in self.write_out(slot, t):
                copy.wait()


SLOTS = 4
EVERY = 3


def train_kernel(n, x, dy, wg, wu, wd, sums, far0, far1, far2, far3, dgu, w_gu, w_d, a1, a2, at, dyv, dyt, h1, pulled, act, buf0, buf1,
                 acc_gu, acc_d, own, got, out, sem, wsem, push_sem, pull_sem, send, recv, out_sem):
    layers, slices = w_d.shape[:2]
    tiles = x.shape[0]
    total = layers * slices
    barrier = pltpu.get_barrier_semaphore()
    ring = Ring(n, own, got, out, sums, (far0, far1, far2, far3), send, recv, out_sem)
    for device in ring.to:
        pl.semaphore_signal(barrier, inc=1, device_id=device, device_id_type=pl.DeviceIdType.MESH)

    def columns(j):
        return pl.ds(pl.multiple_of(j * (2 * FS), 2 * FS), 2 * FS)

    def weights(l, j):
        return (
            pltpu.make_async_copy(wg.at[l, :, pl.ds(j * FS, FS)], w_gu.at[l, :, pl.ds(2 * j * FS, FS)], wsem.at[l, j, 0]),
            pltpu.make_async_copy(wu.at[l, :, pl.ds(j * FS, FS)], w_gu.at[l, :, pl.ds(2 * j * FS + FS, FS)], wsem.at[l, j, 1]),
            pltpu.make_async_copy(wd.at[l, pl.ds(j * FS, FS), :], w_d.at[l, j], wsem.at[l, j, 2]),
        )

    def state(m):
        return pltpu.make_async_copy(x.at[m], h1.at[m], sem.at[m])

    def cotangent(m):
        return pltpu.make_async_copy(dy.at[m], dyv.at[m], sem.at[tiles + m])

    state(0).start()
    for j in range(slices):
        for c in weights(0, j)[:2]:
            c.start()
    state(1).start()
    for j in range(slices):
        weights(0, j)[2].start()
    cotangent(0).start()
    for m in range(2, tiles):
        state(m).start()
        cotangent(m - 1).start()
    cotangent(tiles - 1).start()
    for j in range(slices):
        for c in weights(1, j):
            c.start()

    def forward_a(m, ready=lambda j: None):
        a1[m] = forward_first(h1[m], w_gu.at[0], act, ready)

    def forward_b(m):
        h = forward_second(h1[m], w_d.at[0], act)
        h1[m] = h
        a = normed(h)
        a2[m] = a
        at[m] = a.T
        dyt[m] = dyv[m].T

    def forward(m, _):
        state(m + 1).wait()
        cotangent(m).wait()
        forward_b(m)
        forward_a(m + 1)
        return 0

    def ready(j):
        for first, last in ((0, 2), (2, slices)):
            if j == first:
                for here in range(first, last):
                    for c in weights(0, here)[:2]:
                        c.wait()

    state(0).wait()
    forward_a(0, ready)
    for j in range(slices):
        weights(0, j)[2].wait()
    lax.fori_loop(0, tiles - 1, forward, 0)
    cotangent(tiles - 1).wait()
    forward_b(tiles - 1)
    for j in range(slices):
        for c in weights(1, j):
            c.wait()
    pl.semaphore_wait(barrier, 2)

    steps = tiles // PAIR
    turns = tiles // steps
    offsets = [1 + EVERY * k for k in range(ring.sends + 1)] + [3 + EVERY * ring.sends]

    def round_of(now):
        found = []
        for ago in range(1 + offsets[-1] // steps):
            place = now - 1 - ago
            t = jnp.where(place >= slices, place - turns, place)
            there = (place >= 0) & (t < total) & ((place < slices) | (t >= slices))
            found.append((there, t, lax.rem(t + SLOTS, SLOTS)))
        return found

    def events(found, u, odd=None):
        for k in reversed(range(len(offsets))):
            ago, at_step = divmod(offsets[k], steps)
            if odd is not None and at_step % 2 != odd:
                continue
            there, t, slot = found[ago]

            @pl.when((u == at_step) & there)
            def _():
                ring.event(slot, t, k)

    def finish(s):
        slot = lax.rem(s, SLOTS)
        wide = acc_gu.shape[0] // n
        own[slot, :, :wide] = acc_gu[...].astype(BF16).reshape(n, wide, 2 * FS)
        own[slot, :, wide:] = acc_d[...].T.astype(BF16).reshape(n, FS // n, -1)
        acc_gu[...] = jnp.zeros_like(acc_gu)
        acc_d[...] = jnp.zeros_like(acc_d)

    def push(u, j, i):
        return pltpu.make_async_copy(
            (buf0, buf1)[i].at[:, :, pl.ds(0, 2 * FS)], dgu.at[pl.ds(u * PAIR, PAIR), :, columns(j)], push_sem.at[i]
        )

    def pull(m):
        return pltpu.make_async_copy(dgu.at[m], pulled.at[lax.rem(m, 2)], pull_sem.at[lax.rem(m, 2)])

    def backward(l):
        second = l == layers - 1
        states = a2 if second else a1

        def slice_a(u, j, buf):
            here = pl.ds(u * PAIR, PAIR)
            rows = (PAIR * TM, dyv.shape[-1])
            slice_first(states[here].reshape(rows), dyv[here].reshape(rows), w_gu[l, :, columns(j)], w_d[l, j], buf)

        def slice_b(u, buf):
            here = pl.ds(u * PAIR, PAIR)
            slice_second(at.at[here], dyt.at[here], buf, acc_gu, acc_d)

        def one_slice(j, _):
            found = round_of(j if second else slices + turns + j)

            def two_steps(i, _):
                for half, here, there in ((0, buf0, buf1), (1, buf1, buf0)):
                    u = 2 * i + half
                    events(found, u, half)
                    if second:
                        @pl.when((i > 0) | (j > 0))
                        def _():
                            push(u, j, half).wait()

                    slice_a(u, j, here)
                    slice_b(lax.rem(u + steps - 1, steps), there)
                    if second:
                        push(u, j, half).start()
                    if half == 0:
                        @pl.when((i == 0) & (j > 0))
                        def _():
                            finish((0 if second else slices) + j - 1)

                return 0

            return lax.fori_loop(0, steps // 2, two_steps, 0)

        buf1[...] = jnp.zeros_like(buf1)
        lax.fori_loop(0, slices, one_slice, 0)
        if second:
            for m in (0, 1):
                pull(m).start()
        slice_b(steps - 1, buf1)
        finish((slices if second else total) - 1)

    def turn(m, _):
        events(round_of(slices + m // steps), lax.rem(m, steps))
        pull(m).wait()
        parts = 2
        size = TM // parts
        for part in range(parts):
            rows = pl.ds(part * size, size)
            da = dot_t(pulled[lax.rem(m, 2), rows], w_gu[layers - 1])
            back = norm_back(da, h1[m, rows], dyv[m, rows])
            dyv[m, rows] = back
            dyt[m, :, rows] = back.T
            at[m, :, rows] = a1[m, rows].T

        @pl.when(m + 2 < tiles)
        def _():
            pull(m + 2).start()

        return 0

    acc_gu[...] = jnp.zeros_like(acc_gu)
    acc_d[...] = jnp.zeros_like(acc_d)
    backward(layers - 1)
    for i in (0, 1):
        push(i, 0, i).wait()
    lax.fori_loop(0, tiles, turn, 0)
    backward(0)

    def drain(now, _):
        found = round_of(now)

        def one(u, _):
            events(found, u)
            return 0

        return lax.fori_loop(0, steps, one, 0)

    end = total + turns
    lax.fori_loop(end, end + 1 + offsets[-1] // steps, drain, 0)


def adam_math(w, m, v, g):
    m = 0.9 * m + 0.1 * g
    v = 0.95 * v + 0.05 * g * g
    step = m * lax.rsqrt(v + 1e-8) + 0.1 * w
    return (w - 0.02 * step).astype(BF16), m, v


def adam_kernel(sources, table, me, *refs):
    count = sum(sources)
    gs, ins, outs = list(refs[:count]), refs[count : count + 9], refs[-9:]
    which = table[pl.program_id(0), 2]
    slices, wide = ins[2].shape[1], ins[0].shape[2]
    for j in range(slices):
        g, place = None, 0
        for i, pieces in enumerate(sources):
            here = [r[j].reshape(r.shape[-2:]) for r in gs[place : place + pieces]]
            here = (here[0] if pieces == 1 else jnp.concatenate(here, axis=0)).astype(F32)
            g = here if g is None else jnp.where(which == i, here, g)
            place += pieces
        columns = slice(j * FS, (j + 1) * FS)
        for i, here in ((0, (0, 0, slice(None), columns)), (1, (0, 0, slice(None), columns)), (2, (0, j, 0))):
            part = (g[:wide, :FS], g[:wide, FS:], g[wide:])[i]
            w, m, v = (ins[k * 3 + i][here] for k in range(3))
            new = adam_math(w.astype(F32), m, v, part)
            for k in range(3):
                outs[k * 3 + i][here] = new[k]


def adam(n, steps, sources, arrays, so_far, vmem):
    layers, slices = arrays[0].shape[0], arrays[2].shape[1]
    blocks = [layers - 1 - steps[0][0]] * len(sources)
    table = []
    for layer, offset, source in steps:
        blocks[source] = layers - 1 - layer
        table.append([layer, offset + n, source] + blocks)
    table = jnp.array(table, jnp.int32)
    me = lax.axis_index("dp").astype(jnp.int32).reshape(1)

    def chunk(s, table, me):
        return lax.rem(me[0] + table[s, 1], n)

    def spec(i, g):
        if g.ndim == 3:
            return pl.BlockSpec((slices,) + g.shape[1:], lambda s, table, me: (table[s, 3 + i], 0, 0))
        return pl.BlockSpec((slices, 1) + g.shape[2:], lambda s, table, me: (table[s, 3 + i], chunk(s, table, me), 0, 0))

    wide = pl.BlockSpec((1, 1) + arrays[0].shape[2:], lambda s, table, me: (table[s, 0], chunk(s, table, me), 0, 0))
    tall = pl.BlockSpec((1, slices, 1) + arrays[2].shape[3:], lambda s, table, me: (table[s, 0], 0, chunk(s, table, me), 0, 0))
    specs = [wide, wide, tall] * 3
    gs = [g for source in sources for g in source]
    extra = [] if so_far is None else list(so_far)
    size = 2 * sum(a.size * a.dtype.itemsize for a in arrays) * len(steps) // (n * layers)
    return pl.pallas_call(
        functools.partial(adam_kernel, [len(source) for source in sources]),
        grid_spec=pltpu.PrefetchScalarGridSpec(
            num_scalar_prefetch=2,
            grid=(len(steps),),
            in_specs=[spec(i, g) for i, source in enumerate(sources) for g in source]
            + specs
            + [pl.BlockSpec(memory_space=pl.ANY)] * len(extra),
            out_specs=specs,
        ),
        out_shape=[jax.ShapeDtypeStruct(a.shape, a.dtype) for a in arrays],
        input_output_aliases={2 + len(gs) + 9 + i: i for i in range(len(extra))},
        compiler_params=pltpu.CompilerParams(vmem_limit_bytes=vmem),
        cost_estimate=pl.CostEstimate(flops=40 * size, bytes_accessed=size, transcendentals=0),
    )(table, me, *gs, *arrays, *extra)


def solution(mesh):
    n = mesh.shape["dp"]

    def step(x, dy, *arrays):
        wg, wu, wd = arrays[:3]
        tokens, d = x.shape[1:]
        layers, _, ff = wg.shape
        tiles, slices = tokens // TM, ff // FS
        x, dy = x.reshape(tiles, TM, d), dy.reshape(tiles, TM, d)
        hbm = pl.BlockSpec(memory_space=pl.ANY)
        half, rows = n // 2, (d + FS) // n
        mm = 2 * tokens * d * ff
        sums, *far, _ = pl.pallas_call(
            functools.partial(train_kernel, n),
            in_specs=[hbm] * 5,
            out_specs=[hbm] * 6,
            out_shape=[jax.ShapeDtypeStruct((layers * slices, n, rows, d), BF16)]
            + [jax.ShapeDtypeStruct((layers * slices, rows // 2, d), BF16)] * 4
            + [jax.ShapeDtypeStruct((tiles, TM, 2 * ff), BF16)],
            scratch_shapes=[
                pltpu.VMEM((layers, d, 2 * ff), BF16),
                pltpu.VMEM((layers, slices, FS, d), BF16),
                pltpu.VMEM((tiles, TM, d), BF16),
                pltpu.VMEM((tiles, TM, d), BF16),
                pltpu.VMEM((tiles, d, TM), BF16),
                pltpu.VMEM((tiles, TM, d), BF16),
                pltpu.VMEM((tiles, d, TM), BF16),
                pltpu.VMEM((tiles, TM, d), BF16),
                pltpu.VMEM((2, TM, 2 * ff), BF16),
                pltpu.VMEM((TM, ff), BF16),
                pltpu.VMEM((PAIR, TM, 3 * FS), BF16),
                pltpu.VMEM((PAIR, TM, 3 * FS), BF16),
                pltpu.VMEM((d, 2 * FS), F32),
                pltpu.VMEM((d, FS), F32),
                pltpu.VMEM((SLOTS, n, rows, d), BF16),
                pltpu.VMEM((SLOTS, half, 2, rows, d), BF16),
                pltpu.VMEM((SLOTS, n, rows, d), BF16),
                pltpu.SemaphoreType.DMA((2 * tiles,)),
                pltpu.SemaphoreType.DMA((layers, slices, 3)),
                pltpu.SemaphoreType.DMA((2,)),
                pltpu.SemaphoreType.DMA((2,)),
                pltpu.SemaphoreType.DMA((SLOTS, 2 * half - 2, 2)),
                pltpu.SemaphoreType.DMA((SLOTS, 2 * half - 2, 2)),
                pltpu.SemaphoreType.DMA((SLOTS, n + 1)),
            ],
            compiler_params=pltpu.CompilerParams(vmem_limit_bytes=VMEM_LIMIT, collective_id=0, has_side_effects=True),
            cost_estimate=pl.CostEstimate(flops=17 * mm, bytes_accessed=90 * 10**6, transcendentals=0),
        )(x, dy, wg, wu, wd)
        chunks = [a.reshape(layers, n, d // n, ff) if a.shape[1] == d else a.reshape(layers, slices, n, FS // n, d) for a in arrays]
        left = [(i, (i + n - 1) % n) for i in range(n)]
        right = [(i, (i + 1) % n) for i in range(n)]

        first, second = range(layers)
        kept = half - 2
        big, small = 60_000_000, 52_000_000
        near, last = [None] * 4, []
        for i, way in ((0, left), (3, right), (1, left), (2, right)):
            near[i] = lax.ppermute(far[i], "dp", way)
        new = adam(n, [(second, o, 0) for o in range(-kept, kept + 1)], [[sums]], chunks, None, big)
        for i, way in ((0, left), (3, right)):
            last.append(lax.ppermute(near[i], "dp", way))
        new = adam(n, [(first, o, 0) for o in range(-kept, kept + 1)], [[sums]], chunks, new, big)
        steps = [(l, sign * (kept + 1), way) for way, sign in ((0, 1), (1, -1)) for l in (second, first)]
        new = adam(n, steps, [near[:2], near[2:]], chunks, new, small)
        new = adam(n, [(second, half, 0), (first, half, 0)], [last], chunks, new, big)
        return tuple(o.reshape(a.shape) for o, a in zip(new, arrays))

    return jax.shard_map(
        step,
        mesh=mesh,
        in_specs=(P(("rep", "dp"), None, None),) * 2 + (P(None, None, None),) * 9,
        out_specs=(P("rep", None, None),) * 9,
        check_vma=False,
    )
```

```python
import functools

import jax
import jax.numpy as jnp
from jax import lax
from jax.experimental import pallas as pl
from jax.experimental.pallas import tpu as pltpu
from jax.sharding import PartitionSpec as P


TM = 512
PAIR = 2
FS = 256
F32, BF16 = jnp.float32, jnp.bfloat16
VMEM_LIMIT = 67_000_000


def dot(a, b):
    return jnp.dot(a, b, preferred_element_type=F32)


def dot_t(a, b):
    return lax.dot_general(a, b, (((1,), (1,)), ((), ())), preferred_element_type=F32)


def scale_of(wide):
    return lax.rsqrt(jnp.mean(wide * wide, -1, keepdims=True) + 1e-6)


def normed(h):
    wide = h.astype(F32)
    return (wide * scale_of(wide)).astype(BF16)


def sigmoid(g):
    return 0.5 * jnp.tanh(0.5 * g) + 0.5


def forward_first(h, w_gu, act_ref, ready=lambda j: None):
    a = normed(h)
    for j in range(w_gu.shape[1] // (2 * FS)):
        ready(j)
        gu = dot(a, w_gu[:, 2 * j * FS : 2 * (j + 1) * FS])
        g, u = gu[:, :FS], gu[:, FS:]
        act_ref[:, j * FS : (j + 1) * FS] = (g * sigmoid(g) * u).astype(BF16)
    return a


def forward_second(h, w_d, act_ref):
    slices = w_d.shape[0]
    y = dot(act_ref[...], w_d[...].reshape(slices * FS, -1)).astype(BF16)
    return (h.astype(F32) + y.astype(F32)).astype(BF16)


def slice_first(a, dy, wgu, wd, buf):
    gu = dot(a, wgu)
    dact = dot_t(dy, wd)
    g, u = gu[:, :FS], gu[:, FS:]
    dact = dact.astype(BF16).astype(F32)
    s = sigmoid(g)
    silu = g * s
    shape = buf.shape[:2] + (FS,)
    buf[:, :, 2 * FS : 3 * FS] = (silu * u).astype(BF16).reshape(shape)
    buf[:, :, FS : 2 * FS] = (dact * silu).astype(BF16).reshape(shape)
    buf[:, :, :FS] = (dact * u * (s + silu * (1.0 - s))).astype(BF16).reshape(shape)


def slice_second(a_t, dy_t, buf, acc_gu, acc_d):
    acc_d[...] += sum(dot(dy_t[i], buf[i, :, 2 * FS : 3 * FS]) for i in range(PAIR))
    acc_gu[...] += sum(dot(a_t[i], buf[i, :, : 2 * FS]) for i in range(PAIR))


def norm_back(da, h, dy):
    d = h.shape[-1]
    da = da.astype(BF16).astype(F32)
    h = h.astype(F32)
    r = scale_of(h)
    along = jnp.sum(da * h, -1, keepdims=True)
    dh = (da * r - h * (along * r * r * r * (1.0 / d))).astype(BF16)
    return (dy.astype(F32) + dh.astype(F32)).astype(BF16)


class Ring:
    def __init__(self, n, own, got, out, sums, far, send, recv, out_sem):
        self.n, self.half, self.rows = n, n // 2, own.shape[2]
        self.kept = self.half - 2
        self.sends = self.half + self.kept
        self.own, self.got, self.out, self.sums, self.far = own, got, out, sums, far
        self.send, self.recv, self.out_sem = send, recv, out_sem
        self.me = lax.axis_index("dp")
        self.to = ({"dp": lax.rem(self.me + n - 1, n)}, {"dp": lax.rem(self.me + 1, n)})

    def chunk(self, way, offset):
        return lax.rem(self.me + (offset if way == 0 else -offset) + self.n, self.n)

    def part(self, way, halved):
        size = self.rows // 2 if halved else self.rows
        return pl.ds(size if halved and way == 1 else 0, size)

    def copy(self, slot, k, way):
        h = self.half
        rows = self.part(way, k == 0)
        chunk = self.chunk(way, k - h)
        if k < h:
            src = self.own.at[slot, chunk, rows]
            dst = self.got.at[slot, k, way, rows]
        else:
            src = dst = self.out.at[slot, chunk, rows]
        return pltpu.make_async_remote_copy(
            src_ref=src,
            dst_ref=dst,
            send_sem=self.send.at[slot, k, way],
            recv_sem=self.recv.at[slot, k, way],
            device_id=self.to[way],
            device_id_type=pl.DeviceIdType.MESH,
        )

    def write_out(self, slot, t):
        copies = []
        for offset in range(-self.kept, self.kept + 1):
            chunk = self.chunk(0, offset)
            copies.append((self.out.at[slot, chunk], self.sums.at[t, chunk]))
        for way in (0, 1):
            chunk = self.chunk(way, self.kept)
            for place, part in ((0, way), (1, 1 - way)):
                copies.append((self.out.at[slot, chunk, self.part(part, True)], self.far[way].at[place, t]))
        return [pltpu.make_async_copy(a, b, self.out_sem.at[slot, i]) for i, (a, b) in enumerate(copies)]

    def event(self, slot, t, k):
        h = self.half
        if 0 < k <= self.sends:
            for way in (0, 1):
                self.copy(slot, k - 1, way).wait_recv()
        if 0 < k < h:
            for way in (0, 1):
                rows, chunk = self.part(way, k == 1), self.chunk(way, k - h)
                came = self.got[slot, k - 1, way, rows].astype(F32)
                self.own[slot, chunk, rows] = (self.own[slot, chunk, rows].astype(F32) + came).astype(BF16)
        if k == h:
            total = self.own[slot, self.me].astype(F32) + self.got[slot, h - 1, 0].astype(F32) + self.got[slot, h - 1, 1].astype(F32)
            self.out[slot, self.me] = total.astype(BF16)
        if k < self.sends:
            for way in (0, 1):
                self.copy(slot, k, way).start()
        if k == self.sends:
            for copy in self.write_out(slot, t):
                copy.start()
        for sent in range(h) if k == h else range(h, self.sends) if k == self.sends else ():
            for way in (0, 1):
                self.copy(slot, sent, way).wait_send()
        if k == self.sends + 1:
            for copy in self.write_out(slot, t):
                copy.wait()


SLOTS = 4
EVERY = 3


def train_kernel(n, x, dy, wg, wu, wd, sums, far0, far1, dgu, w_gu, w_d, a1, a2, at, dyv, dyt, h1, pulled, act, buf0, buf1,
                 acc_gu, acc_d, own, got, out, sem, wsem, push_sem, pull_sem, send, recv, out_sem):
    layers, slices = w_d.shape[:2]
    tiles = x.shape[0]
    total = layers * slices
    barrier = pltpu.get_barrier_semaphore()
    ring = Ring(n, own, got, out, sums, (far0, far1), send, recv, out_sem)
    for device in ring.to:
        pl.semaphore_signal(barrier, inc=1, device_id=device, device_id_type=pl.DeviceIdType.MESH)

    def columns(j):
        return pl.ds(pl.multiple_of(j * (2 * FS), 2 * FS), 2 * FS)

    def weights(l, j):
        return (
            pltpu.make_async_copy(wg.at[l, :, pl.ds(j * FS, FS)], w_gu.at[l, :, pl.ds(2 * j * FS, FS)], wsem.at[l, j, 0]),
            pltpu.make_async_copy(wu.at[l, :, pl.ds(j * FS, FS)], w_gu.at[l, :, pl.ds(2 * j * FS + FS, FS)], wsem.at[l, j, 1]),
            pltpu.make_async_copy(wd.at[l, pl.ds(j * FS, FS), :], w_d.at[l, j], wsem.at[l, j, 2]),
        )

    def state(m):
        return pltpu.make_async_copy(x.at[m], h1.at[m], sem.at[m])

    def cotangent(m):
        return pltpu.make_async_copy(dy.at[m], dyv.at[m], sem.at[tiles + m])

    state(0).start()
    for j in range(slices):
        for c in weights(0, j)[:2]:
            c.start()
    state(1).start()
    for j in range(slices):
        weights(0, j)[2].start()
    cotangent(0).start()
    for m in range(2, tiles):
        state(m).start()
        cotangent(m - 1).start()
    cotangent(tiles - 1).start()
    for j in range(slices):
        for c in weights(1, j):
            c.start()

    def forward_a(m, ready=lambda j: None):
        a1[m] = forward_first(h1[m], w_gu.at[0], act, ready)

    def forward_b(m):
        h = forward_second(h1[m], w_d.at[0], act)
        h1[m] = h
        a = normed(h)
        a2[m] = a
        at[m] = a.T
        dyt[m] = dyv[m].T

    def forward(m, _):
        state(m + 1).wait()
        cotangent(m).wait()
        forward_b(m)
        forward_a(m + 1)
        return 0

    def ready(j):
        for first, last in ((0, 2), (2, slices)):
            if j == first:
                for here in range(first, last):
                    for c in weights(0, here)[:2]:
                        c.wait()

    state(0).wait()
    forward_a(0, ready)
    for j in range(slices):
        weights(0, j)[2].wait()
    lax.fori_loop(0, tiles - 1, forward, 0)
    cotangent(tiles - 1).wait()
    forward_b(tiles - 1)
    for j in range(slices):
        for c in weights(1, j):
            c.wait()
    pl.semaphore_wait(barrier, 2)

    steps = tiles // PAIR
    turns = tiles // steps
    offsets = [1 + EVERY * k for k in range(ring.sends + 1)] + [3 + EVERY * ring.sends]

    def round_of(now):
        found = []
        for ago in range(1 + offsets[-1] // steps):
            place = now - 1 - ago
            t = jnp.where(place >= slices, place - turns, place)
            there = (place >= 0) & (t < total) & ((place < slices) | (t >= slices))
            found.append((there, t, lax.rem(t + SLOTS, SLOTS)))
        return found

    def events(found, u, odd=None):
        for k in reversed(range(len(offsets))):
            ago, at_step = divmod(offsets[k], steps)
            if odd is not None and at_step % 2 != odd:
                continue
            there, t, slot = found[ago]

            @pl.when((u == at_step) & there)
            def _():
                ring.event(slot, t, k)

    def finish(s):
        slot = lax.rem(s, SLOTS)
        wide = acc_gu.shape[0] // n
        own[slot, :, :wide] = acc_gu[...].astype(BF16).reshape(n, wide, 2 * FS)
        own[slot, :, wide:] = acc_d[...].T.astype(BF16).reshape(n, FS // n, -1)
        acc_gu[...] = jnp.zeros_like(acc_gu)
        acc_d[...] = jnp.zeros_like(acc_d)

    def push(u, j, i):
        return pltpu.make_async_copy(
            (buf0, buf1)[i].at[:, :, pl.ds(0, 2 * FS)], dgu.at[pl.ds(u * PAIR, PAIR), :, columns(j)], push_sem.at[i]
        )

    def pull(m):
        return pltpu.make_async_copy(dgu.at[m], pulled.at[lax.rem(m, 2)], pull_sem.at[lax.rem(m, 2)])

    def backward(l):
        second = l == layers - 1
        states = a2 if second else a1

        def slice_a(u, j, buf):
            here = pl.ds(u * PAIR, PAIR)
            rows = (PAIR * TM, dyv.shape[-1])
            slice_first(states[here].reshape(rows), dyv[here].reshape(rows), w_gu[l, :, columns(j)], w_d[l, j], buf)

        def slice_b(u, buf):
            here = pl.ds(u * PAIR, PAIR)
            slice_second(at.at[here], dyt.at[here], buf, acc_gu, acc_d)

        def one_slice(j, _):
            found = round_of(j if second else slices + turns + j)

            def two_steps(i, _):
                for half, here, there in ((0, buf0, buf1), (1, buf1, buf0)):
                    u = 2 * i + half
                    events(found, u, half)
                    if second:
                        @pl.when((i > 0) | (j > 0))
                        def _():
                            push(u, j, half).wait()

                    slice_a(u, j, here)
                    slice_b(lax.rem(u + steps - 1, steps), there)
                    if second:
                        push(u, j, half).start()
                    if half == 0:
                        @pl.when((i == 0) & (j > 0))
                        def _():
                            finish((0 if second else slices) + j - 1)

                return 0

            return lax.fori_loop(0, steps // 2, two_steps, 0)

        buf1[...] = jnp.zeros_like(buf1)
        lax.fori_loop(0, slices, one_slice, 0)
        if second:
            for m in (0, 1):
                pull(m).start()
        slice_b(steps - 1, buf1)
        finish((slices if second else total) - 1)

    def turn(m, _):
        events(round_of(slices + m // steps), lax.rem(m, steps))
        pull(m).wait()
        parts = 2
        size = TM // parts
        for part in range(parts):
            rows = pl.ds(part * size, size)
            da = dot_t(pulled[lax.rem(m, 2), rows], w_gu[layers - 1])
            back = norm_back(da, h1[m, rows], dyv[m, rows])
            dyv[m, rows] = back
            dyt[m, :, rows] = back.T
            at[m, :, rows] = a1[m, rows].T

        @pl.when(m + 2 < tiles)
        def _():
            pull(m + 2).start()

        return 0

    acc_gu[...] = jnp.zeros_like(acc_gu)
    acc_d[...] = jnp.zeros_like(acc_d)
    backward(layers - 1)
    for i in (0, 1):
        push(i, 0, i).wait()
    lax.fori_loop(0, tiles, turn, 0)
    backward(0)

    left = {}
    for t in range(total):
        start = steps * (t + 1 + (turns if t >= slices else 0))
        late = [(k, start + offset - steps * (total + turns)) for k, offset in enumerate(offsets)]
        late = [(k, at) for k, at in late if at >= 0]
        if late:
            left[t] = late[0]
    for t, k in drain_order(left, ring.half, ring.sends):
        ring.event(t % SLOTS, t, k)


def drain_order(left, half, sends):
    step, beyond, now, wire, order = 0.92, 1.3, 0.0, 1.0, []
    ready = {t: 0.0 if k == 0 else max(0.0, (at - EVERY) * step + 1 + beyond) for t, (k, at) in left.items()}
    todo = {t: k for t, (k, _) in left.items()}
    while todo:
        can = [t for t, k in todo.items() if k < half - 1 or t - SLOTS not in todo]
        rank = {t: (todo[t] if todo[t] <= sends else -1 if t + SLOTS in todo else sends + 1, -t) for t in can}
        arrived = [t for t in can if ready[t] <= now]
        t = min(arrived, key=lambda t: rank[t]) if arrived else min(can, key=lambda t: (ready[t], rank[t]))
        k = todo[t]
        now = max(now, ready[t]) + 0.05
        order.append((t, k))
        if k < sends:
            wire = max(wire, now) + (0.5 if k == 0 else 1.0)
        ready[t] = wire + beyond if k < sends else now + 0.5
        todo[t] = k + 1
        if k > sends:
            del todo[t]
    return order


def adam_math(w, m, v, g):
    m = 0.9 * m + 0.1 * g
    v = 0.95 * v + 0.05 * g * g
    step = m * lax.rsqrt(v + 1e-8) + 0.1 * w
    return (w - 0.02 * step).astype(BF16), m, v


def adam_kernel(pieces, me, *refs):
    gs, ins, outs = refs[:pieces], refs[pieces : pieces + 9], refs[-9:]
    slices, wide = ins[2].shape[1], ins[0].shape[2]
    for j in range(slices):
        g = [(r[j] if r.shape[0] == slices else r[0, j]).reshape(r.shape[-2:]) for r in gs]
        g = [g[0] if pieces == 1 else jnp.concatenate(g[i : i + 2], axis=0) for i in range(0, pieces, 2)]
        g = [part.astype(F32) for part in g]
        g = g[0] if len(g) == 1 else jnp.where(pl.program_id(1) == 0, g[0], g[1])
        columns = slice(j * FS, (j + 1) * FS)
        for i, here in ((0, (0, 0, slice(None), columns)), (1, (0, 0, slice(None), columns)), (2, (0, j, 0))):
            part = (g[:wide, :FS], g[:wide, FS:], g[wide:])[i]
            w, m, v = (ins[k * 3 + i][here] for k in range(3))
            new = adam_math(w.astype(F32), m, v, part)
            for k in range(3):
                outs[k * 3 + i][here] = new[k]


def adam(n, first, stride, count, gs, arrays, so_far, vmem):
    layers, slices = arrays[0].shape[0], arrays[2].shape[1]
    me = lax.axis_index("dp").astype(jnp.int32).reshape(1)

    def chunk(o, me):
        return lax.rem(me[0] + o * stride + (first + n), n)

    def spec(g, place):
        if g.shape[1] == n:
            return pl.BlockSpec((slices, 1) + g.shape[2:], lambda l, o, me: (layers - 1 - l, chunk(o, me), 0, 0))
        if g.ndim == 3:
            return pl.BlockSpec((slices,) + g.shape[1:], lambda l, o, me: (layers - 1 - l, 0, 0))
        return pl.BlockSpec((1, slices) + g.shape[2:], lambda l, o, me: (place, layers - 1 - l, 0, 0))

    wide = pl.BlockSpec((1, 1) + arrays[0].shape[2:], lambda l, o, me: (l, chunk(o, me), 0, 0))
    tall = pl.BlockSpec((1, slices, 1) + arrays[2].shape[3:], lambda l, o, me: (l, 0, chunk(o, me), 0, 0))
    specs = [wide, wide, tall] * 3
    extra = [] if so_far is None else list(so_far)
    size = 2 * sum(a.size * a.dtype.itemsize for a in arrays) * count // n
    return pl.pallas_call(
        functools.partial(adam_kernel, len(gs)),
        grid_spec=pltpu.PrefetchScalarGridSpec(
            num_scalar_prefetch=1,
            grid=(layers, count),
            in_specs=[spec(g, place) for g, place in gs] + specs + [pl.BlockSpec(memory_space=pl.ANY)] * len(extra),
            out_specs=specs,
        ),
        out_shape=[jax.ShapeDtypeStruct(a.shape, a.dtype) for a in arrays],
        input_output_aliases={1 + len(gs) + 9 + i: i for i in range(len(extra))},
        compiler_params=pltpu.CompilerParams(vmem_limit_bytes=vmem),
        cost_estimate=pl.CostEstimate(flops=40 * size, bytes_accessed=size, transcendentals=0),
    )(me, *[g for g, _ in gs], *arrays, *extra)


def solution(mesh):
    n = mesh.shape["dp"]

    def step(x, dy, *arrays):
        wg, wu, wd = arrays[:3]
        tokens, d = x.shape[1:]
        layers, _, ff = wg.shape
        tiles, slices = tokens // TM, ff // FS
        x, dy = x.reshape(tiles, TM, d), dy.reshape(tiles, TM, d)
        hbm = pl.BlockSpec(memory_space=pl.ANY)
        half, rows = n // 2, (d + FS) // n
        mm = 2 * tokens * d * ff
        sums, *far, _ = pl.pallas_call(
            functools.partial(train_kernel, n),
            in_specs=[hbm] * 5,
            out_specs=[hbm] * 4,
            out_shape=[jax.ShapeDtypeStruct((layers * slices, n, rows, d), BF16)]
            + [jax.ShapeDtypeStruct((2, layers * slices, rows // 2, d), BF16)] * 2
            + [jax.ShapeDtypeStruct((tiles, TM, 2 * ff), BF16)],
            scratch_shapes=[
                pltpu.VMEM((layers, d, 2 * ff), BF16),
                pltpu.VMEM((layers, slices, FS, d), BF16),
                pltpu.VMEM((tiles, TM, d), BF16),
                pltpu.VMEM((tiles, TM, d), BF16),
                pltpu.VMEM((tiles, d, TM), BF16),
                pltpu.VMEM((tiles, TM, d), BF16),
                pltpu.VMEM((tiles, d, TM), BF16),
                pltpu.VMEM((tiles, TM, d), BF16),
                pltpu.VMEM((2, TM, 2 * ff), BF16),
                pltpu.VMEM((TM, ff), BF16),
                pltpu.VMEM((PAIR, TM, 3 * FS), BF16),
                pltpu.VMEM((PAIR, TM, 3 * FS), BF16),
                pltpu.VMEM((d, 2 * FS), F32),
                pltpu.VMEM((d, FS), F32),
                pltpu.VMEM((SLOTS, n, rows, d), BF16),
                pltpu.VMEM((SLOTS, half, 2, rows, d), BF16),
                pltpu.VMEM((SLOTS, n, rows, d), BF16),
                pltpu.SemaphoreType.DMA((2 * tiles,)),
                pltpu.SemaphoreType.DMA((layers, slices, 3)),
                pltpu.SemaphoreType.DMA((2,)),
                pltpu.SemaphoreType.DMA((2,)),
                pltpu.SemaphoreType.DMA((SLOTS, 2 * half - 2, 2)),
                pltpu.SemaphoreType.DMA((SLOTS, 2 * half - 2, 2)),
                pltpu.SemaphoreType.DMA((SLOTS, n + 1)),
            ],
            compiler_params=pltpu.CompilerParams(vmem_limit_bytes=VMEM_LIMIT, collective_id=0, has_side_effects=True),
            cost_estimate=pl.CostEstimate(flops=17 * mm, bytes_accessed=90 * 10**6, transcendentals=0),
        )(x, dy, wg, wu, wd)
        chunks = [a.reshape(layers, n, d // n, ff) if a.shape[1] == d else a.reshape(layers, slices, n, FS // n, d) for a in arrays]
        left = [(i, (i + n - 1) % n) for i in range(n)]
        right = [(i, (i + 1) % n) for i in range(n)]

        kept = half - 2
        near, last = [], []
        for i, way in enumerate((left, right)):
            near.append(lax.ppermute(far[i], "dp", way))
        new = adam(n, -kept, 1, 2 * kept + 1, [(sums, 0)], chunks, None, 60_000_000)
        for i, way in enumerate((left, right)):
            last.append(lax.ppermute(near[i][0], "dp", way))
        sides = [(near[0], 0), (near[0], 1), (near[1], 1), (near[1], 0)]
        new = adam(n, kept + 1, -2 * (kept + 1), 2, sides, chunks, new, 52_000_000)
        new = adam(n, half, 1, 1, [(a, 0) for a in last], chunks, new, 60_000_000)
        return tuple(o.reshape(a.shape) for o, a in zip(new, arrays))

    return jax.shard_map(
        step,
        mesh=mesh,
        in_specs=(P(("rep", "dp"), None, None),) * 2 + (P(None, None, None),) * 9,
        out_specs=(P("rep", None, None),) * 9,
        check_vma=False,
    )
```

```python
import functools

import jax
import jax.numpy as jnp
from jax import lax
from jax.experimental import pallas as pl
from jax.experimental.pallas import tpu as pltpu
from jax.sharding import PartitionSpec as P


TM = 512
PAIR = 2
FS = 256
F32, BF16 = jnp.float32, jnp.bfloat16
VMEM_LIMIT = 67_000_000


def dot(a, b):
    return jnp.dot(a, b, preferred_element_type=F32)


def dot_t(a, b):
    return lax.dot_general(a, b, (((1,), (1,)), ((), ())), preferred_element_type=F32)


def scale_of(wide):
    return lax.rsqrt(jnp.mean(wide * wide, -1, keepdims=True) + 1e-6)


def normed(h):
    wide = h.astype(F32)
    return (wide * scale_of(wide)).astype(BF16)


def sigmoid(g):
    return 0.5 * jnp.tanh(0.5 * g) + 0.5


def forward_first(h, w_gu, act_ref, ready=lambda j: None):
    a = normed(h)
    for j in range(w_gu.shape[1] // (2 * FS)):
        ready(j)
        gu = dot(a, w_gu[:, 2 * j * FS : 2 * (j + 1) * FS])
        g, u = gu[:, :FS], gu[:, FS:]
        act_ref[:, j * FS : (j + 1) * FS] = (g * sigmoid(g) * u).astype(BF16)
    return a


def forward_second(h, w_d, act_ref):
    slices = w_d.shape[0]
    y = dot(act_ref[...], w_d[...].reshape(slices * FS, -1)).astype(BF16)
    return (h.astype(F32) + y.astype(F32)).astype(BF16)


def slice_first(a, dy, wgu, wd, buf):
    gu = dot(a, wgu)
    dact = dot_t(dy, wd)
    g, u = gu[:, :FS], gu[:, FS:]
    dact = dact.astype(BF16).astype(F32)
    s = sigmoid(g)
    silu = g * s
    shape = buf.shape[:2] + (FS,)
    buf[:, :, 2 * FS : 3 * FS] = (silu * u).astype(BF16).reshape(shape)
    buf[:, :, FS : 2 * FS] = (dact * silu).astype(BF16).reshape(shape)
    buf[:, :, :FS] = (dact * u * (s + silu * (1.0 - s))).astype(BF16).reshape(shape)


def slice_second(a_t, dy_t, buf, acc_gu, acc_d):
    acc_d[...] += sum(dot(dy_t[i], buf[i, :, 2 * FS : 3 * FS]) for i in range(PAIR))
    acc_gu[...] += sum(dot(a_t[i], buf[i, :, : 2 * FS]) for i in range(PAIR))


def norm_back(da, h, dy):
    d = h.shape[-1]
    da = da.astype(BF16).astype(F32)
    h = h.astype(F32)
    r = scale_of(h)
    along = jnp.sum(da * h, -1, keepdims=True)
    dh = (da * r - h * (along * r * r * r * (1.0 / d))).astype(BF16)
    return (dy.astype(F32) + dh.astype(F32)).astype(BF16)


class Ring:
    def __init__(self, n, own, got, out, sums, far, send, recv, out_sem):
        self.n, self.half, self.rows = n, n // 2, own.shape[2]
        self.kept = self.half - 2
        self.sends = self.half + self.kept
        self.own, self.got, self.out, self.sums, self.far = own, got, out, sums, far
        self.send, self.recv, self.out_sem = send, recv, out_sem
        self.me = lax.axis_index("dp")
        self.to = ({"dp": lax.rem(self.me + n - 1, n)}, {"dp": lax.rem(self.me + 1, n)})

    def chunk(self, way, offset):
        return lax.rem(self.me + (offset if way == 0 else -offset) + self.n, self.n)

    def part(self, way, halved):
        size = self.rows // 2 if halved else self.rows
        return pl.ds(size if halved and way == 1 else 0, size)

    def copy(self, slot, k, way):
        h = self.half
        rows = self.part(way, k == 0)
        chunk = self.chunk(way, k - h)
        if k < h:
            src = self.own.at[slot, chunk, rows]
            dst = self.got.at[slot, k, way, rows]
        else:
            src = dst = self.out.at[slot, chunk, rows]
        return pltpu.make_async_remote_copy(
            src_ref=src,
            dst_ref=dst,
            send_sem=self.send.at[slot, k, way],
            recv_sem=self.recv.at[slot, k, way],
            device_id=self.to[way],
            device_id_type=pl.DeviceIdType.MESH,
        )

    def write_out(self, slot, t):
        copies = []
        for offset in range(-self.kept, self.kept + 1):
            chunk = self.chunk(0, offset)
            copies.append((self.out.at[slot, chunk], self.sums.at[t, chunk]))
        for way in (0, 1):
            chunk = self.chunk(way, self.kept)
            for place, part in ((0, way), (1, 1 - way)):
                copies.append((self.out.at[slot, chunk, self.part(part, True)], self.far[way].at[place, t]))
        return [pltpu.make_async_copy(a, b, self.out_sem.at[slot, i]) for i, (a, b) in enumerate(copies)]

    def event(self, slot, t, k):
        h = self.half
        if 0 < k <= self.sends:
            for way in (0, 1):
                self.copy(slot, k - 1, way).wait_recv()
        if 0 < k < h:
            for way in (0, 1):
                rows, chunk = self.part(way, k == 1), self.chunk(way, k - h)
                came = self.got[slot, k - 1, way, rows].astype(F32)
                self.own[slot, chunk, rows] = (self.own[slot, chunk, rows].astype(F32) + came).astype(BF16)
        if k == h:
            total = self.own[slot, self.me].astype(F32) + self.got[slot, h - 1, 0].astype(F32) + self.got[slot, h - 1, 1].astype(F32)
            self.out[slot, self.me] = total.astype(BF16)
        if k < self.sends:
            for way in (0, 1):
                self.copy(slot, k, way).start()
        if k == self.sends:
            for copy in self.write_out(slot, t):
                copy.start()
        for sent in range(h) if k == h else range(h, self.sends) if k == self.sends else ():
            for way in (0, 1):
                self.copy(slot, sent, way).wait_send()
        if k == self.sends + 1:
            for copy in self.write_out(slot, t):
                copy.wait()


SLOTS = 4
EVERY = 3
STARTS = (5, 9, 13, 20, 26, 27, 31, 41, 45, 49, 53, 63, 64, 65)


def train_kernel(n, x, dy, wg, wu, wd, sums, far0, far1, dgu, w_gu, w_d, a1, a2, at, dyv, dyt, h1, pulled, act, buf0, buf1,
                 acc_gu, acc_d, own, got, out, sem, wsem, push_sem, pull_sem, send, recv, out_sem):
    layers, slices = w_d.shape[:2]
    tiles = x.shape[0]
    total = layers * slices
    barrier = pltpu.get_barrier_semaphore()
    ring = Ring(n, own, got, out, sums, (far0, far1), send, recv, out_sem)
    for device in ring.to:
        pl.semaphore_signal(barrier, inc=1, device_id=device, device_id_type=pl.DeviceIdType.MESH)

    def columns(j):
        return pl.ds(pl.multiple_of(j * (2 * FS), 2 * FS), 2 * FS)

    def weights(l, j):
        return (
            pltpu.make_async_copy(wg.at[l, :, pl.ds(j * FS, FS)], w_gu.at[l, :, pl.ds(2 * j * FS, FS)], wsem.at[l, j, 0]),
            pltpu.make_async_copy(wu.at[l, :, pl.ds(j * FS, FS)], w_gu.at[l, :, pl.ds(2 * j * FS + FS, FS)], wsem.at[l, j, 1]),
            pltpu.make_async_copy(wd.at[l, pl.ds(j * FS, FS), :], w_d.at[l, j], wsem.at[l, j, 2]),
        )

    def state(m):
        return pltpu.make_async_copy(x.at[m], h1.at[m], sem.at[m])

    def cotangent(m):
        return pltpu.make_async_copy(dy.at[m], dyv.at[m], sem.at[tiles + m])

    state(0).start()
    for j in range(slices):
        for c in weights(0, j)[:2]:
            c.start()
    state(1).start()
    for j in range(slices):
        weights(0, j)[2].start()
    cotangent(0).start()
    for m in range(2, tiles):
        state(m).start()
        cotangent(m - 1).start()
    cotangent(tiles - 1).start()
    for j in range(slices):
        for c in weights(1, j):
            c.start()

    def forward_a(m, ready=lambda j: None):
        a1[m] = forward_first(h1[m], w_gu.at[0], act, ready)

    def forward_b(m):
        h = forward_second(h1[m], w_d.at[0], act)
        h1[m] = h
        a = normed(h)
        a2[m] = a
        at[m] = a.T
        dyt[m] = dyv[m].T

    def forward(m, _):
        state(m + 1).wait()
        cotangent(m).wait()
        forward_b(m)
        forward_a(m + 1)
        return 0

    def ready(j):
        for first, last in ((0, 2), (2, slices)):
            if j == first:
                for here in range(first, last):
                    for c in weights(0, here)[:2]:
                        c.wait()

    state(0).wait()
    forward_a(0, ready)
    for j in range(slices):
        weights(0, j)[2].wait()
    lax.fori_loop(0, tiles - 1, forward, 0)
    cotangent(tiles - 1).wait()
    forward_b(tiles - 1)
    for j in range(slices):
        for c in weights(1, j):
            c.wait()
    pl.semaphore_wait(barrier, 2)

    steps = tiles // PAIR
    turn_at, first_at, end_at = slices * steps, slices * steps + tiles, total * steps + tiles
    soonest = [steps * (t + 1) + (tiles if t >= slices else 0) + 1 for t in range(total)]
    starts = STARTS if len(STARTS) == total and all(a >= b for a, b in zip(STARTS, soonest)) else soonest
    plan, left = {}, {}
    for t, start in enumerate(starts):
        for k in range(ring.sends + 2):
            due = start + EVERY * k if k <= ring.sends else start + EVERY * ring.sends + 2
            if due < end_at:
                plan.setdefault(due, []).append((t, k))
            elif t not in left:
                left[t] = (k, due - end_at)
    most, kinds, base = max(len(some) for some in plan.values()), ring.sends + 2, total * (ring.sends + 2) + 1

    def events(step, low, high):
        held = jnp.int32(0)
        for due in range(low, high):
            number = 0
            for t, k in sorted(plan.get(due, ()), key=lambda e: e[1]):
                number = number * base + t * kinds + k + 1
            if number:
                held = jnp.where(step == due, number, held)

        def one(_, held):
            here = lax.rem(held, base)
            t = lax.div(lax.max(here - 1, 0), kinds)
            which = here - 1 - t * kinds
            for k in range(kinds):

                @pl.when((here > 0) & (which == k))
                def _():
                    ring.event(lax.rem(t, SLOTS), t, k)

            return lax.div(held, base)

        lax.fori_loop(0, most, one, held)

    def finish(s):
        slot = lax.rem(s, SLOTS)
        wide = acc_gu.shape[0] // n
        own[slot, :, :wide] = acc_gu[...].astype(BF16).reshape(n, wide, 2 * FS)
        own[slot, :, wide:] = acc_d[...].T.astype(BF16).reshape(n, FS // n, -1)
        acc_gu[...] = jnp.zeros_like(acc_gu)
        acc_d[...] = jnp.zeros_like(acc_d)

    def push(u, j, i):
        return pltpu.make_async_copy(
            (buf0, buf1)[i].at[:, :, pl.ds(0, 2 * FS)], dgu.at[pl.ds(u * PAIR, PAIR), :, columns(j)], push_sem.at[i]
        )

    def pull(m):
        return pltpu.make_async_copy(dgu.at[m], pulled.at[lax.rem(m, 2)], pull_sem.at[lax.rem(m, 2)])

    def backward(l):
        second = l == layers - 1
        states = a2 if second else a1

        def slice_a(u, j, buf):
            here = pl.ds(u * PAIR, PAIR)
            rows = (PAIR * TM, dyv.shape[-1])
            slice_first(states[here].reshape(rows), dyv[here].reshape(rows), w_gu[l, :, columns(j)], w_d[l, j], buf)

        def slice_b(u, buf):
            here = pl.ds(u * PAIR, PAIR)
            slice_second(at.at[here], dyt.at[here], buf, acc_gu, acc_d)

        def one_slice(j, _):
            def two_steps(i, _):
                for half, here, there in ((0, buf0, buf1), (1, buf1, buf0)):
                    u = 2 * i + half
                    events((0 if second else first_at) + j * steps + u, *((0, turn_at) if second else (first_at, end_at)))
                    if second:
                        @pl.when((i > 0) | (j > 0))
                        def _():
                            push(u, j, half).wait()

                    slice_a(u, j, here)
                    slice_b(lax.rem(u + steps - 1, steps), there)
                    if second:
                        push(u, j, half).start()
                    if half == 0:
                        @pl.when((i == 0) & (j > 0))
                        def _():
                            finish((0 if second else slices) + j - 1)

                return 0

            return lax.fori_loop(0, steps // 2, two_steps, 0)

        buf1[...] = jnp.zeros_like(buf1)
        lax.fori_loop(0, slices, one_slice, 0)
        if second:
            for m in (0, 1):
                pull(m).start()
        slice_b(steps - 1, buf1)
        finish((slices if second else total) - 1)

    def turn(m, _):
        events(turn_at + m, turn_at, first_at)
        pull(m).wait()
        parts = 2
        size = TM // parts
        for part in range(parts):
            rows = pl.ds(part * size, size)
            da = dot_t(pulled[lax.rem(m, 2), rows], w_gu[layers - 1])
            back = norm_back(da, h1[m, rows], dyv[m, rows])
            dyv[m, rows] = back
            dyt[m, :, rows] = back.T
            at[m, :, rows] = a1[m, rows].T

        @pl.when(m + 2 < tiles)
        def _():
            pull(m + 2).start()

        return 0

    acc_gu[...] = jnp.zeros_like(acc_gu)
    acc_d[...] = jnp.zeros_like(acc_d)
    backward(layers - 1)
    for i in (0, 1):
        push(i, 0, i).wait()
    lax.fori_loop(0, tiles, turn, 0)
    backward(0)

    for t, k in drain_order(left, ring.half, ring.sends):
        ring.event(t % SLOTS, t, k)


def drain_order(left, half, sends):
    step, beyond, now, wire, order = 0.92, 1.3, 0.0, 1.0, []
    ready = {t: 0.0 if k == 0 else max(0.0, (at - EVERY) * step + 1 + beyond) for t, (k, at) in left.items()}
    todo = {t: k for t, (k, _) in left.items()}
    while todo:
        can = [t for t, k in todo.items() if k < half - 1 or t - SLOTS not in todo]
        rank = {t: (todo[t] if todo[t] <= sends else -1 if t + SLOTS in todo else sends + 1, -t) for t in can}
        arrived = [t for t in can if ready[t] <= now]
        t = min(arrived, key=lambda t: rank[t]) if arrived else min(can, key=lambda t: (ready[t], rank[t]))
        k = todo[t]
        now = max(now, ready[t]) + 0.05
        order.append((t, k))
        if k < sends:
            wire = max(wire, now) + (0.5 if k == 0 else 1.0)
        ready[t] = wire + beyond if k < sends else now + 0.5
        todo[t] = k + 1
        if k > sends:
            del todo[t]
    return order


def adam_math(w, m, v, g):
    m = 0.9 * m + 0.1 * g
    v = 0.95 * v + 0.05 * g * g
    step = m * lax.rsqrt(v + 1e-8) + 0.1 * w
    return (w - 0.02 * step).astype(BF16), m, v


def adam_kernel(pieces, me, *refs):
    gs, ins, outs = refs[:pieces], refs[pieces : pieces + 9], refs[-9:]
    slices, wide = ins[2].shape[1], ins[0].shape[2]
    for j in range(slices):
        g = [(r[j] if r.shape[0] == slices else r[0, j]).reshape(r.shape[-2:]) for r in gs]
        g = [g[0] if pieces == 1 else jnp.concatenate(g[i : i + 2], axis=0) for i in range(0, pieces, 2)]
        g = [part.astype(F32) for part in g]
        g = g[0] if len(g) == 1 else jnp.where(pl.program_id(1) == 0, g[0], g[1])
        columns = slice(j * FS, (j + 1) * FS)
        for i, here in ((0, (0, 0, slice(None), columns)), (1, (0, 0, slice(None), columns)), (2, (0, j, 0))):
            part = (g[:wide, :FS], g[:wide, FS:], g[wide:])[i]
            w, m, v = (ins[k * 3 + i][here] for k in range(3))
            new = adam_math(w.astype(F32), m, v, part)
            for k in range(3):
                outs[k * 3 + i][here] = new[k]


def adam(n, first, stride, count, gs, arrays, so_far, vmem):
    layers, slices = arrays[0].shape[0], arrays[2].shape[1]
    me = lax.axis_index("dp").astype(jnp.int32).reshape(1)

    def chunk(o, me):
        return lax.rem(me[0] + o * stride + (first + n), n)

    def spec(g, place):
        if g.shape[1] == n:
            return pl.BlockSpec((slices, 1) + g.shape[2:], lambda l, o, me: (layers - 1 - l, chunk(o, me), 0, 0))
        if g.ndim == 3:
            return pl.BlockSpec((slices,) + g.shape[1:], lambda l, o, me: (layers - 1 - l, 0, 0))
        return pl.BlockSpec((1, slices) + g.shape[2:], lambda l, o, me: (place, layers - 1 - l, 0, 0))

    wide = pl.BlockSpec((1, 1) + arrays[0].shape[2:], lambda l, o, me: (l, chunk(o, me), 0, 0))
    tall = pl.BlockSpec((1, slices, 1) + arrays[2].shape[3:], lambda l, o, me: (l, 0, chunk(o, me), 0, 0))
    specs = [wide, wide, tall] * 3
    extra = [] if so_far is None else list(so_far)
    size = 2 * sum(a.size * a.dtype.itemsize for a in arrays) * count // n
    return pl.pallas_call(
        functools.partial(adam_kernel, len(gs)),
        grid_spec=pltpu.PrefetchScalarGridSpec(
            num_scalar_prefetch=1,
            grid=(layers, count),
            in_specs=[spec(g, place) for g, place in gs] + specs + [pl.BlockSpec(memory_space=pl.ANY)] * len(extra),
            out_specs=specs,
        ),
        out_shape=[jax.ShapeDtypeStruct(a.shape, a.dtype) for a in arrays],
        input_output_aliases={1 + len(gs) + 9 + i: i for i in range(len(extra))},
        compiler_params=pltpu.CompilerParams(vmem_limit_bytes=vmem),
        cost_estimate=pl.CostEstimate(flops=40 * size, bytes_accessed=size, transcendentals=0),
    )(me, *[g for g, _ in gs], *arrays, *extra)


def solution(mesh):
    n = mesh.shape["dp"]

    def step(x, dy, *arrays):
        wg, wu, wd = arrays[:3]
        tokens, d = x.shape[1:]
        layers, _, ff = wg.shape
        tiles, slices = tokens // TM, ff // FS
        x, dy = x.reshape(tiles, TM, d), dy.reshape(tiles, TM, d)
        hbm = pl.BlockSpec(memory_space=pl.ANY)
        half, rows = n // 2, (d + FS) // n
        mm = 2 * tokens * d * ff
        sums, *far, _ = pl.pallas_call(
            functools.partial(train_kernel, n),
            in_specs=[hbm] * 5,
            out_specs=[hbm] * 4,
            out_shape=[jax.ShapeDtypeStruct((layers * slices, n, rows, d), BF16)]
            + [jax.ShapeDtypeStruct((2, layers * slices, rows // 2, d), BF16)] * 2
            + [jax.ShapeDtypeStruct((tiles, TM, 2 * ff), BF16)],
            scratch_shapes=[
                pltpu.VMEM((layers, d, 2 * ff), BF16),
                pltpu.VMEM((layers, slices, FS, d), BF16),
                pltpu.VMEM((tiles, TM, d), BF16),
                pltpu.VMEM((tiles, TM, d), BF16),
                pltpu.VMEM((tiles, d, TM), BF16),
                pltpu.VMEM((tiles, TM, d), BF16),
                pltpu.VMEM((tiles, d, TM), BF16),
                pltpu.VMEM((tiles, TM, d), BF16),
                pltpu.VMEM((2, TM, 2 * ff), BF16),
                pltpu.VMEM((TM, ff), BF16),
                pltpu.VMEM((PAIR, TM, 3 * FS), BF16),
                pltpu.VMEM((PAIR, TM, 3 * FS), BF16),
                pltpu.VMEM((d, 2 * FS), F32),
                pltpu.VMEM((d, FS), F32),
                pltpu.VMEM((SLOTS, n, rows, d), BF16),
                pltpu.VMEM((SLOTS, half, 2, rows, d), BF16),
                pltpu.VMEM((SLOTS, n, rows, d), BF16),
                pltpu.SemaphoreType.DMA((2 * tiles,)),
                pltpu.SemaphoreType.DMA((layers, slices, 3)),
                pltpu.SemaphoreType.DMA((2,)),
                pltpu.SemaphoreType.DMA((2,)),
                pltpu.SemaphoreType.DMA((SLOTS, 2 * half - 2, 2)),
                pltpu.SemaphoreType.DMA((SLOTS, 2 * half - 2, 2)),
                pltpu.SemaphoreType.DMA((SLOTS, n + 1)),
            ],
            compiler_params=pltpu.CompilerParams(vmem_limit_bytes=VMEM_LIMIT, collective_id=0, has_side_effects=True),
            cost_estimate=pl.CostEstimate(flops=17 * mm, bytes_accessed=90 * 10**6, transcendentals=0),
        )(x, dy, wg, wu, wd)
        chunks = [a.reshape(layers, n, d // n, ff) if a.shape[1] == d else a.reshape(layers, slices, n, FS // n, d) for a in arrays]
        left = [(i, (i + n - 1) % n) for i in range(n)]
        right = [(i, (i + 1) % n) for i in range(n)]

        kept = half - 2
        near, last = [], []
        for i, way in enumerate((left, right)):
            near.append(lax.ppermute(far[i], "dp", way))
        new = adam(n, -kept, 1, 2 * kept + 1, [(sums, 0)], chunks, None, 60_000_000)
        for i, way in enumerate((left, right)):
            last.append(lax.ppermute(near[i][0], "dp", way))
        sides = [(near[0], 0), (near[0], 1), (near[1], 1), (near[1], 0)]
        new = adam(n, kept + 1, -2 * (kept + 1), 2, sides, chunks, new, 52_000_000)
        new = adam(n, half, 1, 1, [(a, 0) for a in last], chunks, new, 52_000_000)
        return tuple(o.reshape(a.shape) for o, a in zip(new, arrays))

    return jax.shard_map(
        step,
        mesh=mesh,
        in_specs=(P(("rep", "dp"), None, None),) * 2 + (P(None, None, None),) * 9,
        out_specs=(P("rep", None, None),) * 9,
        check_vma=False,
    )
```

```python
import functools

import jax
import jax.numpy as jnp
from jax import lax
from jax.experimental import pallas as pl
from jax.experimental.pallas import tpu as pltpu
from jax.sharding import PartitionSpec as P


TM = 512
PAIR = 2
FS = 256
F32, BF16 = jnp.float32, jnp.bfloat16
VMEM_LIMIT = 67_000_000


def dot(a, b):
    return jnp.dot(a, b, preferred_element_type=F32)


def dot_t(a, b):
    return lax.dot_general(a, b, (((1,), (1,)), ((), ())), preferred_element_type=F32)


def scale_of(wide):
    return lax.rsqrt(jnp.mean(wide * wide, -1, keepdims=True) + 1e-6)


def normed(h):
    wide = h.astype(F32)
    return (wide * scale_of(wide)).astype(BF16)


def sigmoid(g):
    return 0.5 * jnp.tanh(0.5 * g) + 0.5


def forward_first(h, w_gu, act_ref, ready=lambda j: None):
    a = normed(h)
    for j in range(w_gu.shape[1] // (2 * FS)):
        ready(j)
        gu = dot(a, w_gu[:, 2 * j * FS : 2 * (j + 1) * FS])
        g, u = gu[:, :FS], gu[:, FS:]
        act_ref[:, j * FS : (j + 1) * FS] = (g * sigmoid(g) * u).astype(BF16)
    return a


def forward_second(h, w_d, act_ref):
    slices = w_d.shape[0]
    y = dot(act_ref[...], w_d[...].reshape(slices * FS, -1)).astype(BF16)
    return (h.astype(F32) + y.astype(F32)).astype(BF16)


def slice_first(a, dy, wgu, wd, buf):
    gu = dot(a, wgu)
    dact = dot_t(dy, wd)
    g, u = gu[:, :FS], gu[:, FS:]
    dact = dact.astype(BF16).astype(F32)
    s = sigmoid(g)
    silu = g * s
    shape = buf.shape[:2] + (FS,)
    buf[:, :, 2 * FS : 3 * FS] = (silu * u).astype(BF16).reshape(shape)
    buf[:, :, FS : 2 * FS] = (dact * silu).astype(BF16).reshape(shape)
    buf[:, :, :FS] = (dact * u * (s + silu * (1.0 - s))).astype(BF16).reshape(shape)


def slice_second(a_t, dy_t, buf, acc_gu, acc_d):
    acc_d[...] += sum(dot(dy_t[i], buf[i, :, 2 * FS : 3 * FS]) for i in range(PAIR))
    acc_gu[...] += sum(dot(a_t[i], buf[i, :, : 2 * FS]) for i in range(PAIR))


def norm_back(da, h, dy):
    d = h.shape[-1]
    da = da.astype(BF16).astype(F32)
    h = h.astype(F32)
    r = scale_of(h)
    along = jnp.sum(da * h, -1, keepdims=True)
    dh = (da * r - h * (along * r * r * r * (1.0 / d))).astype(BF16)
    return (dy.astype(F32) + dh.astype(F32)).astype(BF16)


class Ring:
    def __init__(self, n, own, got, out, sums, far, send, recv, out_sem):
        self.n, self.half, self.rows = n, n // 2, own.shape[2]
        self.kept = self.half - 2
        self.sends = self.half + self.kept
        self.own, self.got, self.out, self.sums, self.far = own, got, out, sums, far
        self.send, self.recv, self.out_sem = send, recv, out_sem
        self.me = lax.axis_index("dp")
        self.to = ({"dp": lax.rem(self.me + n - 1, n)}, {"dp": lax.rem(self.me + 1, n)})

    def chunk(self, way, offset):
        return lax.rem(self.me + (offset if way == 0 else -offset) + self.n, self.n)

    def part(self, way, halved):
        size = self.rows // 2 if halved else self.rows
        return pl.ds(size if halved and way == 1 else 0, size)

    def copy(self, slot, k, way):
        h = self.half
        rows = self.part(way, k == 0)
        chunk = self.chunk(way, k - h)
        if k < h:
            src = self.own.at[slot, chunk, rows]
            dst = self.got.at[slot, k, way, rows]
        else:
            src = dst = self.out.at[slot, chunk, rows]
        return pltpu.make_async_remote_copy(
            src_ref=src,
            dst_ref=dst,
            send_sem=self.send.at[slot, k, way],
            recv_sem=self.recv.at[slot, k, way],
            device_id=self.to[way],
            device_id_type=pl.DeviceIdType.MESH,
        )

    def write_out(self, slot, t):
        copies = []
        for offset in range(-self.kept, self.kept + 1):
            chunk = self.chunk(0, offset)
            copies.append((self.out.at[slot, chunk], self.sums.at[t, chunk]))
        for way in (0, 1):
            chunk = self.chunk(way, self.kept)
            for place, part in ((0, way), (1, 1 - way)):
                copies.append((self.out.at[slot, chunk, self.part(part, True)], self.far[way].at[place, t]))
        return [pltpu.make_async_copy(a, b, self.out_sem.at[slot, i]) for i, (a, b) in enumerate(copies)]

    def event(self, slot, t, k):
        h = self.half
        if 0 < k <= self.sends:
            for way in (0, 1):
                self.copy(slot, k - 1, way).wait_recv()
        if 0 < k < h:
            for way in (0, 1):
                rows, chunk = self.part(way, k == 1), self.chunk(way, k - h)
                came = self.got[slot, k - 1, way, rows].astype(F32)
                self.own[slot, chunk, rows] = (self.own[slot, chunk, rows].astype(F32) + came).astype(BF16)
        if k == h:
            total = self.own[slot, self.me].astype(F32) + self.got[slot, h - 1, 0].astype(F32) + self.got[slot, h - 1, 1].astype(F32)
            self.out[slot, self.me] = total.astype(BF16)
        if k < self.sends:
            for way in (0, 1):
                self.copy(slot, k, way).start()
        if k == self.sends:
            for copy in self.write_out(slot, t):
                copy.start()
        for sent in range(h) if k == h else range(h, self.sends) if k == self.sends else ():
            for way in (0, 1):
                self.copy(slot, sent, way).wait_send()
        if k == self.sends + 1:
            for copy in self.write_out(slot, t):
                copy.wait()


SLOTS = 4
EVERY = 3


def train_kernel(n, x, dy, wg, wu, wd, sums, far0, far1, dgu, w_gu, w_d, a1, a2, at, dyv, dyt, h1, pulled, act, buf0, buf1,
                 acc_gu, acc_d, own, got, out, sem, wsem, push_sem, pull_sem, send, recv, out_sem):
    layers, slices = w_d.shape[:2]
    tiles = x.shape[0]
    total = layers * slices
    barrier = pltpu.get_barrier_semaphore()
    ring = Ring(n, own, got, out, sums, (far0, far1), send, recv, out_sem)
    for device in ring.to:
        pl.semaphore_signal(barrier, inc=1, device_id=device, device_id_type=pl.DeviceIdType.MESH)

    def columns(j):
        return pl.ds(pl.multiple_of(j * (2 * FS), 2 * FS), 2 * FS)

    def weights(l, j):
        return (
            pltpu.make_async_copy(wg.at[l, :, pl.ds(j * FS, FS)], w_gu.at[l, :, pl.ds(2 * j * FS, FS)], wsem.at[l, j, 0]),
            pltpu.make_async_copy(wu.at[l, :, pl.ds(j * FS, FS)], w_gu.at[l, :, pl.ds(2 * j * FS + FS, FS)], wsem.at[l, j, 1]),
            pltpu.make_async_copy(wd.at[l, pl.ds(j * FS, FS), :], w_d.at[l, j], wsem.at[l, j, 2]),
        )

    def state(m):
        return pltpu.make_async_copy(x.at[m], h1.at[m], sem.at[m])

    def cotangent(m):
        return pltpu.make_async_copy(dy.at[m], dyv.at[m], sem.at[tiles + m])

    state(0).start()
    for j in range(slices):
        for c in weights(0, j)[:2]:
            c.start()

    def forward_a(m, ready=lambda j: None):
        a1[m] = forward_first(h1[m], w_gu.at[0], act, ready)

    def forward_b(m):
        h = forward_second(h1[m], w_d.at[0], act)
        h1[m] = h
        a = normed(h)
        a2[m] = a
        at[m] = a.T
        dyt[m] = dyv[m].T

    def forward(m, _):
        state(m + 1).wait()
        cotangent(m).wait()
        forward_b(m)
        forward_a(m + 1)
        return 0

    def ready(j):
        for first, last in ((0, 1), (1, slices)):
            if j == first:
                for here in range(first, last):
                    for c in weights(0, here)[:2]:
                        c.wait()
                if last < slices:
                    for here in range(slices):
                        weights(0, here)[2].start()
                    state(1).start()
                    cotangent(0).start()
                else:
                    for m in range(2, tiles):
                        state(m).start()
                        cotangent(m - 1).start()
                    cotangent(tiles - 1).start()
                    for here in range(slices):
                        for c in weights(1, here):
                            c.start()

    state(0).wait()
    forward_a(0, ready)
    for j in range(slices):
        weights(0, j)[2].wait()
    lax.fori_loop(0, tiles - 1, forward, 0)
    cotangent(tiles - 1).wait()
    forward_b(tiles - 1)
    for j in range(slices):
        for c in weights(1, j):
            c.wait()
    pl.semaphore_wait(barrier, 2)

    steps = tiles // PAIR
    turns = tiles // steps
    offsets = [1 + EVERY * k for k in range(ring.sends + 1)] + [3 + EVERY * ring.sends]

    def round_of(now):
        found = []
        for ago in range(1 + offsets[-1] // steps):
            place = now - 1 - ago
            t = jnp.where(place >= slices, place - turns, place)
            there = (place >= 0) & (t < total) & ((place < slices) | (t >= slices))
            found.append((there, t, lax.rem(t + SLOTS, SLOTS)))
        return found

    def events(found, u, odd=None):
        for k in range(len(offsets)):
            ago, at_step = divmod(offsets[k], steps)
            if odd is not None and at_step % 2 != odd:
                continue
            there, t, slot = found[ago]

            @pl.when((u == at_step) & there)
            def _():
                ring.event(slot, t, k)

    def finish(s):
        slot = lax.rem(s, SLOTS)
        wide = acc_gu.shape[0] // n
        own[slot, :, :wide] = acc_gu[...].astype(BF16).reshape(n, wide, 2 * FS)
        own[slot, :, wide:] = acc_d[...].T.astype(BF16).reshape(n, FS // n, -1)
        acc_gu[...] = jnp.zeros_like(acc_gu)
        acc_d[...] = jnp.zeros_like(acc_d)

    def push(u, j, i):
        return pltpu.make_async_copy(
            (buf0, buf1)[i].at[:, :, pl.ds(0, 2 * FS)], dgu.at[pl.ds(u * PAIR, PAIR), :, columns(j)], push_sem.at[i]
        )

    def pull(m):
        return pltpu.make_async_copy(dgu.at[m], pulled.at[lax.rem(m, 2)], pull_sem.at[lax.rem(m, 2)])

    def backward(l):
        second = l == layers - 1
        states = a2 if second else a1

        def slice_a(u, j, buf):
            here = pl.ds(u * PAIR, PAIR)
            rows = (PAIR * TM, dyv.shape[-1])
            slice_first(states[here].reshape(rows), dyv[here].reshape(rows), w_gu[l, :, columns(j)], w_d[l, j], buf)

        def slice_b(u, buf):
            here = pl.ds(u * PAIR, PAIR)
            slice_second(at.at[here], dyt.at[here], buf, acc_gu, acc_d)

        def one_slice(j, _):
            found = round_of(j if second else slices + turns + j)

            def two_steps(i, _):
                for half, here, there in ((0, buf0, buf1), (1, buf1, buf0)):
                    u = 2 * i + half
                    events(found, u, half)
                    if second:
                        @pl.when((i > 0) | (j > 0))
                        def _():
                            push(u, j, half).wait()

                    slice_a(u, j, here)
                    slice_b(lax.rem(u + steps - 1, steps), there)
                    if second:
                        push(u, j, half).start()
                    if half == 0:
                        @pl.when((i == 0) & (j > 0))
                        def _():
                            finish((0 if second else slices) + j - 1)

                return 0

            return lax.fori_loop(0, steps // 2, two_steps, 0)

        buf1[...] = jnp.zeros_like(buf1)
        lax.fori_loop(0, slices, one_slice, 0)
        if second:
            for m in (0, 1):
                pull(m).start()
        slice_b(steps - 1, buf1)
        finish((slices if second else total) - 1)

    def turn(m, _):
        events(round_of(slices + m // steps), lax.rem(m, steps))
        pull(m).wait()
        parts = 2
        size = TM // parts
        for part in range(parts):
            rows = pl.ds(part * size, size)
            da = dot_t(pulled[lax.rem(m, 2), rows], w_gu[layers - 1])
            back = norm_back(da, h1[m, rows], dyv[m, rows])
            dyv[m, rows] = back
            dyt[m, :, rows] = back.T
            at[m, :, rows] = a1[m, rows].T

        @pl.when(m + 2 < tiles)
        def _():
            pull(m + 2).start()

        return 0

    acc_gu[...] = jnp.zeros_like(acc_gu)
    acc_d[...] = jnp.zeros_like(acc_d)
    backward(layers - 1)
    for i in (0, 1):
        push(i, 0, i).wait()
    lax.fori_loop(0, tiles, turn, 0)
    backward(0)

    left = {}
    for t in range(total):
        start = steps * (t + 1 + (turns if t >= slices else 0))
        late = [(k, start + offset - steps * (total + turns)) for k, offset in enumerate(offsets)]
        late = [(k, at) for k, at in late if at >= 0]
        if late:
            left[t] = late[0]
    for t, k in drain_order(left, ring.half, ring.sends):
        ring.event(t % SLOTS, t, k)


def drain_order(left, half, sends):
    step, beyond, now, wire, order = 0.92, 1.3, 0.0, 1.0, []
    ready = {t: 0.0 if k == 0 else max(0.0, (at - EVERY) * step + 1 + beyond) for t, (k, at) in left.items()}
    todo = {t: k for t, (k, _) in left.items()}
    while todo:
        can = [t for t, k in todo.items() if k < half - 1 or t - SLOTS not in todo]
        rank = {t: (todo[t] if todo[t] <= sends else -1 if t + SLOTS in todo else sends + 1, -t) for t in can}
        arrived = [t for t in can if ready[t] <= now]
        t = min(arrived, key=lambda t: rank[t]) if arrived else min(can, key=lambda t: (ready[t], rank[t]))
        k = todo[t]
        now = max(now, ready[t]) + 0.05
        order.append((t, k))
        if k < sends:
            wire = max(wire, now) + (0.5 if k == 0 else 1.0)
        ready[t] = wire + beyond if k < sends else now + 0.5
        todo[t] = k + 1
        if k > sends:
            del todo[t]
    return order


def adam_math(w, m, v, g):
    m = 0.9 * m + 0.1 * g
    v = 0.95 * v + 0.05 * g * g
    step = m * lax.rsqrt(v + 1e-8) + 0.1 * w
    return (w - 0.02 * step).astype(BF16), m, v


def adam_kernel(pieces, me, *refs):
    gs, ins, outs = refs[:pieces], refs[pieces : pieces + 9], refs[-9:]
    slices, wide = ins[2].shape[1], ins[0].shape[2]
    for j in range(slices):
        g = [(r[j] if r.shape[0] == slices else r[0, j]).reshape(r.shape[-2:]) for r in gs]
        g = [g[0] if pieces == 1 else jnp.concatenate(g[i : i + 2], axis=0) for i in range(0, pieces, 2)]
        g = [part.astype(F32) for part in g]
        g = g[0] if len(g) == 1 else jnp.where(pl.program_id(1) == 0, g[0], g[1])
        columns = slice(j * FS, (j + 1) * FS)
        for i, here in ((0, (0, 0, slice(None), columns)), (1, (0, 0, slice(None), columns)), (2, (0, j, 0))):
            part = (g[:wide, :FS], g[:wide, FS:], g[wide:])[i]
            w, m, v = (ins[k * 3 + i][here] for k in range(3))
            new = adam_math(w.astype(F32), m, v, part)
            for k in range(3):
                outs[k * 3 + i][here] = new[k]


def adam(n, first, stride, count, gs, arrays, so_far, vmem):
    layers, slices = arrays[0].shape[0], arrays[2].shape[1]
    me = lax.axis_index("dp").astype(jnp.int32).reshape(1)

    def chunk(o, me):
        return lax.rem(me[0] + o * stride + (first + n), n)

    def spec(g, place):
        if g.shape[1] == n:
            return pl.BlockSpec((slices, 1) + g.shape[2:], lambda l, o, me: (layers - 1 - l, chunk(o, me), 0, 0))
        if g.ndim == 3:
            return pl.BlockSpec((slices,) + g.shape[1:], lambda l, o, me: (layers - 1 - l, 0, 0))
        return pl.BlockSpec((1, slices) + g.shape[2:], lambda l, o, me: (place, layers - 1 - l, 0, 0))

    wide = pl.BlockSpec((1, 1) + arrays[0].shape[2:], lambda l, o, me: (l, chunk(o, me), 0, 0))
    tall = pl.BlockSpec((1, slices, 1) + arrays[2].shape[3:], lambda l, o, me: (l, 0, chunk(o, me), 0, 0))
    specs = [wide, wide, tall] * 3
    extra = [] if so_far is None else list(so_far)
    size = 2 * sum(a.size * a.dtype.itemsize for a in arrays) * count // n
    return pl.pallas_call(
        functools.partial(adam_kernel, len(gs)),
        grid_spec=pltpu.PrefetchScalarGridSpec(
            num_scalar_prefetch=1,
            grid=(layers, count),
            in_specs=[spec(g, place) for g, place in gs] + specs + [pl.BlockSpec(memory_space=pl.ANY)] * len(extra),
            out_specs=specs,
        ),
        out_shape=[jax.ShapeDtypeStruct(a.shape, a.dtype) for a in arrays],
        input_output_aliases={1 + len(gs) + 9 + i: i for i in range(len(extra))},
        compiler_params=pltpu.CompilerParams(vmem_limit_bytes=vmem),
        cost_estimate=pl.CostEstimate(flops=40 * size, bytes_accessed=size, transcendentals=0),
    )(me, *[g for g, _ in gs], *arrays, *extra)


def solution(mesh):
    n = mesh.shape["dp"]

    def step(x, dy, *arrays):
        wg, wu, wd = arrays[:3]
        tokens, d = x.shape[1:]
        layers, _, ff = wg.shape
        tiles, slices = tokens // TM, ff // FS
        x, dy = x.reshape(tiles, TM, d), dy.reshape(tiles, TM, d)
        hbm = pl.BlockSpec(memory_space=pl.ANY)
        half, rows = n // 2, (d + FS) // n
        mm = 2 * tokens * d * ff
        sums, *far, _ = pl.pallas_call(
            functools.partial(train_kernel, n),
            in_specs=[hbm] * 5,
            out_specs=[hbm] * 4,
            out_shape=[jax.ShapeDtypeStruct((layers * slices, n, rows, d), BF16)]
            + [jax.ShapeDtypeStruct((2, layers * slices, rows // 2, d), BF16)] * 2
            + [jax.ShapeDtypeStruct((tiles, TM, 2 * ff), BF16)],
            scratch_shapes=[
                pltpu.VMEM((layers, d, 2 * ff), BF16),
                pltpu.VMEM((layers, slices, FS, d), BF16),
                pltpu.VMEM((tiles, TM, d), BF16),
                pltpu.VMEM((tiles, TM, d), BF16),
                pltpu.VMEM((tiles, d, TM), BF16),
                pltpu.VMEM((tiles, TM, d), BF16),
                pltpu.VMEM((tiles, d, TM), BF16),
                pltpu.VMEM((tiles, TM, d), BF16),
                pltpu.VMEM((2, TM, 2 * ff), BF16),
                pltpu.VMEM((TM, ff), BF16),
                pltpu.VMEM((PAIR, TM, 3 * FS), BF16),
                pltpu.VMEM((PAIR, TM, 3 * FS), BF16),
                pltpu.VMEM((d, 2 * FS), F32),
                pltpu.VMEM((d, FS), F32),
                pltpu.VMEM((SLOTS, n, rows, d), BF16),
                pltpu.VMEM((SLOTS, half, 2, rows, d), BF16),
                pltpu.VMEM((SLOTS, n, rows, d), BF16),
                pltpu.SemaphoreType.DMA((2 * tiles,)),
                pltpu.SemaphoreType.DMA((layers, slices, 3)),
                pltpu.SemaphoreType.DMA((2,)),
                pltpu.SemaphoreType.DMA((2,)),
                pltpu.SemaphoreType.DMA((SLOTS, 2 * half - 2, 2)),
                pltpu.SemaphoreType.DMA((SLOTS, 2 * half - 2, 2)),
                pltpu.SemaphoreType.DMA((SLOTS, n + 1)),
            ],
            compiler_params=pltpu.CompilerParams(vmem_limit_bytes=VMEM_LIMIT, collective_id=0, has_side_effects=True),
            cost_estimate=pl.CostEstimate(flops=17 * mm, bytes_accessed=90 * 10**6, transcendentals=0),
        )(x, dy, wg, wu, wd)
        chunks = [a.reshape(layers, n, d // n, ff) if a.shape[1] == d else a.reshape(layers, slices, n, FS // n, d) for a in arrays]
        left = [(i, (i + n - 1) % n) for i in range(n)]
        right = [(i, (i + 1) % n) for i in range(n)]

        kept = half - 2
        near, last = [], []
        for i, way in enumerate((left, right)):
            near.append(lax.ppermute(far[i], "dp", way))
        new = adam(n, -kept, 1, 2 * kept + 1, [(sums, 0)], chunks, None, 60_000_000)
        for i, way in enumerate((left, right)):
            last.append(lax.ppermute(near[i][0], "dp", way))
        sides = [(near[0], 0), (near[0], 1), (near[1], 1), (near[1], 0)]
        new = adam(n, kept + 1, -2 * (kept + 1), 2, sides, chunks, new, 52_000_000)
        new = adam(n, half, 1, 1, [(a, 0) for a in last], chunks, new, 52_000_000)
        return tuple(o.reshape(a.shape) for o, a in zip(new, arrays))

    return jax.shard_map(
        step,
        mesh=mesh,
        in_specs=(P(("rep", "dp"), None, None),) * 2 + (P(None, None, None),) * 9,
        out_specs=(P("rep", None, None),) * 9,
        check_vma=False,
    )
```
